8 devices in a mesh: dp: 2 (over z, y), a: 4 (over x, core).
Axes of the slice: x: 2, y: 2, z: 1, core: 2. Of those that a mesh axis runs over, the one named last changes fastest.
Arguments:
- hidden_in: bfloat16 [16, 2560], P('dp'), parts along dimension 0
- loc_k: bfloat16 [16, 4, 6144, 256], P('dp', None, 'a'), parts along dimension 0
- loc_v: bfloat16 [16, 4, 6144, 256], P('dp', None, 'a'), parts along dimension 0
- glo_k: bfloat16 [16, 4, 6144, 256], P('dp', None, 'a'), parts along dimension 0
- glo_v: bfloat16 [16, 4, 6144, 256], P('dp', None, 'a'), parts along dimension 0
- loc_wq: bfloat16 [2560, 2048], P(None, 'a')
- loc_wk: bfloat16 [2560, 1024], P(None, 'a')
- loc_wv: bfloat16 [2560, 1024], P(None, 'a')
- loc_wo: bfloat16 [2048, 2560], P('a')
- loc_pre: bfloat16 [2560], replicated
- loc_post: bfloat16 [2560], replicated
- glo_wq: bfloat16 [2560, 2048], P(None, 'a')
- glo_wk: bfloat16 [2560, 1024], P(None, 'a')
- glo_wv: bfloat16 [2560, 1024], P(None, 'a')
- glo_wo: bfloat16 [2048, 2560], P('a')
- glo_pre: bfloat16 [2560], replicated
- glo_post: bfloat16 [2560], replicated
Outputs:
- output 1: bfloat16 [16, 2560], P('dp'), parts along dimension 0
- output 2: bfloat16 [16, 4, 4096, 256], P('dp', 'a'), parts along dimension 0
- output 3: bfloat16 [16, 4, 4096, 256], P('dp', 'a'), parts along dimension 0
- output 4: bfloat16 [16, 4, 6656, 256], P('dp', 'a'), parts along dimension 0
- output 5: bfloat16 [16, 4, 6656, 256], P('dp', 'a'), parts along dimension 0
There are 2 independent parts. The reference program is written for one: setup_inputs(seed, part) draws one part's arguments, and reference() takes and returns one part's arrays. A program takes and returns all parts, laid end to end along the dimension named above; an argument that names none is the same for every part.
All inputs are finite; a program needn't handle non-finite values.
Results may differ from the reference program's by a relative error of at most 0.02.
Values are sent between devices in bfloat16 or wider.
A program may use at most 1 GiB of HBM per device.

```python
import jax
import jax.numpy as jnp
from jax import lax

BATCH_SIZE = 8
SEQ_LEN = 6144
WINDOW = 4096
D_MODEL = 2560
NUM_HEADS = 8
KV_HEADS = 4
HEAD_DIM = 256
CACHE_ROOM = 512

Q_GROUPS = NUM_HEADS // KV_HEADS
Q_COLS = NUM_HEADS * HEAD_DIM
KV_COLS = KV_HEADS * HEAD_DIM
SOFTCAP = 50.0
NORM_EPS = 1e-6
ROPE_BASE = 10000.0
KEY_GAIN = 4.0


def draw_normal(rng_key, shape, std_dev):
    return (std_dev * jax.random.normal(rng_key, shape, jnp.float32)).astype(jnp.bfloat16)


def setup_inputs(seed: int = 0, part: int = 0) -> dict:
    part_keys = jax.random.split(jax.random.fold_in(jax.random.key(seed), part), 5)
    shared_keys = jax.random.split(jax.random.key(seed + 1), 12)
    cache_shape = (BATCH_SIZE, KV_HEADS, SEQ_LEN, HEAD_DIM)
    in_std = D_MODEL ** -0.5
    key_std = KEY_GAIN * in_std
    out_std = Q_COLS ** -0.5
    return {
        'hidden_in': draw_normal(part_keys[0], (BATCH_SIZE, D_MODEL), 1.0),
        'loc_k': draw_normal(part_keys[1], cache_shape, 1.0),
        'loc_v': draw_normal(part_keys[2], cache_shape, 1.0),
        'glo_k': draw_normal(part_keys[3], cache_shape, 1.0),
        'glo_v': draw_normal(part_keys[4], cache_shape, 1.0),
        'loc_wq': draw_normal(shared_keys[0], (D_MODEL, Q_COLS), in_std),
        'loc_wk': draw_normal(shared_keys[1], (D_MODEL, KV_COLS), key_std),
        'loc_wv': draw_normal(shared_keys[2], (D_MODEL, KV_COLS), in_std),
        'loc_wo': draw_normal(shared_keys[3], (Q_COLS, D_MODEL), out_std),
        'loc_pre': draw_normal(shared_keys[4], (D_MODEL,), 0.5),
        'loc_post': draw_normal(shared_keys[5], (D_MODEL,), 0.5),
        'glo_wq': draw_normal(shared_keys[6], (D_MODEL, Q_COLS), in_std),
        'glo_wk': draw_normal(shared_keys[7], (D_MODEL, KV_COLS), key_std),
        'glo_wv': draw_normal(shared_keys[8], (D_MODEL, KV_COLS), in_std),
        'glo_wo': draw_normal(shared_keys[9], (Q_COLS, D_MODEL), out_std),
        'glo_pre': draw_normal(shared_keys[10], (D_MODEL,), 0.5),
        'glo_post': draw_normal(shared_keys[11], (D_MODEL,), 0.5),
    }


def rms_norm(hidden, gain):
    mean_sq = jnp.mean(hidden * hidden, axis=-1, keepdims=True)
    return hidden * lax.rsqrt(mean_sq + NORM_EPS) * (1.0 + gain.astype(jnp.float32))


def rope_at(heads, position):
    half_dim = HEAD_DIM // 2
    inv_freq = ROPE_BASE ** (-2.0 * jnp.arange(half_dim, dtype=jnp.float32) / HEAD_DIM)
    angles = position * inv_freq
    cosine = jnp.cos(angles)
    sine_val = jnp.sin(angles)
    first_half = heads[..., :half_dim]
    second_half = heads[..., half_dim:]
    return jnp.concatenate([first_half * cosine - second_half * sine_val, second_half * cosine + first_half * sine_val], axis=-1)


def attend(q_heads, keys_all, values_all):
    scores = jnp.einsum('bkgd,bkld->bkgl', q_heads.astype(jnp.float32), keys_all.astype(jnp.float32)) * HEAD_DIM ** -0.5
    scores = SOFTCAP * jnp.tanh(scores / SOFTCAP)
    top_score = jnp.max(scores, axis=-1, keepdims=True)
    weights = jnp.exp(scores - top_score)
    denom_sum = jnp.sum(weights, axis=-1, keepdims=True)
    weighted = jnp.einsum('bkgl,bkld->bkgd', weights.astype(jnp.bfloat16).astype(jnp.float32), values_all.astype(jnp.float32))
    return (weighted / denom_sum).astype(jnp.bfloat16).reshape(BATCH_SIZE, Q_COLS)


def layer_step(hidden, cache_k, cache_v, w_q, w_k, w_v, w_o, pre_gain, post_gain, is_local):
    normed = rms_norm(hidden.astype(jnp.float32), pre_gain).astype(jnp.bfloat16)
    q_proj = jnp.dot(normed, w_q, preferred_element_type=jnp.float32).reshape(BATCH_SIZE, KV_HEADS, Q_GROUPS, HEAD_DIM)
    q_heads = rope_at(q_proj, SEQ_LEN).astype(jnp.bfloat16)
    k_proj = jnp.dot(normed, w_k, preferred_element_type=jnp.float32).reshape(BATCH_SIZE, KV_HEADS, 1, HEAD_DIM)
    new_k = rope_at(k_proj, SEQ_LEN).astype(jnp.bfloat16)
    new_v = jnp.dot(normed, w_v, preferred_element_type=jnp.float32).astype(jnp.bfloat16).reshape(BATCH_SIZE, KV_HEADS, 1, HEAD_DIM)
    if is_local:
        ordered_k = jnp.concatenate([cache_k[:, :, SEQ_LEN - WINDOW + 1:], new_k], axis=2)
        ordered_v = jnp.concatenate([cache_v[:, :, SEQ_LEN - WINDOW + 1:], new_v], axis=2)
        attn_out = attend(q_heads, ordered_k, ordered_v)
        out_k = jnp.roll(ordered_k, (SEQ_LEN + 1) % WINDOW, axis=2)
        out_v = jnp.roll(ordered_v, (SEQ_LEN + 1) % WINDOW, axis=2)
    else:
        zero_pad = jnp.zeros((BATCH_SIZE, KV_HEADS, CACHE_ROOM - 1, HEAD_DIM), jnp.bfloat16)
        out_k = jnp.concatenate([cache_k, new_k, zero_pad], axis=2)
        out_v = jnp.concatenate([cache_v, new_v, zero_pad], axis=2)
        attn_out = attend(q_heads, out_k[:, :, :SEQ_LEN + 1], out_v[:, :, :SEQ_LEN + 1])
    proj_out = jnp.dot(attn_out, w_o, preferred_element_type=jnp.float32)
    hidden = (hidden.astype(jnp.float32) + rms_norm(proj_out, post_gain)).astype(jnp.bfloat16)
    return hidden, out_k, out_v


def reference(hidden_in, loc_k, loc_v, glo_k, glo_v, loc_wq, loc_wk, loc_wv, loc_wo, loc_pre, loc_post, glo_wq, glo_wk, glo_wv, glo_wo, glo_pre, glo_post):
    hidden, loc_k_out, loc_v_out = layer_step(hidden_in, loc_k, loc_v, loc_wq, loc_wk, loc_wv, loc_wo, loc_pre, loc_post, True)
    hidden_out, glo_k_out, glo_v_out = layer_step(hidden, glo_k, glo_v, glo_wq, glo_wk, glo_wv, glo_wo, glo_pre, glo_post, False)
    return (hidden_out, loc_k_out, loc_v_out, glo_k_out, glo_v_out)
```

```python
import jax
import jax.numpy as jnp
import numpy as np
from jax import lax
from jax.experimental import pallas as pl
from jax.experimental.pallas import tpu as pltpu
from jax.sharding import PartitionSpec as P

SOFTCAP = 50.0
NORM_EPS = 1e-6
ROPE_BASE = 10000.0
WINDOW = 4096
CACHE_ROOM = 512

GROUP = 4
ROWS = 8
BLOCK = 1536
UNIT = 512
HEAD = 256
SEQ = GROUP * BLOCK
PER = BLOCK // UNIT
GLO_UNITS = SEQ // UNIT
LOC_UNITS = WINDOW // UNIT
FIRST_UNIT = (SEQ - WINDOW) // UNIT
STEPS = 4 * ROWS * PER
DEPTH = 2
LEFT = 0
MESH = pl.DeviceIdType.MESH
LOW = -1e30


def peers(me):
    return (me + 1 - 2 * (me % 2), (me + 2) % 4, 3 - me)


def norm(hidden, gain):
    mean_sq = jnp.mean(hidden * hidden, axis=-1, keepdims=True)
    return hidden * lax.rsqrt(mean_sq + NORM_EPS) * (1.0 + gain.astype(jnp.float32))


def softcap(scores):
    return SOFTCAP * jnp.tanh(scores * (HEAD ** -0.5) / SOFTCAP)


def move_kernel(hid, trig, lpre, lpost, gpre, gpost, lk, lv, gk, gv, lwq, lwk, lwv, lwo, gwq, gwk, gwv, gwo,
                land_lk, land_lv, land_gk, land_gv, hid_out, new_kv,
                wq, wk, wv, wo, kvbuf, qbuf, part, precv, ybuf,
                bulk_send, loc_recv, glo_recv, w_sem, kv_sem, ex_send, ex_recv):
    dp = lax.axis_index("dp")
    me = lax.axis_index("a")
    dest = peers(me)
    caches = (lk, lv, gk, gv)
    lands = (land_lk, land_lv, land_gk, land_gv)

    barrier = pltpu.get_barrier_semaphore()
    for peer in dest:
        pl.semaphore_signal(barrier, inc=1, device_id=(dp, peer), device_id_type=MESH)
    pl.semaphore_wait(barrier, 3)

    def valid(step, k):
        c, r, j = step // (ROWS * PER), (step // PER) % ROWS, step % PER
        in_window = jnp.logical_or(c >= 2, PER * me + j >= FIRST_UNIT)
        ok = jnp.logical_and(step >= 0, in_window)
        if k == 1 and LEFT:
            later = jnp.logical_and(jnp.logical_and(c == 3, r >= ROWS - LEFT), me >= 2)
            ok = jnp.logical_and(ok, jnp.logical_not(later))
        return ok

    def pump(step):
        c, r, j = step // (ROWS * PER), (step // PER) % ROWS, step % PER
        slot = step % DEPTH
        for k in range(3):
            @pl.when(valid(step - DEPTH, k))
            def _():
                pltpu.make_async_remote_copy(
                    src_ref=gk.at[0, 0, pl.ds(0, UNIT)], dst_ref=land_gk.at[0, 0, pl.ds(0, UNIT)],
                    send_sem=bulk_send.at[k, slot], recv_sem=glo_recv.at[0, 0],
                    device_id=(dp, dest[k]), device_id_type=MESH).wait_send()
        unit = PER * me + j
        for i in range(4):
            place = unit % LOC_UNITS if i < 2 else unit
            sem = loc_recv.at[i, place] if i < 2 else glo_recv.at[i - 2, place]
            for k in range(3):
                @pl.when(jnp.logical_and(c == i, valid(step, k)))
                def _():
                    pltpu.make_async_remote_copy(
                        src_ref=caches[i].at[r, dest[k], pl.ds(pl.multiple_of(j * UNIT, UNIT), UNIT)],
                        dst_ref=lands[i].at[r, 0, pl.ds(pl.multiple_of(place * UNIT, UNIT), UNIT)],
                        send_sem=bulk_send.at[k, slot], recv_sem=sem,
                        device_id=(dp, dest[k]), device_id_type=MESH).start()

    def exchange(index, src_of, dst):
        copies = []
        for k in range(3):
            copies.append(pltpu.make_async_remote_copy(
                src_ref=src_of(dest[k]), dst_ref=dst.at[me], send_sem=ex_send.at[index, k], recv_sem=ex_recv.at[index, k],
                device_id=(dp, dest[k]), device_id_type=MESH))
        for copy in copies:
            copy.start()
        return copies

    def finish(copies):
        for copy in copies:
            copy.wait()

    weights = [pltpu.make_async_copy(src, dst, w_sem.at[i]) for i, (src, dst) in enumerate((
        (lwq, wq.at[0]), (lwk, wk.at[0]), (lwv, wv.at[0]), (lwo, wo.at[0]),
        (gwq, wq.at[1]), (gwk, wk.at[1]), (gwv, wv.at[1]), (gwo, wo.at[1])))]

    pump(0)
    for copy in weights:
        copy.start()
    pump(1)

    cosine, sine = trig[0:1, :], trig[1:2, :]

    def rope(heads):
        first, second = heads[:, :HEAD // 2], heads[:, HEAD // 2:]
        return jnp.concatenate([first * cosine - second * sine, second * cosine + first * sine], axis=-1)

    def layer(index, hidden, key_ref, value_ref, pre, post, step):
        normed = norm(hidden, pre[...]).astype(jnp.bfloat16)
        if index == 0:
            for copy in weights[:4]:
                copy.wait()
        else:
            for copy in weights[4:]:
                copy.wait()
        q = jnp.dot(normed, wq[index], preferred_element_type=jnp.float32)
        q = jnp.concatenate([rope(q[:, :HEAD]), rope(q[:, HEAD:])], axis=0).astype(jnp.bfloat16)
        new_k = rope(jnp.dot(normed, wk[index], preferred_element_type=jnp.float32)).astype(jnp.bfloat16)
        new_v = jnp.dot(normed, wv[index], preferred_element_type=jnp.float32).astype(jnp.bfloat16)
        new_kv[2 * index] = new_k
        new_kv[2 * index + 1] = new_v
        own_q = qbuf.at[index]
        own_q[me] = q
        sent = exchange(3 * index, lambda peer: own_q.at[me], own_q)
        pump(step)
        finish(sent)

        def fetch(item, slot):
            h, r = item // ROWS, item % ROWS
            return (pltpu.make_async_copy(key_ref.at[r, h], kvbuf.at[slot, 0], kv_sem.at[slot, 0]),
                    pltpu.make_async_copy(value_ref.at[r, h], kvbuf.at[slot, 1], kv_sem.at[slot, 1]))

        for copy in fetch(0, 0):
            copy.start()
        items = GROUP * ROWS

        def body(item, carry):
            pump(step + 1 + item)
            slot = item % 2
            h, r = item // ROWS, item % ROWS

            @pl.when(item + 1 < items)
            def _():
                for copy in fetch(item + 1, 1 - slot):
                    copy.start()

            copy_k, copy_v = fetch(item, slot)
            copy_k.wait()
            scores = softcap(lax.dot_general(own_q[h], kvbuf[slot, 0], (((1,), (1,)), ((), ())),
                                             preferred_element_type=jnp.float32))
            if index == 0:
                place = me * BLOCK + lax.broadcasted_iota(jnp.int32, scores.shape, 1)
                inside = place > SEQ - WINDOW
                scores = jnp.where(inside, scores, LOW)
            top = jnp.max(scores, axis=-1, keepdims=True)
            e = jnp.exp(scores - top)
            if index == 0:
                e = jnp.where(inside, e, 0.0)
            total = jnp.sum(e, axis=-1, keepdims=True)
            copy_v.wait()
            out = jnp.dot(e.astype(jnp.bfloat16), kvbuf[slot, 1], preferred_element_type=jnp.float32)
            wide = jnp.concatenate([out, jnp.broadcast_to(top, (2 * ROWS, 128)),
                                    jnp.broadcast_to(total, (2 * ROWS, 128))], axis=-1)
            row = lax.broadcasted_iota(jnp.int32, wide.shape, 0) % ROWS
            part[index, h] = jnp.where(row == r, wide, part[index, h])
            return carry

        lax.fori_loop(0, items, body, 0)
        step = step + 1 + items

        sent = exchange(3 * index + 1, lambda peer: part.at[index, peer], precv.at[index])
        precv[index, me] = part[index, me]
        pump(step)
        new_k2 = jnp.concatenate([new_k, new_k], axis=0).astype(jnp.float32)
        new_v2 = jnp.concatenate([new_v, new_v], axis=0).astype(jnp.float32)
        new_s = softcap(jnp.sum(q.astype(jnp.float32) * new_k2, axis=-1, keepdims=True))
        finish(sent)
        top = new_s
        for d in range(GROUP):
            top = jnp.maximum(top, precv[index, d, :, HEAD:HEAD + 1])
        new_e = jnp.exp(new_s - top)
        total = new_e
        acc = new_e.astype(jnp.bfloat16).astype(jnp.float32) * new_v2
        for d in range(GROUP):
            scale = jnp.exp(precv[index, d, :, HEAD:HEAD + 1] - top)
            total = total + scale * precv[index, d, :, HEAD + 128:HEAD + 129]
            acc = acc + scale * precv[index, d, :, :HEAD]
        att = (acc / total).astype(jnp.bfloat16)
        own = jnp.concatenate([att[:ROWS], att[ROWS:]], axis=-1)
        y = jnp.dot(own, wo[index], preferred_element_type=jnp.float32).astype(jnp.bfloat16)
        y_ref = ybuf.at[index]
        y_ref[me] = y
        sent = exchange(3 * index + 2, lambda peer: y_ref.at[me], y_ref)
        pump(step + 1)
        finish(sent)
        summed = y_ref[0].astype(jnp.float32)
        for d in range(1, GROUP):
            summed = summed + y_ref[d].astype(jnp.float32)
        return (hidden + norm(summed, post[...])).astype(jnp.bfloat16), step + 2

    part[...] = jnp.zeros_like(part)
    hidden, step = layer(0, hid[...].astype(jnp.float32), lk, lv, lpre, lpost, 2)
    hidden, step = layer(1, hidden.astype(jnp.float32), gk, gv, gpre, gpost, step)
    hid_out[...] = hidden

    def rest(s, carry):
        pump(s)
        return carry

    lax.fori_loop(step, STEPS, rest, 0)

    for s in range(STEPS - DEPTH, STEPS):
        for k in range(3):
            @pl.when(valid(s, k))
            def _():
                pltpu.make_async_remote_copy(
                    src_ref=gk.at[0, 0, pl.ds(0, UNIT)], dst_ref=land_gk.at[0, 0, pl.ds(0, UNIT)],
                    send_sem=bulk_send.at[k, s % DEPTH], recv_sem=glo_recv.at[0, 0],
                    device_id=(dp, dest[k]), device_id_type=MESH).wait_send()
    for i in range(4):
        for u in range(LOC_UNITS if i < 2 else GLO_UNITS):
            owner = (u if i >= 2 or u >= FIRST_UNIT else u + LOC_UNITS) // PER
            sem = loc_recv.at[i, u] if i < 2 else glo_recv.at[i - 2, u]

            def await_rows(rows):
                view = lands[i].at[pl.ds(0, rows), :, pl.ds(u * UNIT, UNIT)]
                pltpu.make_async_remote_copy(
                    src_ref=view, dst_ref=view, send_sem=bulk_send.at[0, 0], recv_sem=sem,
                    device_id=(dp, dest[0]), device_id_type=MESH).wait_recv()

            if LEFT and i == 3 and owner >= 2:
                short = me == owner - 2

                @pl.when(short)
                def _():
                    await_rows(ROWS - LEFT)

                @pl.when(jnp.logical_and(me != owner, jnp.logical_not(short)))
                def _():
                    await_rows(ROWS)
            else:
                @pl.when(me != owner)
                def _():
                    await_rows(ROWS)


SLOTS = 6


def write_kernel(hid, new_kv, lk, lv, gk, gv, land_lk, land_lv, land_gk, land_gv,
                 hid_out, lk_out, lv_out, gk_out, gv_out, buf, in_sem, out_sem):
    me = lax.axis_index("a")
    hid_out[...] = hid[...]
    jobs = []
    for i in range(4):
        for u in range(LOC_UNITS if i < 2 else GLO_UNITS + 1):
            jobs.append((i, u))
    caches = (lk, lv, gk, gv)
    lands = (land_lk, land_lv, land_gk, land_gv)
    outs = (lk_out, lv_out, gk_out, gv_out)

    def load(n):
        i, u = jobs[n]
        slot = n % SLOTS
        if i >= 2 and u == GLO_UNITS:
            return
        full = u if i >= 2 or u >= FIRST_UNIT else u + LOC_UNITS
        owner, j = full // PER, full % PER

        @pl.when(me == owner)
        def _():
            pltpu.make_async_copy(caches[i].at[:, owner, pl.ds(j * UNIT, UNIT)], buf.at[slot], in_sem.at[slot]).start()

        @pl.when(me != owner)
        def _():
            pltpu.make_async_copy(lands[i].at[:, 0, pl.ds(u * UNIT, UNIT)], buf.at[slot], in_sem.at[slot]).start()

    def store(n):
        i, u = jobs[n]
        slot = n % SLOTS
        return pltpu.make_async_copy(buf.at[slot], outs[i].at[:, 0, pl.ds(u * UNIT, UNIT)], out_sem.at[slot])

    ahead = SLOTS // 2
    for n in range(ahead):
        load(n)
    for n, (i, u) in enumerate(jobs):
        slot = n % SLOTS
        if n + ahead < len(jobs):
            if n + ahead >= SLOTS:
                store(n + ahead - SLOTS).wait()
            load(n + ahead)
        pad = i >= 2 and u == GLO_UNITS
        if not pad:
            pltpu.make_async_copy(lands[i].at[:, 0, pl.ds(0, UNIT)], buf.at[slot], in_sem.at[slot]).wait()
        else:
            buf[slot] = jnp.zeros((ROWS, UNIT, HEAD), jnp.bfloat16)
        if pad or (i < 2 and u == SEQ % WINDOW // UNIT):
            head = buf[slot, :, 0:16, :].astype(jnp.float32)
            first = lax.broadcasted_iota(jnp.int32, head.shape, 1) == 0
            new = jnp.broadcast_to(new_kv[i].astype(jnp.float32)[:, None, :], head.shape)
            buf[slot, :, 0:16, :] = jnp.where(first, new, head).astype(jnp.bfloat16)
        store(n).start()
    for n in range(len(jobs) - SLOTS, len(jobs)):
        store(n).wait()


def trig_table():
    half = HEAD // 2
    inv_freq = ROPE_BASE ** (-2.0 * np.arange(half) / HEAD)
    angles = SEQ * inv_freq
    return np.stack([np.cos(angles), np.sin(angles)]).astype(np.float32)


def solution(mesh):
    cache_in = P('dp', None, 'a', None)
    cache_out = P('dp', 'a', None, None)
    rows_spec = P('dp', None)
    layer_specs = (P(None, 'a'), P(None, 'a'), P(None, 'a'), P('a', None), P(None), P(None))
    in_specs = (rows_spec, cache_in, cache_in, cache_in, cache_in) + layer_specs + layer_specs
    out_specs = (rows_spec, cache_out, cache_out, cache_out, cache_out)
    bf16, f32 = jnp.bfloat16, jnp.float32
    anywhere = pl.BlockSpec(memory_space=pl.ANY)
    vmem = pl.BlockSpec(memory_space=pltpu.VMEM)

    def device_step(hidden_in, loc_k, loc_v, glo_k, glo_v, loc_wq, loc_wk, loc_wv, loc_wo, loc_pre, loc_post, glo_wq, glo_wk, glo_wv, glo_wo, glo_pre, glo_post):
        model = hidden_in.shape[1]
        gains = [g.reshape(1, model) for g in (loc_pre, loc_post, glo_pre, glo_post)]
        loc_land = jax.ShapeDtypeStruct((ROWS, 1, WINDOW, HEAD), bf16)
        glo_land = jax.ShapeDtypeStruct((ROWS, 1, SEQ, HEAD), bf16)
        dma = pltpu.SemaphoreType.DMA
        moved = pl.pallas_call(
            move_kernel,
            out_shape=(loc_land, loc_land, glo_land, glo_land,
                       jax.ShapeDtypeStruct((ROWS, model), bf16), jax.ShapeDtypeStruct((4, ROWS, HEAD), bf16)),
            in_specs=[vmem] * 6 + [anywhere] * 12,
            out_specs=(anywhere,) * 4 + (vmem, vmem),
            scratch_shapes=[
                pltpu.VMEM((2,) + loc_wq.shape, bf16), pltpu.VMEM((2,) + loc_wk.shape, bf16),
                pltpu.VMEM((2,) + loc_wv.shape, bf16), pltpu.VMEM((2,) + loc_wo.shape, bf16),
                pltpu.VMEM((2, 2, BLOCK, HEAD), bf16),
                pltpu.VMEM((2, GROUP, 2 * ROWS, HEAD), bf16),
                pltpu.VMEM((2, GROUP, 2 * ROWS, 2 * HEAD), f32),
                pltpu.VMEM((2, GROUP, 2 * ROWS, 2 * HEAD), f32),
                pltpu.VMEM((2, GROUP, ROWS, model), bf16),
                dma((3, DEPTH)), dma((2, LOC_UNITS)), dma((2, GLO_UNITS)), dma((8,)), dma((2, 2)),
                dma((6, 3)), dma((6, 3))],
            compiler_params=pltpu.CompilerParams(collective_id=0, has_side_effects=True),
        )(hidden_in, jnp.asarray(trig_table()), *gains, loc_k, loc_v, glo_k, glo_v,
          loc_wq, loc_wk, loc_wv, loc_wo, glo_wq, glo_wk, glo_wv, glo_wo)
        land, hid, new_kv = moved[:4], moved[4], moved[5]
        return pl.pallas_call(
            write_kernel,
            out_shape=(jax.ShapeDtypeStruct((ROWS, model), bf16),)
            + (jax.ShapeDtypeStruct((ROWS, 1, WINDOW, HEAD), bf16),) * 2
            + (jax.ShapeDtypeStruct((ROWS, 1, SEQ + CACHE_ROOM, HEAD), bf16),) * 2,
            in_specs=[vmem, vmem] + [anywhere] * 8,
            out_specs=(vmem,) + (anywhere,) * 4,
            scratch_shapes=[pltpu.VMEM((SLOTS, ROWS, UNIT, HEAD), bf16), dma((SLOTS,)), dma((SLOTS,))],
            cost_estimate=pl.CostEstimate(flops=10 ** 9, bytes_accessed=180 * 10 ** 6, transcendentals=0),
        )(hid, new_kv, loc_k, loc_v, glo_k, glo_v, *land)

    return jax.shard_map(device_step, mesh=mesh, in_specs=in_specs, out_specs=out_specs, check_vma=False)
```

```python
import jax
import jax.numpy as jnp
import numpy as np
from jax import lax
from jax.experimental import pallas as pl
from jax.experimental.pallas import tpu as pltpu
from jax.sharding import PartitionSpec as P

SOFTCAP = 50.0
NORM_EPS = 1e-6
ROPE_BASE = 10000.0
WINDOW = 4096
CACHE_ROOM = 512

GROUP = 4
ROWS = 8
BLOCK = 1536
UNIT = 512
HEAD = 256
SEQ = GROUP * BLOCK
PER = BLOCK // UNIT
GLO_UNITS = SEQ // UNIT
LOC_UNITS = WINDOW // UNIT
FIRST_UNIT = (SEQ - WINDOW) // UNIT
STEPS = 4 * ROWS * PER
DEPTH = 2
LEFT = 4
MESH = pl.DeviceIdType.MESH
LOW = -1e30


def peers(me):
    return (me + 1 - 2 * (me % 2), (me + 2) % 4, 3 - me)


def norm(hidden, gain):
    mean_sq = jnp.mean(hidden * hidden, axis=-1, keepdims=True)
    return hidden * lax.rsqrt(mean_sq + NORM_EPS) * (1.0 + gain.astype(jnp.float32).reshape(1, -1))


def softcap(scores):
    return SOFTCAP * jnp.tanh(scores * (HEAD ** -0.5) / SOFTCAP)


def move_kernel(hid, trig, lpre, lpost, gpre, gpost, lk, lv, gk, gv, lwq, lwk, lwv, lwo, gwq, gwk, gwv, gwo,
                land_lk, land_lv, land_gk, land_gv, hid_out, new_kv, later,
                wq, wk, wv, wo, kvbuf, qbuf, part, precv, ybuf,
                bulk_send, loc_recv, glo_recv, w_sem, kv_sem, ex_send, ex_recv, late_sem):
    dp = lax.axis_index("dp")
    me = lax.axis_index("a")
    dest = peers(me)
    caches = (lk, lv, gk, gv)
    lands = (land_lk, land_lv, land_gk, land_gv)

    barrier = pltpu.get_barrier_semaphore()
    for peer in dest:
        pl.semaphore_signal(barrier, inc=1, device_id=(dp, peer), device_id_type=MESH)
    pl.semaphore_wait(barrier, 3)

    def coords(step):
        c = (step // (ROWS * PER) + 2 - 2 * (me // 2)) % 4
        return c, (step // PER) % ROWS, step % PER

    def valid(step, k):
        c, r, j = coords(step)
        in_window = jnp.logical_or(c >= 2, PER * me + j >= FIRST_UNIT)
        ok = jnp.logical_and(step >= 0, in_window)
        if k == 1 and LEFT:
            late = jnp.logical_and(jnp.logical_and(c == 3, r >= ROWS - LEFT), me >= 2)
            ok = jnp.logical_and(ok, jnp.logical_not(late))
        return ok

    def pump(step):
        c, r, j = coords(step)
        slot = step % DEPTH
        for k in range(3):
            @pl.when(valid(step - DEPTH, k))
            def _():
                pltpu.make_async_remote_copy(
                    src_ref=gk.at[0, 0, pl.ds(0, UNIT)], dst_ref=land_gk.at[0, 0, pl.ds(0, UNIT)],
                    send_sem=bulk_send.at[k, slot], recv_sem=glo_recv.at[0, 0],
                    device_id=(dp, dest[k]), device_id_type=MESH).wait_send()
        unit = PER * me + j
        for i in range(4):
            place = unit % LOC_UNITS if i < 2 else unit
            sem = loc_recv.at[i, place] if i < 2 else glo_recv.at[i - 2, place]
            for k in range(3):
                @pl.when(jnp.logical_and(c == i, valid(step, k)))
                def _():
                    pltpu.make_async_remote_copy(
                        src_ref=caches[i].at[r, dest[k], pl.ds(pl.multiple_of(j * UNIT, UNIT), UNIT)],
                        dst_ref=lands[i].at[r, 0, pl.ds(pl.multiple_of(place * UNIT, UNIT), UNIT)],
                        send_sem=bulk_send.at[k, slot], recv_sem=sem,
                        device_id=(dp, dest[k]), device_id_type=MESH).start()

    def exchange(index, src_of, dst):
        copies = []
        for k in range(3):
            copies.append(pltpu.make_async_remote_copy(
                src_ref=src_of(dest[k]), dst_ref=dst.at[me], send_sem=ex_send.at[index, k], recv_sem=ex_recv.at[index, k],
                device_id=(dp, dest[k]), device_id_type=MESH))
        for copy in copies:
            copy.start()
        return copies

    def finish(copies):
        for copy in copies:
            copy.wait()

    weights = [pltpu.make_async_copy(src, dst, w_sem.at[i]) for i, (src, dst) in enumerate((
        (lwq, wq.at[0]), (lwk, wk.at[0]), (lwv, wv.at[0]), (lwo, wo.at[0]),
        (gwq, wq.at[1]), (gwk, wk.at[1]), (gwv, wv.at[1]), (gwo, wo.at[1])))]

    pump(0)
    for copy in weights:
        copy.start()
    pump(1)

    cosine, sine = trig[0:1, :], trig[1:2, :]

    def rope(heads):
        first, second = heads[:, :HEAD // 2], heads[:, HEAD // 2:]
        return jnp.concatenate([first * cosine - second * sine, second * cosine + first * sine], axis=-1)

    def layer(index, hidden, key_ref, value_ref, pre, post, step):
        normed = norm(hidden, pre[...]).astype(jnp.bfloat16)
        if index == 0:
            for copy in weights[:4]:
                copy.wait()
        else:
            for copy in weights[4:]:
                copy.wait()
        q = jnp.dot(normed, wq[index], preferred_element_type=jnp.float32)
        q = jnp.concatenate([rope(q[:, :HEAD]), rope(q[:, HEAD:])], axis=0).astype(jnp.bfloat16)
        new_k = rope(jnp.dot(normed, wk[index], preferred_element_type=jnp.float32)).astype(jnp.bfloat16)
        new_v = jnp.dot(normed, wv[index], preferred_element_type=jnp.float32).astype(jnp.bfloat16)
        new_kv[2 * index] = new_k
        new_kv[2 * index + 1] = new_v
        own_q = qbuf.at[index]
        own_q[me] = q
        sent = exchange(3 * index, lambda peer: own_q.at[me], own_q)
        pump(step)
        finish(sent)

        def fetch(item, slot):
            h, r = item // ROWS, item % ROWS
            return (pltpu.make_async_copy(key_ref.at[r, h], kvbuf.at[slot, 0], kv_sem.at[slot, 0]),
                    pltpu.make_async_copy(value_ref.at[r, h], kvbuf.at[slot, 1], kv_sem.at[slot, 1]))

        for copy in fetch(0, 0):
            copy.start()
        items = GROUP * ROWS

        def body(item, carry):
            pump(step + 1 + item)
            slot = item % 2
            h, r = item // ROWS, item % ROWS

            @pl.when(item + 1 < items)
            def _():
                for copy in fetch(item + 1, 1 - slot):
                    copy.start()

            copy_k, copy_v = fetch(item, slot)
            copy_k.wait()
            scores = softcap(lax.dot_general(own_q[h], kvbuf[slot, 0], (((1,), (1,)), ((), ())),
                                             preferred_element_type=jnp.float32))
            if index == 0:
                place = me * BLOCK + lax.broadcasted_iota(jnp.int32, scores.shape, 1)
                inside = place > SEQ - WINDOW
                scores = jnp.where(inside, scores, LOW)
            top = jnp.max(scores, axis=-1, keepdims=True)
            e = jnp.exp(scores - top)
            if index == 0:
                e = jnp.where(inside, e, 0.0)
            total = jnp.sum(e, axis=-1, keepdims=True)
            copy_v.wait()
            out = jnp.dot(e.astype(jnp.bfloat16), kvbuf[slot, 1], preferred_element_type=jnp.float32)
            wide = jnp.concatenate([out, jnp.broadcast_to(top, (2 * ROWS, 128)),
                                    jnp.broadcast_to(total, (2 * ROWS, 128))], axis=-1)
            row = lax.broadcasted_iota(jnp.int32, wide.shape, 0) % ROWS
            part[index, h] = jnp.where(row == r, wide, part[index, h])
            return carry

        lax.fori_loop(0, items, body, 0)
        step = step + 1 + items

        sent = exchange(3 * index + 1, lambda peer: part.at[index, peer], precv.at[index])
        precv[index, me] = part[index, me]
        pump(step)
        new_k2 = jnp.concatenate([new_k, new_k], axis=0).astype(jnp.float32)
        new_v2 = jnp.concatenate([new_v, new_v], axis=0).astype(jnp.float32)
        new_s = softcap(jnp.sum(q.astype(jnp.float32) * new_k2, axis=-1, keepdims=True))
        finish(sent)
        top = new_s
        for d in range(GROUP):
            top = jnp.maximum(top, precv[index, d, :, HEAD:HEAD + 1])
        new_e = jnp.exp(new_s - top)
        total = new_e
        acc = new_e.astype(jnp.bfloat16).astype(jnp.float32) * new_v2
        for d in range(GROUP):
            scale = jnp.exp(precv[index, d, :, HEAD:HEAD + 1] - top)
            total = total + scale * precv[index, d, :, HEAD + 128:HEAD + 129]
            acc = acc + scale * precv[index, d, :, :HEAD]
        att = (acc / total).astype(jnp.bfloat16)
        own = jnp.concatenate([att[:ROWS], att[ROWS:]], axis=-1)
        y = jnp.dot(own, wo[index], preferred_element_type=jnp.float32).astype(jnp.bfloat16)
        y_ref = ybuf.at[index]
        y_ref[me] = y
        sent = exchange(3 * index + 2, lambda peer: y_ref.at[me], y_ref)
        pump(step + 1)
        finish(sent)
        summed = y_ref[0].astype(jnp.float32)
        for d in range(1, GROUP):
            summed = summed + y_ref[d].astype(jnp.float32)
        return (hidden + norm(summed, post[...])).astype(jnp.bfloat16), step + 2

    part[...] = jnp.zeros_like(part)
    hidden, step = layer(0, hid[...].astype(jnp.float32), lk, lv, lpre, lpost, 2)
    hidden, step = layer(1, hidden.astype(jnp.float32), gk, gv, gpre, gpost, step)
    hid_out[...] = hidden

    def late_in(r):
        return pltpu.make_async_copy(gv.at[ROWS - LEFT + r, dest[1]], kvbuf.at[r // 2, r % 2], late_sem.at[0, r])

    def late_out(r):
        return pltpu.make_async_copy(kvbuf.at[r // 2, r % 2], later.at[r], late_sem.at[1, r])

    for r in range(LEFT):
        late_in(r).start()
    for r in range(LEFT):
        late_in(r).wait()
        late_out(r).start()
    for r in range(LEFT):
        late_out(r).wait()

    def rest(s, carry):
        pump(s)
        return carry

    lax.fori_loop(step, STEPS, rest, 0)

    for s in range(STEPS - DEPTH, STEPS):
        for k in range(3):
            @pl.when(valid(s, k))
            def _():
                pltpu.make_async_remote_copy(
                    src_ref=gk.at[0, 0, pl.ds(0, UNIT)], dst_ref=land_gk.at[0, 0, pl.ds(0, UNIT)],
                    send_sem=bulk_send.at[k, s % DEPTH], recv_sem=glo_recv.at[0, 0],
                    device_id=(dp, dest[k]), device_id_type=MESH).wait_send()
    for i in range(4):
        for u in range(LOC_UNITS if i < 2 else GLO_UNITS):
            owner = (u if i >= 2 or u >= FIRST_UNIT else u + LOC_UNITS) // PER
            sem = loc_recv.at[i, u] if i < 2 else glo_recv.at[i - 2, u]

            def await_rows(rows):
                view = lands[i].at[pl.ds(0, rows), :, pl.ds(u * UNIT, UNIT)]
                pltpu.make_async_remote_copy(
                    src_ref=view, dst_ref=view, send_sem=bulk_send.at[0, 0], recv_sem=sem,
                    device_id=(dp, dest[0]), device_id_type=MESH).wait_recv()

            if LEFT and i == 3 and owner >= 2:
                short = me == owner - 2

                @pl.when(short)
                def _():
                    await_rows(ROWS - LEFT)

                @pl.when(jnp.logical_and(me != owner, jnp.logical_not(short)))
                def _():
                    await_rows(ROWS)
            else:
                @pl.when(me != owner)
                def _():
                    await_rows(ROWS)


SLOTS = 6


def write_kernel(hid, new_kv, lk, lv, gk, gv, land_lk, land_lv, land_gk, land_gv,
                 hid_out, lk_out, lv_out, gk_out, gv_out, buf, in_sem, out_sem):
    me = lax.axis_index("a")
    hid_out[...] = hid[...]
    jobs = []
    for i in range(4):
        for u in range(LOC_UNITS if i < 2 else GLO_UNITS + 1):
            jobs.append((i, u))
    caches = (lk, lv, gk, gv)
    lands = (land_lk, land_lv, land_gk, land_gv)
    outs = (lk_out, lv_out, gk_out, gv_out)

    def load(n):
        i, u = jobs[n]
        slot = n % SLOTS
        if i >= 2 and u == GLO_UNITS:
            return
        full = u if i >= 2 or u >= FIRST_UNIT else u + LOC_UNITS
        owner, j = full // PER, full % PER

        @pl.when(me == owner)
        def _():
            pltpu.make_async_copy(caches[i].at[:, owner, pl.ds(j * UNIT, UNIT)], buf.at[slot], in_sem.at[slot]).start()

        @pl.when(me != owner)
        def _():
            pltpu.make_async_copy(lands[i].at[:, 0, pl.ds(u * UNIT, UNIT)], buf.at[slot], in_sem.at[slot]).start()

    def store(n):
        i, u = jobs[n]
        slot = n % SLOTS
        return pltpu.make_async_copy(buf.at[slot], outs[i].at[:, 0, pl.ds(u * UNIT, UNIT)], out_sem.at[slot])

    ahead = SLOTS // 2
    for n in range(ahead):
        load(n)
    for n, (i, u) in enumerate(jobs):
        slot = n % SLOTS
        if n + ahead < len(jobs):
            if n + ahead >= SLOTS:
                store(n + ahead - SLOTS).wait()
            load(n + ahead)
        pad = i >= 2 and u == GLO_UNITS
        if not pad:
            pltpu.make_async_copy(lands[i].at[:, 0, pl.ds(0, UNIT)], buf.at[slot], in_sem.at[slot]).wait()
        else:
            buf[slot] = jnp.zeros((ROWS, UNIT, HEAD), jnp.bfloat16)
        if pad or (i < 2 and u == SEQ % WINDOW // UNIT):
            head = buf[slot, :, 0:16, :].astype(jnp.float32)
            first = lax.broadcasted_iota(jnp.int32, head.shape, 1) == 0
            new = jnp.broadcast_to(new_kv[i].astype(jnp.float32)[:, None, :], head.shape)
            buf[slot, :, 0:16, :] = jnp.where(first, new, head).astype(jnp.bfloat16)
        store(n).start()
    for n in range(len(jobs) - SLOTS, len(jobs)):
        store(n).wait()


def late_kernel(late, old, out, sem):
    me = lax.axis_index("a")

    @pl.when(me < 2)
    def _():
        place = pl.multiple_of((me + 2) * BLOCK, BLOCK)
        copy = pltpu.make_async_copy(late, out.at[pl.ds(ROWS - LEFT, LEFT), 0, pl.ds(place, BLOCK)], sem)
        copy.start()
        copy.wait()


def trig_table():
    half = HEAD // 2
    inv_freq = ROPE_BASE ** (-2.0 * np.arange(half) / HEAD)
    angles = SEQ * inv_freq
    return np.stack([np.cos(angles), np.sin(angles)]).astype(np.float32)


def solution(mesh):
    cache_in = P('dp', None, 'a', None)
    cache_out = P('dp', 'a', None, None)
    rows_spec = P('dp', None)
    layer_specs = (P(None, 'a'), P(None, 'a'), P(None, 'a'), P('a', None), P(None), P(None))
    in_specs = (rows_spec, cache_in, cache_in, cache_in, cache_in) + layer_specs + layer_specs
    out_specs = (rows_spec, cache_out, cache_out, cache_out, cache_out)
    bf16, f32 = jnp.bfloat16, jnp.float32
    anywhere = pl.BlockSpec(memory_space=pl.ANY)
    vmem = pl.BlockSpec(memory_space=pltpu.VMEM)

    def device_step(hidden_in, loc_k, loc_v, glo_k, glo_v, loc_wq, loc_wk, loc_wv, loc_wo, loc_pre, loc_post, glo_wq, glo_wk, glo_wv, glo_wo, glo_pre, glo_post):
        model = hidden_in.shape[1]
        gains = [loc_pre, loc_post, glo_pre, glo_post]
        loc_land = jax.ShapeDtypeStruct((ROWS, 1, WINDOW, HEAD), bf16)
        glo_land = jax.ShapeDtypeStruct((ROWS, 1, SEQ, HEAD), bf16)
        dma = pltpu.SemaphoreType.DMA
        moved = pl.pallas_call(
            move_kernel,
            out_shape=(loc_land, loc_land, glo_land, glo_land,
                       jax.ShapeDtypeStruct((ROWS, model), bf16), jax.ShapeDtypeStruct((4, ROWS, HEAD), bf16),
                       jax.ShapeDtypeStruct((LEFT, BLOCK, HEAD), bf16)),
            in_specs=[vmem] * 6 + [anywhere] * 12,
            out_specs=(anywhere,) * 4 + (vmem, vmem, anywhere),
            scratch_shapes=[
                pltpu.VMEM((2,) + loc_wq.shape, bf16), pltpu.VMEM((2,) + loc_wk.shape, bf16),
                pltpu.VMEM((2,) + loc_wv.shape, bf16), pltpu.VMEM((2,) + loc_wo.shape, bf16),
                pltpu.VMEM((2, 2, BLOCK, HEAD), bf16),
                pltpu.VMEM((2, GROUP, 2 * ROWS, HEAD), bf16),
                pltpu.VMEM((2, GROUP, 2 * ROWS, 2 * HEAD), f32),
                pltpu.VMEM((2, GROUP, 2 * ROWS, 2 * HEAD), f32),
                pltpu.VMEM((2, GROUP, ROWS, model), bf16),
                dma((3, DEPTH)), dma((2, LOC_UNITS)), dma((2, GLO_UNITS)), dma((8,)), dma((2, 2)),
                dma((6, 3)), dma((6, 3)), dma((2, LEFT))],
            compiler_params=pltpu.CompilerParams(collective_id=0, has_side_effects=True),
        )(hidden_in, jnp.asarray(trig_table()), *gains, loc_k, loc_v, glo_k, glo_v,
          loc_wq, loc_wk, loc_wv, loc_wo, glo_wq, glo_wk, glo_wv, glo_wo)
        land, hid, new_kv, later = moved[:4], moved[4], moved[5], moved[6]
        late = lax.ppermute(later, 'a', [(2, 0), (3, 1)])
        hidden_out, loc_k_out, loc_v_out, glo_k_out, glo_v_out = pl.pallas_call(
            write_kernel,
            out_shape=(jax.ShapeDtypeStruct((ROWS, model), bf16),)
            + (jax.ShapeDtypeStruct((ROWS, 1, WINDOW, HEAD), bf16),) * 2
            + (jax.ShapeDtypeStruct((ROWS, 1, SEQ + CACHE_ROOM, HEAD), bf16),) * 2,
            in_specs=[vmem, vmem] + [anywhere] * 8,
            out_specs=(vmem,) + (anywhere,) * 4,
            scratch_shapes=[pltpu.VMEM((SLOTS, ROWS, UNIT, HEAD), bf16), dma((SLOTS,)), dma((SLOTS,))],
            cost_estimate=pl.CostEstimate(flops=10 ** 9, bytes_accessed=180 * 10 ** 6, transcendentals=0),
        )(hid, new_kv, loc_k, loc_v, glo_k, glo_v, *land)
        glo_v_out = pl.pallas_call(
            late_kernel,
            out_shape=jax.ShapeDtypeStruct(glo_v_out.shape, bf16),
            in_specs=[vmem, anywhere],
            out_specs=anywhere,
            scratch_shapes=[dma],
            input_output_aliases={1: 0},
            compiler_params=pltpu.CompilerParams(vmem_limit_bytes=8 * 2 ** 20),
            cost_estimate=pl.CostEstimate(flops=10 ** 7, bytes_accessed=4 * late.size, transcendentals=0),
        )(late, glo_v_out)
        return hidden_out, loc_k_out, loc_v_out, glo_k_out, glo_v_out

    return jax.shard_map(device_step, mesh=mesh, in_specs=in_specs, out_specs=out_specs, check_vma=False)
```

```python
import jax
import jax.numpy as jnp
import numpy as np
from jax import lax
from jax.experimental import pallas as pl
from jax.experimental.pallas import tpu as pltpu
from jax.sharding import PartitionSpec as P

SOFTCAP = 50.0
NORM_EPS = 1e-6
ROPE_BASE = 10000.0
WINDOW = 4096
CACHE_ROOM = 512

GROUP = 4
ROWS = 8
BLOCK = 1536
UNIT = 512
HEAD = 256
SEQ = GROUP * BLOCK
PER = BLOCK // UNIT
GLO_UNITS = SEQ // UNIT
LOC_UNITS = WINDOW // UNIT
FIRST_UNIT = (SEQ - WINDOW) // UNIT
STEPS = 4 * ROWS * PER
DEPTH = 2
LATE = (5, 4)
MESH = pl.DeviceIdType.MESH
LOW = -1e30


def peers(me):
    return (me + 1 - 2 * (me % 2), (me + 2) % 4, 3 - me)


def norm(hidden, gain):
    mean_sq = jnp.mean(hidden * hidden, axis=-1, keepdims=True)
    return hidden * lax.rsqrt(mean_sq + NORM_EPS) * (1.0 + gain.astype(jnp.float32).reshape(1, -1))


def softcap(scores):
    return SOFTCAP * jnp.tanh(scores * (HEAD ** -0.5) / SOFTCAP)


def move_kernel(hid_in, trig_in, lpre_in, lpost_in, gpre_in, gpost_in, lk, lv, gk, gv, lwq, lwk, lwv, lwo, gwq, gwk, gwv, gwo,
                land_lk, land_lv, land_gk, land_gv, hid_out, new_out, late_a, late_b,
                hid, trig, lpre, lpost, gpre, gpost, new_kv, hid_end, wq, wk, wv, wo, kvbuf, qbuf, part, precv, ybuf,
                bulk_send, loc_recv, glo_recv, w_sem, kv_sem, ex_send, ex_recv, late_sem, tail_send, small_sem, out_sem):
    dp = lax.axis_index("dp")
    me = lax.axis_index("a")
    dest = peers(me)
    caches = (lk, lv, gk, gv)
    lands = (land_lk, land_lv, land_gk, land_gv)

    barrier = pltpu.get_barrier_semaphore()
    for peer in dest:
        pl.semaphore_signal(barrier, inc=1, device_id=(dp, peer), device_id_type=MESH)
    pl.semaphore_wait(barrier, 3)

    def coords(step):
        c = (step // (ROWS * PER) + 2 - 2 * (me // 2)) % 4
        return c, (step // PER) % ROWS, step % PER

    def valid(step, k):
        c, r, j = coords(step)
        in_window = jnp.logical_or(c >= 2, PER * me + j >= FIRST_UNIT)
        ok = jnp.logical_and(step >= 0, in_window)
        if k == 1:
            late = jnp.logical_and(jnp.logical_and(c == 3, r >= ROWS - LATE[0]), me >= 2)
            ok = jnp.logical_and(ok, jnp.logical_not(late))
        return ok

    def pump(step):
        c, r, j = coords(step)
        slot = step % DEPTH
        for k in range(3):
            @pl.when(valid(step - DEPTH, k))
            def _():
                pltpu.make_async_remote_copy(
                    src_ref=gk.at[0, 0, pl.ds(0, UNIT)], dst_ref=land_gk.at[0, 0, pl.ds(0, UNIT)],
                    send_sem=bulk_send.at[k, slot], recv_sem=glo_recv.at[0, 0],
                    device_id=(dp, dest[k]), device_id_type=MESH).wait_send()
        unit = PER * me + j
        for i in range(4):
            place = unit % LOC_UNITS if i < 2 else unit
            sem = loc_recv.at[i, place] if i < 2 else glo_recv.at[i - 2, place]
            for k in range(3):
                @pl.when(jnp.logical_and(c == i, valid(step, k)))
                def _():
                    pltpu.make_async_remote_copy(
                        src_ref=caches[i].at[r, dest[k], pl.ds(pl.multiple_of(j * UNIT, UNIT), UNIT)],
                        dst_ref=lands[i].at[r, 0, pl.ds(pl.multiple_of(place * UNIT, UNIT), UNIT)],
                        send_sem=bulk_send.at[k, slot], recv_sem=sem,
                        device_id=(dp, dest[k]), device_id_type=MESH).start()

    def exchange(index, src_of, dst):
        copies = []
        for k in range(3):
            copies.append(pltpu.make_async_remote_copy(
                src_ref=src_of(dest[k]), dst_ref=dst.at[me], send_sem=ex_send.at[index, k], recv_sem=ex_recv.at[index, k],
                device_id=(dp, dest[k]), device_id_type=MESH))
        for copy in copies:
            copy.start()
        return copies

    def finish(copies):
        for copy in copies:
            copy.wait()

    weights = [pltpu.make_async_copy(src, dst, w_sem.at[i]) for i, (src, dst) in enumerate((
        (lwq, wq.at[0]), (lwk, wk.at[0]), (lwv, wv.at[0]), (lwo, wo.at[0]),
        (gwq, wq.at[1]), (gwk, wk.at[1]), (gwv, wv.at[1]), (gwo, wo.at[1])))]

    small = [pltpu.make_async_copy(src, dst, small_sem.at[i]) for i, (src, dst) in enumerate((
        (hid_in, hid), (trig_in, trig), (lpre_in, lpre), (lpost_in, lpost),
        (gpre_in, gpre), (gpost_in, gpost)))]

    pump(0)
    pump(1)
    for copy in small + weights:
        copy.start()
    for copy in small:
        copy.wait()

    cosine, sine = trig[0:1, :], trig[1:2, :]

    def rope(heads):
        first, second = heads[:, :HEAD // 2], heads[:, HEAD // 2:]
        return jnp.concatenate([first * cosine - second * sine, second * cosine + first * sine], axis=-1)

    def layer(index, hidden, key_ref, value_ref, pre, post, step):
        normed = norm(hidden, pre[...]).astype(jnp.bfloat16)
        if index == 0:
            for copy in weights[:4]:
                copy.wait()
        else:
            for copy in weights[4:]:
                copy.wait()
        q = jnp.dot(normed, wq[index], preferred_element_type=jnp.float32)
        q = jnp.concatenate([rope(q[:, :HEAD]), rope(q[:, HEAD:])], axis=0).astype(jnp.bfloat16)
        new_k = rope(jnp.dot(normed, wk[index], preferred_element_type=jnp.float32)).astype(jnp.bfloat16)
        new_v = jnp.dot(normed, wv[index], preferred_element_type=jnp.float32).astype(jnp.bfloat16)
        new_kv[2 * index] = new_k
        new_kv[2 * index + 1] = new_v
        own_q = qbuf.at[index]
        own_q[me] = q
        sent = exchange(3 * index, lambda peer: own_q.at[me], own_q)
        pump(step)
        finish(sent)

        def fetch(item, slot):
            h, r = item // ROWS, item % ROWS
            return (pltpu.make_async_copy(key_ref.at[r, h], kvbuf.at[slot, 0], kv_sem.at[slot, 0]),
                    pltpu.make_async_copy(value_ref.at[r, h], kvbuf.at[slot, 1], kv_sem.at[slot, 1]))

        for copy in fetch(0, 0):
            copy.start()
        items = GROUP * ROWS

        def body(item, carry):
            pump(step + 1 + item)
            slot = item % 2
            h, r = item // ROWS, item % ROWS

            @pl.when(item + 1 < items)
            def _():
                for copy in fetch(item + 1, 1 - slot):
                    copy.start()

            copy_k, copy_v = fetch(item, slot)
            copy_k.wait()
            scores = softcap(lax.dot_general(own_q[h], kvbuf[slot, 0], (((1,), (1,)), ((), ())),
                                             preferred_element_type=jnp.float32))
            if index == 0:
                place = me * BLOCK + lax.broadcasted_iota(jnp.int32, scores.shape, 1)
                inside = place > SEQ - WINDOW
                scores = jnp.where(inside, scores, LOW)
            top = jnp.max(scores, axis=-1, keepdims=True)
            e = jnp.exp(scores - top)
            if index == 0:
                e = jnp.where(inside, e, 0.0)
            total = jnp.sum(e, axis=-1, keepdims=True)
            copy_v.wait()
            out = jnp.dot(e.astype(jnp.bfloat16), kvbuf[slot, 1], preferred_element_type=jnp.float32)
            wide = jnp.concatenate([out, jnp.broadcast_to(top, (2 * ROWS, 128)),
                                    jnp.broadcast_to(total, (2 * ROWS, 128))], axis=-1)
            row = lax.broadcasted_iota(jnp.int32, wide.shape, 0) % ROWS
            part[index, h] = jnp.where(row == r, wide, part[index, h])
            return carry

        lax.fori_loop(0, items, body, 0)
        step = step + 1 + items

        sent = exchange(3 * index + 1, lambda peer: part.at[index, peer], precv.at[index])
        precv[index, me] = part[index, me]
        pump(step)
        new_k2 = jnp.concatenate([new_k, new_k], axis=0).astype(jnp.float32)
        new_v2 = jnp.concatenate([new_v, new_v], axis=0).astype(jnp.float32)
        new_s = softcap(jnp.sum(q.astype(jnp.float32) * new_k2, axis=-1, keepdims=True))
        finish(sent)
        top = new_s
        for d in range(GROUP):
            top = jnp.maximum(top, precv[index, d, :, HEAD:HEAD + 1])
        new_e = jnp.exp(new_s - top)
        total = new_e
        acc = new_e.astype(jnp.bfloat16).astype(jnp.float32) * new_v2
        for d in range(GROUP):
            scale = jnp.exp(precv[index, d, :, HEAD:HEAD + 1] - top)
            total = total + scale * precv[index, d, :, HEAD + 128:HEAD + 129]
            acc = acc + scale * precv[index, d, :, :HEAD]
        att = (acc / total).astype(jnp.bfloat16)
        own = jnp.concatenate([att[:ROWS], att[ROWS:]], axis=-1)
        y = jnp.dot(own, wo[index], preferred_element_type=jnp.float32).astype(jnp.bfloat16)
        y_ref = ybuf.at[index]
        y_ref[me] = y
        sent = exchange(3 * index + 2, lambda peer: y_ref.at[me], y_ref)
        pump(step + 1)
        finish(sent)
        summed = y_ref[0].astype(jnp.float32)
        for d in range(1, GROUP):
            summed = summed + y_ref[d].astype(jnp.float32)
        return (hidden + norm(summed, post[...])).astype(jnp.bfloat16), step + 2

    part[...] = jnp.zeros_like(part)
    hidden, step = layer(0, hid[...].astype(jnp.float32), lk, lv, lpre, lpost, 2)
    hidden, step = layer(1, hidden.astype(jnp.float32), gk, gv, gpre, gpost, step)
    hid_end[...] = hidden
    outs = (pltpu.make_async_copy(hid_end, hid_out, out_sem.at[0]), pltpu.make_async_copy(new_kv, new_out, out_sem.at[1]))
    for copy in outs:
        copy.start()
    for copy in outs:
        copy.wait()

    for late, target, rows in ((late_a, 0, LATE[0]), (late_b, 1, LATE[1])):
        @pl.when(me == target + 2)
        def _():
            def late_in(r):
                return pltpu.make_async_copy(gv.at[ROWS - rows + r, target], kvbuf.at[(r // 2) % 2, r % 2], late_sem.at[0, r])

            def late_out(r):
                return pltpu.make_async_copy(kvbuf.at[(r // 2) % 2, r % 2], late.at[r], late_sem.at[1, r])

            for r in range(rows):
                if r >= 4:
                    late_out(r - 4).wait()
                late_in(r).start()
                if r >= 1:
                    late_in(r - 1).wait()
                    late_out(r - 1).start()
            late_in(rows - 1).wait()
            late_out(rows - 1).start()
            for r in range(max(rows - 4, 0), rows):
                late_out(r).wait()

    def rest(s, carry):
        pump(s)
        return carry

    lax.fori_loop(step, STEPS, rest, 0)

    def tail(r, j):
        unit = PER * me + j
        return pltpu.make_async_remote_copy(
            src_ref=gv.at[r, dest[1], pl.ds(j * UNIT, UNIT)],
            dst_ref=land_gv.at[r, 0, pl.ds(pl.multiple_of(unit * UNIT, UNIT), UNIT)],
            send_sem=tail_send.at[r - ROWS + LATE[0], j], recv_sem=glo_recv.at[1, unit],
            device_id=(dp, dest[1]), device_id_type=MESH)

    tails = [(r, j) for r in range(ROWS - LATE[0], ROWS - LATE[1]) for j in range(PER)]

    @pl.when(me == 3)
    def _():
        for piece in tails:
            tail(*piece).start()

    for s in range(STEPS - DEPTH, STEPS):
        for k in range(3):
            @pl.when(valid(s, k))
            def _():
                pltpu.make_async_remote_copy(
                    src_ref=gk.at[0, 0, pl.ds(0, UNIT)], dst_ref=land_gk.at[0, 0, pl.ds(0, UNIT)],
                    send_sem=bulk_send.at[k, s % DEPTH], recv_sem=glo_recv.at[0, 0],
                    device_id=(dp, dest[k]), device_id_type=MESH).wait_send()

    @pl.when(me == 3)
    def _():
        for piece in tails:
            tail(*piece).wait_send()

    for i in range(4):
        for u in range(LOC_UNITS if i < 2 else GLO_UNITS):
            owner = (u if i >= 2 or u >= FIRST_UNIT else u + LOC_UNITS) // PER
            sem = loc_recv.at[i, u] if i < 2 else glo_recv.at[i - 2, u]

            def await_rows(rows):
                view = lands[i].at[pl.ds(0, rows), :, pl.ds(u * UNIT, UNIT)]
                pltpu.make_async_remote_copy(
                    src_ref=view, dst_ref=view, send_sem=bulk_send.at[0, 0], recv_sem=sem,
                    device_id=(dp, dest[0]), device_id_type=MESH).wait_recv()

            if i == 3 and owner >= 2:
                short = me == owner - 2

                @pl.when(short)
                def _():
                    await_rows(ROWS - LATE[owner - 2])

                @pl.when(jnp.logical_and(me != owner, jnp.logical_not(short)))
                def _():
                    await_rows(ROWS)
            else:
                @pl.when(me != owner)
                def _():
                    await_rows(ROWS)


SLOTS = 6


def write_kernel(hid, new_kv, lk, lv, gk, gv, land_lk, land_lv, land_gk, land_gv,
                 hid_out, lk_out, lv_out, gk_out, gv_out, buf, in_sem, out_sem):
    me = lax.axis_index("a")
    hid_out[...] = hid[...]
    jobs = []
    for i in range(4):
        for u in range(LOC_UNITS if i < 2 else GLO_UNITS + 1):
            jobs.append((i, u))
    caches = (lk, lv, gk, gv)
    lands = (land_lk, land_lv, land_gk, land_gv)
    outs = (lk_out, lv_out, gk_out, gv_out)

    def load(n):
        i, u = jobs[n]
        slot = n % SLOTS
        if i >= 2 and u == GLO_UNITS:
            return
        full = u if i >= 2 or u >= FIRST_UNIT else u + LOC_UNITS
        owner, j = full // PER, full % PER

        @pl.when(me == owner)
        def _():
            pltpu.make_async_copy(caches[i].at[:, owner, pl.ds(j * UNIT, UNIT)], buf.at[slot], in_sem.at[slot]).start()

        @pl.when(me != owner)
        def _():
            pltpu.make_async_copy(lands[i].at[:, 0, pl.ds(u * UNIT, UNIT)], buf.at[slot], in_sem.at[slot]).start()

    def store(n):
        i, u = jobs[n]
        slot = n % SLOTS
        return pltpu.make_async_copy(buf.at[slot], outs[i].at[:, 0, pl.ds(u * UNIT, UNIT)], out_sem.at[slot])

    ahead = SLOTS // 2
    for n in range(ahead):
        load(n)
    for n, (i, u) in enumerate(jobs):
        slot = n % SLOTS
        if n + ahead < len(jobs):
            if n + ahead >= SLOTS:
                store(n + ahead - SLOTS).wait()
            load(n + ahead)
        pad = i >= 2 and u == GLO_UNITS
        if not pad:
            pltpu.make_async_copy(lands[i].at[:, 0, pl.ds(0, UNIT)], buf.at[slot], in_sem.at[slot]).wait()
        else:
            buf[slot] = jnp.zeros((ROWS, UNIT, HEAD), jnp.bfloat16)
        if pad or (i < 2 and u == SEQ % WINDOW // UNIT):
            head = buf[slot, :, 0:16, :].astype(jnp.float32)
            first = lax.broadcasted_iota(jnp.int32, head.shape, 1) == 0
            new = jnp.broadcast_to(new_kv[i].astype(jnp.float32)[:, None, :], head.shape)
            buf[slot, :, 0:16, :] = jnp.where(first, new, head).astype(jnp.bfloat16)
        store(n).start()
    for n in range(len(jobs) - SLOTS, len(jobs)):
        store(n).wait()


def late_kernel(late_a, late_b, old, out, sem):
    me = lax.axis_index("a")
    for target, late in enumerate((late_a, late_b)):
        rows = LATE[target]

        @pl.when(me == target)
        def _():
            copy = pltpu.make_async_copy(late, out.at[pl.ds(ROWS - rows, rows), 0, pl.ds((target + 2) * BLOCK, BLOCK)], sem)
            copy.start()
            copy.wait()


def trig_table():
    half = HEAD // 2
    inv_freq = ROPE_BASE ** (-2.0 * np.arange(half) / HEAD)
    angles = SEQ * inv_freq
    return np.stack([np.cos(angles), np.sin(angles)]).astype(np.float32)


def solution(mesh):
    cache_in = P('dp', None, 'a', None)
    cache_out = P('dp', 'a', None, None)
    rows_spec = P('dp', None)
    layer_specs = (P(None, 'a'), P(None, 'a'), P(None, 'a'), P('a', None), P(None), P(None))
    in_specs = (rows_spec, cache_in, cache_in, cache_in, cache_in) + layer_specs + layer_specs
    out_specs = (rows_spec, cache_out, cache_out, cache_out, cache_out)
    bf16, f32 = jnp.bfloat16, jnp.float32
    anywhere = pl.BlockSpec(memory_space=pl.ANY)
    vmem = pl.BlockSpec(memory_space=pltpu.VMEM)

    def device_step(hidden_in, loc_k, loc_v, glo_k, glo_v, loc_wq, loc_wk, loc_wv, loc_wo, loc_pre, loc_post, glo_wq, glo_wk, glo_wv, glo_wo, glo_pre, glo_post):
        model = hidden_in.shape[1]
        gains = [loc_pre, loc_post, glo_pre, glo_post]
        loc_land = jax.ShapeDtypeStruct((ROWS, 1, WINDOW, HEAD), bf16)
        glo_land = jax.ShapeDtypeStruct((ROWS, 1, SEQ, HEAD), bf16)
        dma = pltpu.SemaphoreType.DMA
        moved = pl.pallas_call(
            move_kernel,
            out_shape=(loc_land, loc_land, glo_land, glo_land,
                       jax.ShapeDtypeStruct((ROWS, model), bf16), jax.ShapeDtypeStruct((4, ROWS, HEAD), bf16),
                       jax.ShapeDtypeStruct((LATE[0], BLOCK, HEAD), bf16), jax.ShapeDtypeStruct((LATE[1], BLOCK, HEAD), bf16)),
            in_specs=[anywhere] * 18,
            out_specs=(anywhere,) * 8,
            scratch_shapes=[
                pltpu.VMEM((ROWS, model), bf16), pltpu.VMEM((2, HEAD // 2), f32),
                pltpu.VMEM((model,), bf16), pltpu.VMEM((model,), bf16), pltpu.VMEM((model,), bf16), pltpu.VMEM((model,), bf16),
                pltpu.VMEM((4, ROWS, HEAD), bf16), pltpu.VMEM((ROWS, model), bf16),
                pltpu.VMEM((2,) + loc_wq.shape, bf16), pltpu.VMEM((2,) + loc_wk.shape, bf16),
                pltpu.VMEM((2,) + loc_wv.shape, bf16), pltpu.VMEM((2,) + loc_wo.shape, bf16),
                pltpu.VMEM((2, 2, BLOCK, HEAD), bf16),
                pltpu.VMEM((2, GROUP, 2 * ROWS, HEAD), bf16),
                pltpu.VMEM((2, GROUP, 2 * ROWS, 2 * HEAD), f32),
                pltpu.VMEM((2, GROUP, 2 * ROWS, 2 * HEAD), f32),
                pltpu.VMEM((2, GROUP, ROWS, model), bf16),
                dma((3, DEPTH)), dma((2, LOC_UNITS)), dma((2, GLO_UNITS)), dma((8,)), dma((2, 2)),
                dma((6, 3)), dma((6, 3)), dma((2, LATE[0])),
                dma((LATE[0] - LATE[1], PER)), dma((6,)), dma((2,))],
            compiler_params=pltpu.CompilerParams(collective_id=0, has_side_effects=True),
        )(hidden_in, jnp.asarray(trig_table()), *gains, loc_k, loc_v, glo_k, glo_v,
          loc_wq, loc_wk, loc_wv, loc_wo, glo_wq, glo_wk, glo_wv, glo_wo)
        land, hid, new_kv = moved[:4], moved[4], moved[5]
        late_a = lax.ppermute(moved[6], 'a', [(2, 0)])
        late_b = lax.ppermute(moved[7], 'a', [(3, 1)])
        hidden_out, loc_k_out, loc_v_out, glo_k_out, glo_v_out = pl.pallas_call(
            write_kernel,
            out_shape=(jax.ShapeDtypeStruct((ROWS, model), bf16),)
            + (jax.ShapeDtypeStruct((ROWS, 1, WINDOW, HEAD), bf16),) * 2
            + (jax.ShapeDtypeStruct((ROWS, 1, SEQ + CACHE_ROOM, HEAD), bf16),) * 2,
            in_specs=[vmem, vmem] + [anywhere] * 8,
            out_specs=(vmem,) + (anywhere,) * 4,
            scratch_shapes=[pltpu.VMEM((SLOTS, ROWS, UNIT, HEAD), bf16), dma((SLOTS,)), dma((SLOTS,))],
            compiler_params=pltpu.CompilerParams(vmem_limit_bytes=50 * 2 ** 20),
            cost_estimate=pl.CostEstimate(flops=10 ** 9, bytes_accessed=180 * 10 ** 6, transcendentals=0),
        )(hid, new_kv, loc_k, loc_v, glo_k, glo_v, *land)
        glo_v_out = pl.pallas_call(
            late_kernel,
            out_shape=jax.ShapeDtypeStruct(glo_v_out.shape, bf16),
            in_specs=[vmem, vmem, anywhere],
            out_specs=anywhere,
            scratch_shapes=[dma],
            input_output_aliases={2: 0},
            compiler_params=pltpu.CompilerParams(vmem_limit_bytes=16 * 2 ** 20),
            cost_estimate=pl.CostEstimate(flops=10 ** 7, bytes_accessed=4 * late_a.size, transcendentals=0),
        )(late_a, late_b, glo_v_out)
        return hidden_out, loc_k_out, loc_v_out, glo_k_out, glo_v_out

    return jax.shard_map(device_step, mesh=mesh, in_specs=in_specs, out_specs=out_specs, check_vma=False)
```

```python
import jax
import jax.numpy as jnp
import numpy as np
from jax import lax
from jax.experimental import pallas as pl
from jax.experimental.pallas import tpu as pltpu
from jax.sharding import PartitionSpec as P

SOFTCAP = 50.0
NORM_EPS = 1e-6
ROPE_BASE = 10000.0
WINDOW = 4096
CACHE_ROOM = 512

GROUP = 4
ROWS = 8
BLOCK = 1536
UNIT = 512
HEAD = 256
SEQ = GROUP * BLOCK
PER = BLOCK // UNIT
GLO_UNITS = SEQ // UNIT
LOC_UNITS = WINDOW // UNIT
FIRST_UNIT = (SEQ - WINDOW) // UNIT
STEPS = 4 * ROWS * PER
DEPTH = 2
LATE = (5, 4)
MESH = pl.DeviceIdType.MESH
STAT = 64
LOW = -1e30


def peers(me):
    return (me + 1 - 2 * (me % 2), (me + 2) % 4, 3 - me)


def norm(hidden, gain):
    mean_sq = jnp.mean(hidden * hidden, axis=-1, keepdims=True)
    return hidden * lax.rsqrt(mean_sq + NORM_EPS) * (1.0 + gain.astype(jnp.float32).reshape(1, -1))


def softcap(scores):
    return SOFTCAP * jnp.tanh(scores * (HEAD ** -0.5) / SOFTCAP)


def move_kernel(hid_in, trig_in, lpre_in, lpost_in, gpre_in, gpost_in, lk, lv, gk, gv, lwq, lwk, lwv, lwo, gwq, gwk, gwv, gwo,
                land_lk, land_lv, land_gk, land_gv, hid_out, new_out, late_a, late_b,
                hid, trig, lpre, lpost, gpre, gpost, new_kv, hid_end, wq, wk, wv, wo, kvbuf, qbuf, part, precv, pair, ybuf, hbuf,
                bulk_send, loc_recv, glo_recv, w_sem, kv_sem, ex_send, ex_recv, late_sem, tail_send, small_sem, out_sem):
    dp = lax.axis_index("dp")
    me = lax.axis_index("a")
    dest = peers(me)
    caches = (lk, lv, gk, gv)
    lands = (land_lk, land_lv, land_gk, land_gv)

    barrier = pltpu.get_barrier_semaphore()
    for peer in dest:
        pl.semaphore_signal(barrier, inc=1, device_id=(dp, peer), device_id_type=MESH)
    pl.semaphore_wait(barrier, 3)

    def coords(step):
        c = (step // (ROWS * PER) + 2 - 2 * (me // 2)) % 4
        return c, (step // PER) % ROWS, step % PER

    def valid(step, k):
        c, r, j = coords(step)
        in_window = jnp.logical_or(c >= 2, PER * me + j >= FIRST_UNIT)
        ok = jnp.logical_and(step >= 0, in_window)
        if k == 1:
            late = jnp.logical_and(jnp.logical_and(c == 3, r >= ROWS - LATE[0]), me >= 2)
            ok = jnp.logical_and(ok, jnp.logical_not(late))
        return ok

    def pump(step):
        c, r, j = coords(step)
        slot = step % DEPTH
        for k in range(3):
            @pl.when(valid(step - DEPTH, k))
            def _():
                pltpu.make_async_remote_copy(
                    src_ref=gk.at[0, 0, pl.ds(0, UNIT)], dst_ref=land_gk.at[0, 0, pl.ds(0, UNIT)],
                    send_sem=bulk_send.at[k, slot], recv_sem=glo_recv.at[0, 0],
                    device_id=(dp, dest[k]), device_id_type=MESH).wait_send()
        unit = PER * me + j
        for i in range(4):
            place = unit % LOC_UNITS if i < 2 else unit
            sem = loc_recv.at[i, place] if i < 2 else glo_recv.at[i - 2, place]
            for k in range(3):
                @pl.when(jnp.logical_and(c == i, valid(step, k)))
                def _():
                    pltpu.make_async_remote_copy(
                        src_ref=caches[i].at[r, dest[k], pl.ds(pl.multiple_of(j * UNIT, UNIT), UNIT)],
                        dst_ref=lands[i].at[r, 0, pl.ds(pl.multiple_of(place * UNIT, UNIT), UNIT)],
                        send_sem=bulk_send.at[k, slot], recv_sem=sem,
                        device_id=(dp, dest[k]), device_id_type=MESH).start()

    def send(index, k, src, dst):
        return pltpu.make_async_remote_copy(
            src_ref=src, dst_ref=dst, send_sem=ex_send.at[index], recv_sem=ex_recv.at[index],
            device_id=(dp, dest[k]), device_id_type=MESH)

    weights = [pltpu.make_async_copy(src, dst, w_sem.at[i]) for i, (src, dst) in enumerate((
        (lwq, wq.at[0]), (lwk, wk.at[0]), (lwv, wv.at[0]), (lwo, wo.at[0]),
        (gwq, wq.at[1]), (gwk, wk.at[1]), (gwv, wv.at[1]), (gwo, wo.at[1])))]

    small = [pltpu.make_async_copy(src, dst, small_sem.at[i]) for i, (src, dst) in enumerate((
        (hid_in, hid), (trig_in, trig), (lpre_in, lpre), (lpost_in, lpost),
        (gpre_in, gpre), (gpost_in, gpost)))]

    pump(0)
    pump(1)
    for copy in small + weights:
        copy.start()
    for copy in small:
        copy.wait()

    cosine, sine = trig[0:1, :], trig[1:2, :]

    def rope(heads):
        first, second = heads[:, :HEAD // 2], heads[:, HEAD // 2:]
        return jnp.concatenate([first * cosine - second * sine, second * cosine + first * sine], axis=-1)

    def layer(index, hidden, key_ref, value_ref, pre, post, step):
        normed = norm(hidden, pre[...]).astype(jnp.bfloat16)
        if index == 0:
            for copy in weights[:4]:
                copy.wait()
        else:
            for copy in weights[4:]:
                copy.wait()
        q = jnp.dot(normed, wq[index], preferred_element_type=jnp.float32)
        q = jnp.concatenate([rope(q[:, :HEAD]), rope(q[:, HEAD:])], axis=0).astype(jnp.bfloat16)
        new_k = rope(jnp.dot(normed, wk[index], preferred_element_type=jnp.float32)).astype(jnp.bfloat16)
        new_v = jnp.dot(normed, wv[index], preferred_element_type=jnp.float32).astype(jnp.bfloat16)
        new_kv[2 * index] = new_k
        new_kv[2 * index + 1] = new_v
        own_q = qbuf.at[index]
        own_q[me] = q
        base = 9 * index
        near = send(base, 0, own_q.at[me], own_q.at[me])
        far = send(base + 1, 1, own_q.at[me], own_q.at[me])
        near.start()
        far.start()
        pump(step)
        far.wait()
        onward = send(base + 2, 0, own_q.at[dest[1]], own_q.at[dest[1]])
        onward.start()
        near.wait()
        onward.wait()

        def fetch(item, slot):
            h, r = item // ROWS, item % ROWS
            return (pltpu.make_async_copy(key_ref.at[r, h], kvbuf.at[slot, 0], kv_sem.at[slot, 0]),
                    pltpu.make_async_copy(value_ref.at[r, h], kvbuf.at[slot, 1], kv_sem.at[slot, 1]))

        for copy in fetch(0, 0):
            copy.start()
        items = GROUP * ROWS

        def body(item, carry):
            pump(step + 1 + item)
            slot = item % 2
            h, r = item // ROWS, item % ROWS

            @pl.when(item + 1 < items)
            def _():
                for copy in fetch(item + 1, 1 - slot):
                    copy.start()

            copy_k, copy_v = fetch(item, slot)
            copy_k.wait()
            scores = softcap(lax.dot_general(own_q[h], kvbuf[slot, 0], (((1,), (1,)), ((), ())),
                                             preferred_element_type=jnp.float32))
            if index == 0:
                place = me * BLOCK + lax.broadcasted_iota(jnp.int32, scores.shape, 1)
                inside = place > SEQ - WINDOW
                scores = jnp.where(inside, scores, LOW)
            top = jnp.max(scores, axis=-1, keepdims=True)
            e = jnp.exp(scores - top)
            if index == 0:
                e = jnp.where(inside, e, 0.0)
            total = jnp.sum(e, axis=-1, keepdims=True)
            copy_v.wait()
            out = jnp.dot(e.astype(jnp.bfloat16), kvbuf[slot, 1], preferred_element_type=jnp.float32)
            wide = jnp.concatenate([out, jnp.broadcast_to(top, (2 * ROWS, STAT)),
                                    jnp.broadcast_to(total, (2 * ROWS, STAT))], axis=-1)
            row = lax.broadcasted_iota(jnp.int32, wide.shape, 0) % ROWS
            part[index, h] = jnp.where(row == r, wide, part[index, h])
            return carry

        lax.fori_loop(0, items, body, 0)
        step = step + 1 + items

        mine = part.at[index]
        theirs = precv.at[index]
        near = (send(base + 3, 0, mine.at[dest[0]], theirs.at[0]), send(base + 4, 0, mine.at[dest[2]], theirs.at[1]))
        for copy in near:
            copy.start()
        new_k2 = jnp.concatenate([new_k, new_k], axis=0).astype(jnp.float32)
        new_v2 = jnp.concatenate([new_v, new_v], axis=0).astype(jnp.float32)
        new_s = softcap(jnp.sum(q.astype(jnp.float32) * new_k2, axis=-1, keepdims=True))
        for copy in near:
            copy.wait()

        def split(block):
            return block[:, :HEAD], block[:, HEAD:HEAD + 1], block[:, HEAD + STAT:HEAD + STAT + 1]

        o_a, m_a, l_a = split(mine[dest[1]])
        o_b, m_b, l_b = split(theirs[1])
        top = jnp.maximum(m_a, m_b)
        scale_a, scale_b = jnp.exp(m_a - top), jnp.exp(m_b - top)
        pair[index] = jnp.concatenate(
            [o_a * scale_a + o_b * scale_b, jnp.broadcast_to(top, (2 * ROWS, STAT)),
             jnp.broadcast_to(l_a * scale_a + l_b * scale_b, (2 * ROWS, STAT))], axis=-1)
        far = send(base + 5, 1, pair.at[index], theirs.at[2])
        far.start()
        pump(step)
        far.wait()
        blocks = [split(mine[me]), split(theirs[0]), split(theirs[2])]
        top = new_s
        for _, m, _ in blocks:
            top = jnp.maximum(top, m)
        new_e = jnp.exp(new_s - top)
        total = new_e
        acc = new_e.astype(jnp.bfloat16).astype(jnp.float32) * new_v2
        for o, m, l in blocks:
            scale = jnp.exp(m - top)
            total = total + scale * l
            acc = acc + scale * o
        att = (acc / total).astype(jnp.bfloat16)
        own = jnp.concatenate([att[:ROWS], att[ROWS:]], axis=-1)
        y = jnp.dot(own, wo[index], preferred_element_type=jnp.float32).astype(jnp.bfloat16)
        y_ref = ybuf.at[index]
        y_ref[me] = y
        near = send(base + 6, 0, y_ref.at[me], y_ref.at[me])
        far = [send(base + 6 + k, k, y_ref.at[me], y_ref.at[me]) for k in (1, 2)]
        half = hbuf.at[index]
        side = me % 2
        back = send(18 + 2 * index, 1, half.at[side], half.at[side])
        swap = send(19 + 2 * index, 0, half.at[side], half.at[side])

        @pl.when(me >= 2)
        def _():
            near.start()

        @pl.when(me < 2)
        def _():
            for copy in far:
                copy.start()

        pump(step + 1)

        @pl.when(me >= 2)
        def _():
            near.wait_recv()
            for copy in far:
                copy.wait_recv()
            summed = y_ref[0].astype(jnp.float32)
            for d in range(1, GROUP):
                summed = summed + y_ref[d].astype(jnp.float32)
            after = (hidden + norm(summed, post[...])).astype(jnp.bfloat16)
            half[0] = after[:, :after.shape[1] // 2]
            half[1] = after[:, after.shape[1] // 2:]
            back.start()

        pump(step + 2)

        @pl.when(me >= 2)
        def _():
            near.wait_send()
            back.wait_send()

        @pl.when(me < 2)
        def _():
            for copy in far:
                copy.wait_send()
            back.wait_recv()
            swap.start()
            swap.wait()

        return jnp.concatenate([half[0], half[1]], axis=-1), step + 3

    part[...] = jnp.zeros_like(part)
    hidden, step = layer(0, hid[...].astype(jnp.float32), lk, lv, lpre, lpost, 2)
    hidden, step = layer(1, hidden.astype(jnp.float32), gk, gv, gpre, gpost, step)
    hid_end[...] = hidden
    outs = (pltpu.make_async_copy(hid_end, hid_out, out_sem.at[0]), pltpu.make_async_copy(new_kv, new_out, out_sem.at[1]))
    for copy in outs:
        copy.start()
    for copy in outs:
        copy.wait()

    for late, target, rows in ((late_a, 0, LATE[0]), (late_b, 1, LATE[1])):
        @pl.when(me == target + 2)
        def _():
            def late_in(r):
                return pltpu.make_async_copy(gv.at[ROWS - rows + r, target], kvbuf.at[(r // 2) % 2, r % 2], late_sem.at[0, r])

            def late_out(r):
                return pltpu.make_async_copy(kvbuf.at[(r // 2) % 2, r % 2], late.at[r], late_sem.at[1, r])

            for r in range(rows):
                if r >= 4:
                    late_out(r - 4).wait()
                late_in(r).start()
                if r >= 1:
                    late_in(r - 1).wait()
                    late_out(r - 1).start()
            late_in(rows - 1).wait()
            late_out(rows - 1).start()
            for r in range(max(rows - 4, 0), rows):
                late_out(r).wait()

    def rest(s, carry):
        pump(s)
        return carry

    lax.fori_loop(step, STEPS, rest, 0)

    def tail(r, j):
        unit = PER * me + j
        return pltpu.make_async_remote_copy(
            src_ref=gv.at[r, dest[1], pl.ds(j * UNIT, UNIT)],
            dst_ref=land_gv.at[r, 0, pl.ds(pl.multiple_of(unit * UNIT, UNIT), UNIT)],
            send_sem=tail_send.at[r - ROWS + LATE[0], j], recv_sem=glo_recv.at[1, unit],
            device_id=(dp, dest[1]), device_id_type=MESH)

    tails = [(r, j) for r in range(ROWS - LATE[0], ROWS - LATE[1]) for j in range(PER)]

    @pl.when(me == 3)
    def _():
        for piece in tails:
            tail(*piece).start()

    for s in range(STEPS - DEPTH, STEPS):
        for k in range(3):
            @pl.when(valid(s, k))
            def _():
                pltpu.make_async_remote_copy(
                    src_ref=gk.at[0, 0, pl.ds(0, UNIT)], dst_ref=land_gk.at[0, 0, pl.ds(0, UNIT)],
                    send_sem=bulk_send.at[k, s % DEPTH], recv_sem=glo_recv.at[0, 0],
                    device_id=(dp, dest[k]), device_id_type=MESH).wait_send()

    @pl.when(me == 3)
    def _():
        for piece in tails:
            tail(*piece).wait_send()

    for i in range(4):
        for u in range(LOC_UNITS if i < 2 else GLO_UNITS):
            owner = (u if i >= 2 or u >= FIRST_UNIT else u + LOC_UNITS) // PER
            sem = loc_recv.at[i, u] if i < 2 else glo_recv.at[i - 2, u]

            def await_rows(rows):
                view = lands[i].at[pl.ds(0, rows), :, pl.ds(u * UNIT, UNIT)]
                pltpu.make_async_remote_copy(
                    src_ref=view, dst_ref=view, send_sem=bulk_send.at[0, 0], recv_sem=sem,
                    device_id=(dp, dest[0]), device_id_type=MESH).wait_recv()

            if i == 3 and owner >= 2:
                short = me == owner - 2

                @pl.when(short)
                def _():
                    await_rows(ROWS - LATE[owner - 2])

                @pl.when(jnp.logical_and(me != owner, jnp.logical_not(short)))
                def _():
                    await_rows(ROWS)
            else:
                @pl.when(me != owner)
                def _():
                    await_rows(ROWS)


SLOTS = 6


def write_kernel(hid, new_kv, lk, lv, gk, gv, land_lk, land_lv, land_gk, land_gv,
                 hid_out, lk_out, lv_out, gk_out, gv_out, buf, in_sem, out_sem):
    me = lax.axis_index("a")
    hid_out[...] = hid[...]
    jobs = []
    for i in range(4):
        for u in range(LOC_UNITS if i < 2 else GLO_UNITS + 1):
            jobs.append((i, u))
    caches = (lk, lv, gk, gv)
    lands = (land_lk, land_lv, land_gk, land_gv)
    outs = (lk_out, lv_out, gk_out, gv_out)

    def load(n):
        i, u = jobs[n]
        slot = n % SLOTS
        if i >= 2 and u == GLO_UNITS:
            return
        full = u if i >= 2 or u >= FIRST_UNIT else u + LOC_UNITS
        owner, j = full // PER, full % PER

        @pl.when(me == owner)
        def _():
            pltpu.make_async_copy(caches[i].at[:, owner, pl.ds(j * UNIT, UNIT)], buf.at[slot], in_sem.at[slot]).start()

        @pl.when(me != owner)
        def _():
            pltpu.make_async_copy(lands[i].at[:, 0, pl.ds(u * UNIT, UNIT)], buf.at[slot], in_sem.at[slot]).start()

    def store(n):
        i, u = jobs[n]
        slot = n % SLOTS
        return pltpu.make_async_copy(buf.at[slot], outs[i].at[:, 0, pl.ds(u * UNIT, UNIT)], out_sem.at[slot])

    ahead = SLOTS // 2
    for n in range(ahead):
        load(n)
    for n, (i, u) in enumerate(jobs):
        slot = n % SLOTS
        if n + ahead < len(jobs):
            if n + ahead >= SLOTS:
                store(n + ahead - SLOTS).wait()
            load(n + ahead)
        pad = i >= 2 and u == GLO_UNITS
        if not pad:
            pltpu.make_async_copy(lands[i].at[:, 0, pl.ds(0, UNIT)], buf.at[slot], in_sem.at[slot]).wait()
        else:
            buf[slot] = jnp.zeros((ROWS, UNIT, HEAD), jnp.bfloat16)
        if pad or (i < 2 and u == SEQ % WINDOW // UNIT):
            head = buf[slot, :, 0:16, :].astype(jnp.float32)
            first = lax.broadcasted_iota(jnp.int32, head.shape, 1) == 0
            new = jnp.broadcast_to(new_kv[i].astype(jnp.float32)[:, None, :], head.shape)
            buf[slot, :, 0:16, :] = jnp.where(first, new, head).astype(jnp.bfloat16)
        store(n).start()
    for n in range(len(jobs) - SLOTS, len(jobs)):
        store(n).wait()


def late_kernel(late_a, late_b, old, out, sem):
    me = lax.axis_index("a")
    for target, late in enumerate((late_a, late_b)):
        rows = LATE[target]

        @pl.when(me == target)
        def _():
            copy = pltpu.make_async_copy(late, out.at[pl.ds(ROWS - rows, rows), 0, pl.ds((target + 2) * BLOCK, BLOCK)], sem)
            copy.start()
            copy.wait()


def trig_table():
    half = HEAD // 2
    inv_freq = ROPE_BASE ** (-2.0 * np.arange(half) / HEAD)
    angles = SEQ * inv_freq
    return np.stack([np.cos(angles), np.sin(angles)]).astype(np.float32)


def solution(mesh):
    cache_in = P('dp', None, 'a', None)
    cache_out = P('dp', 'a', None, None)
    rows_spec = P('dp', None)
    layer_specs = (P(None, 'a'), P(None, 'a'), P(None, 'a'), P('a', None), P(None), P(None))
    in_specs = (rows_spec, cache_in, cache_in, cache_in, cache_in) + layer_specs + layer_specs
    out_specs = (rows_spec, cache_out, cache_out, cache_out, cache_out)
    bf16, f32 = jnp.bfloat16, jnp.float32
    anywhere = pl.BlockSpec(memory_space=pl.ANY)
    vmem = pl.BlockSpec(memory_space=pltpu.VMEM)

    def device_step(hidden_in, loc_k, loc_v, glo_k, glo_v, loc_wq, loc_wk, loc_wv, loc_wo, loc_pre, loc_post, glo_wq, glo_wk, glo_wv, glo_wo, glo_pre, glo_post):
        model = hidden_in.shape[1]
        gains = [loc_pre, loc_post, glo_pre, glo_post]
        loc_land = jax.ShapeDtypeStruct((ROWS, 1, WINDOW, HEAD), bf16)
        glo_land = jax.ShapeDtypeStruct((ROWS, 1, SEQ, HEAD), bf16)
        dma = pltpu.SemaphoreType.DMA
        moved = pl.pallas_call(
            move_kernel,
            out_shape=(loc_land, loc_land, glo_land, glo_land,
                       jax.ShapeDtypeStruct((ROWS, model), bf16), jax.ShapeDtypeStruct((4, ROWS, HEAD), bf16),
                       jax.ShapeDtypeStruct((LATE[0], BLOCK, HEAD), bf16), jax.ShapeDtypeStruct((LATE[1], BLOCK, HEAD), bf16)),
            in_specs=[anywhere] * 18,
            out_specs=(anywhere,) * 8,
            scratch_shapes=[
                pltpu.VMEM((ROWS, model), bf16), pltpu.VMEM((2, HEAD // 2), f32),
                pltpu.VMEM((model,), bf16), pltpu.VMEM((model,), bf16), pltpu.VMEM((model,), bf16), pltpu.VMEM((model,), bf16),
                pltpu.VMEM((4, ROWS, HEAD), bf16), pltpu.VMEM((ROWS, model), bf16),
                pltpu.VMEM((2,) + loc_wq.shape, bf16), pltpu.VMEM((2,) + loc_wk.shape, bf16),
                pltpu.VMEM((2,) + loc_wv.shape, bf16), pltpu.VMEM((2,) + loc_wo.shape, bf16),
                pltpu.VMEM((2, 2, BLOCK, HEAD), bf16),
                pltpu.VMEM((2, GROUP, 2 * ROWS, HEAD), bf16),
                pltpu.VMEM((2, GROUP, 2 * ROWS, HEAD + 2 * STAT), f32),
                pltpu.VMEM((2, 3, 2 * ROWS, HEAD + 2 * STAT), f32),
                pltpu.VMEM((2, 2 * ROWS, HEAD + 2 * STAT), f32),
                pltpu.VMEM((2, GROUP, ROWS, model), bf16), pltpu.VMEM((2, 2, ROWS, model // 2), bf16),
                dma((3, DEPTH)), dma((2, LOC_UNITS)), dma((2, GLO_UNITS)), dma((8,)), dma((2, 2)),
                dma((22,)), dma((22,)), dma((2, LATE[0])),
                dma((LATE[0] - LATE[1], PER)), dma((6,)), dma((2,))],
            compiler_params=pltpu.CompilerParams(collective_id=0, has_side_effects=True),
        )(hidden_in, jnp.asarray(trig_table()), *gains, loc_k, loc_v, glo_k, glo_v,
          loc_wq, loc_wk, loc_wv, loc_wo, glo_wq, glo_wk, glo_wv, glo_wo)
        land, hid, new_kv = moved[:4], moved[4], moved[5]
        late_a = lax.ppermute(moved[6], 'a', [(2, 0)])
        late_b = lax.ppermute(moved[7], 'a', [(3, 1)])
        hidden_out, loc_k_out, loc_v_out, glo_k_out, glo_v_out = pl.pallas_call(
            write_kernel,
            out_shape=(jax.ShapeDtypeStruct((ROWS, model), bf16),)
            + (jax.ShapeDtypeStruct((ROWS, 1, WINDOW, HEAD), bf16),) * 2
            + (jax.ShapeDtypeStruct((ROWS, 1, SEQ + CACHE_ROOM, HEAD), bf16),) * 2,
            in_specs=[vmem, vmem] + [anywhere] * 8,
            out_specs=(vmem,) + (anywhere,) * 4,
            scratch_shapes=[pltpu.VMEM((SLOTS, ROWS, UNIT, HEAD), bf16), dma((SLOTS,)), dma((SLOTS,))],
            compiler_params=pltpu.CompilerParams(vmem_limit_bytes=50 * 2 ** 20),
            cost_estimate=pl.CostEstimate(flops=10 ** 9, bytes_accessed=180 * 10 ** 6, transcendentals=0),
        )(hid, new_kv, loc_k, loc_v, glo_k, glo_v, *land)
        glo_v_out = pl.pallas_call(
            late_kernel,
            out_shape=jax.ShapeDtypeStruct(glo_v_out.shape, bf16),
            in_specs=[vmem, vmem, anywhere],
            out_specs=anywhere,
            scratch_shapes=[dma],
            input_output_aliases={2: 0},
            compiler_params=pltpu.CompilerParams(vmem_limit_bytes=16 * 2 ** 20),
            cost_estimate=pl.CostEstimate(flops=10 ** 7, bytes_accessed=4 * late_a.size, transcendentals=0),
        )(late_a, late_b, glo_v_out)
        return hidden_out, loc_k_out, loc_v_out, glo_k_out, glo_v_out

    return jax.shard_map(device_step, mesh=mesh, in_specs=in_specs, out_specs=out_specs, check_vma=False)
```

```python
import jax
import jax.numpy as jnp
import numpy as np
from jax import lax
from jax.experimental import pallas as pl
from jax.experimental.pallas import tpu as pltpu
from jax.sharding import PartitionSpec as P

SOFTCAP = 50.0
NORM_EPS = 1e-6
ROPE_BASE = 10000.0
WINDOW = 4096
CACHE_ROOM = 512

GROUP = 4
ROWS = 8
BLOCK = 1536
UNIT = 512
HEAD = 256
SEQ = GROUP * BLOCK
PER = BLOCK // UNIT
GLO_UNITS = SEQ // UNIT
LOC_UNITS = WINDOW // UNIT
FIRST_UNIT = (SEQ - WINDOW) // UNIT
STEPS = 4 * ROWS * PER
DEPTH = 2
LATE = (5, 4)
MESH = pl.DeviceIdType.MESH
STAT = 64
LOW = -1e30


def peers(me):
    return (me + 1 - 2 * (me % 2), (me + 2) % 4, 3 - me)


def norm(hidden, gain):
    mean_sq = jnp.mean(hidden * hidden, axis=-1, keepdims=True)
    return hidden * lax.rsqrt(mean_sq + NORM_EPS) * (1.0 + gain.astype(jnp.float32).reshape(1, -1))


def softcap(scores):
    return SOFTCAP * jnp.tanh(scores * (HEAD ** -0.5) / SOFTCAP)


def move_kernel(hid_in, trig_in, lpre_in, lpost_in, gpre_in, gpost_in, lk, lv, gk, gv, lwq, lwk, lwv, lwo, gwq, gwk, gwv, gwo,
                land_lk, land_lv, land_gk, land_gv, hid_out, new_out, late_a, late_b, late_c,
                hid, trig, lpre, lpost, gpre, gpost, new_kv, hid_end, wq, wk, wv, wo, kvbuf, qbuf, part, precv, pair, att, ybuf, hbuf,
                bulk_send, loc_recv, glo_recv, w_sem, kv_sem, ex_send, ex_recv, late_sem, tail_send, small_sem, out_sem, first_sem):
    dp = lax.axis_index("dp")
    me = lax.axis_index("a")
    dest = peers(me)
    caches = (lk, lv, gk, gv)
    lands = (land_lk, land_lv, land_gk, land_gv)

    first = [pltpu.make_async_copy(lk.at[0, dest[k], pl.ds(0, UNIT)], kvbuf.at[0, k - 1, pl.ds(0, UNIT)], first_sem.at[k - 1])
             for k in (1, 2)]

    @pl.when(me >= 2)
    def _():
        for copy in first:
            copy.start()

    barrier = pltpu.get_barrier_semaphore()
    for peer in dest:
        pl.semaphore_signal(barrier, inc=1, device_id=(dp, peer), device_id_type=MESH)
    pl.semaphore_wait(barrier, 3)

    def coords(step):
        c = (step // (ROWS * PER) + 2 - 2 * (me // 2)) % 4
        return c, (step // PER) % ROWS, step % PER

    def valid(step, k):
        c, r, j = coords(step)
        in_window = jnp.logical_or(c >= 2, PER * me + j >= FIRST_UNIT)
        ok = jnp.logical_and(step >= 0, in_window)
        if k == 1:
            late = jnp.logical_and(jnp.logical_and(c == 3, r >= ROWS - LATE[0]), me >= 2)
            ok = jnp.logical_and(ok, jnp.logical_not(late))
        return ok

    def pump(step, opening=False):
        c, r, j = coords(step)
        slot = step % DEPTH
        for k in range(3):
            @pl.when(valid(step - DEPTH, k))
            def _():
                pltpu.make_async_remote_copy(
                    src_ref=gk.at[0, 0, pl.ds(0, UNIT)], dst_ref=land_gk.at[0, 0, pl.ds(0, UNIT)],
                    send_sem=bulk_send.at[k, slot], recv_sem=glo_recv.at[0, 0],
                    device_id=(dp, dest[k]), device_id_type=MESH).wait_send()
        unit = PER * me + j
        for i in range(4):
            place = unit % LOC_UNITS if i < 2 else unit
            sem = loc_recv.at[i, place] if i < 2 else glo_recv.at[i - 2, place]
            for k in range(3):
                now = jnp.logical_and(c == i, valid(step, k))
                if opening and k:
                    now = jnp.logical_and(now, me < 2)

                @pl.when(now)
                def _():
                    pltpu.make_async_remote_copy(
                        src_ref=caches[i].at[r, dest[k], pl.ds(pl.multiple_of(j * UNIT, UNIT), UNIT)],
                        dst_ref=lands[i].at[r, 0, pl.ds(pl.multiple_of(place * UNIT, UNIT), UNIT)],
                        send_sem=bulk_send.at[k, slot], recv_sem=sem,
                        device_id=(dp, dest[k]), device_id_type=MESH).start()

    def send(index, k, src, dst):
        return pltpu.make_async_remote_copy(
            src_ref=src, dst_ref=dst, send_sem=ex_send.at[index], recv_sem=ex_recv.at[index],
            device_id=(dp, dest[k]), device_id_type=MESH)

    weights = [pltpu.make_async_copy(src, dst, w_sem.at[i]) for i, (src, dst) in enumerate((
        (lwq, wq.at[0]), (lwk, wk.at[0]), (lwv, wv.at[0]), (lwo, wo.at[0]),
        (gwq, wq.at[1]), (gwk, wk.at[1]), (gwv, wv.at[1]), (gwo, wo.at[1])))]

    small = [pltpu.make_async_copy(src, dst, small_sem.at[i]) for i, (src, dst) in enumerate((
        (hid_in, hid), (trig_in, trig), (lpre_in, lpre), (lpost_in, lpost),
        (gpre_in, gpre), (gpost_in, gpost)))]

    @pl.when(me >= 2)
    def _():
        place = (PER * me) % LOC_UNITS
        for k in (1, 2):
            first[k - 1].wait()
            pltpu.make_async_remote_copy(
                src_ref=kvbuf.at[0, k - 1, pl.ds(0, UNIT)],
                dst_ref=land_lk.at[0, 0, pl.ds(pl.multiple_of(place * UNIT, UNIT), UNIT)],
                send_sem=bulk_send.at[k, 0], recv_sem=loc_recv.at[0, place],
                device_id=(dp, dest[k]), device_id_type=MESH).start()

    pump(0, opening=True)
    pump(1)
    for copy in small + weights:
        copy.start()
    for copy in small:
        copy.wait()

    cosine, sine = trig[0:1, :], trig[1:2, :]

    def rope(heads):
        first, second = heads[:, :HEAD // 2], heads[:, HEAD // 2:]
        return jnp.concatenate([first * cosine - second * sine, second * cosine + first * sine], axis=-1)

    def layer(index, hidden, key_ref, value_ref, pre, post, step):
        normed = norm(hidden, pre[...]).astype(jnp.bfloat16)
        if index == 0:
            for copy in weights[:4]:
                copy.wait()
        else:
            for copy in weights[4:]:
                copy.wait()
        q = jnp.dot(normed, wq[index], preferred_element_type=jnp.float32)
        q = jnp.concatenate([rope(q[:, :HEAD]), rope(q[:, HEAD:])], axis=0).astype(jnp.bfloat16)
        new_k = rope(jnp.dot(normed, wk[index], preferred_element_type=jnp.float32)).astype(jnp.bfloat16)
        new_v = jnp.dot(normed, wv[index], preferred_element_type=jnp.float32).astype(jnp.bfloat16)
        new_kv[2 * index] = new_k
        new_kv[2 * index + 1] = new_v
        own_q = qbuf.at[index]
        own_q[me] = q
        base = 11 * index
        near = send(base, 0, own_q.at[me], own_q.at[me])
        far = send(base + 1, 1, own_q.at[me], own_q.at[me])
        near.start()
        far.start()
        pump(step)
        far.wait()
        onward = send(base + 2, 0, own_q.at[dest[1]], own_q.at[dest[1]])
        onward.start()
        near.wait()
        onward.wait()

        def fetch(item, slot):
            h, r = item // ROWS, item % ROWS
            return (pltpu.make_async_copy(key_ref.at[r, h], kvbuf.at[slot, 0], kv_sem.at[slot, 0]),
                    pltpu.make_async_copy(value_ref.at[r, h], kvbuf.at[slot, 1], kv_sem.at[slot, 1]))

        for copy in fetch(0, 0):
            copy.start()
        items = GROUP * ROWS

        def body(item, carry):
            pump(step + 1 + item)
            slot = item % 2
            h, r = item // ROWS, item % ROWS

            @pl.when(item + 1 < items)
            def _():
                for copy in fetch(item + 1, 1 - slot):
                    copy.start()

            copy_k, copy_v = fetch(item, slot)
            copy_k.wait()
            scores = softcap(lax.dot_general(own_q[h], kvbuf[slot, 0], (((1,), (1,)), ((), ())),
                                             preferred_element_type=jnp.float32))
            if index == 0:
                place = me * BLOCK + lax.broadcasted_iota(jnp.int32, scores.shape, 1)
                inside = place > SEQ - WINDOW
                scores = jnp.where(inside, scores, LOW)
            top = jnp.max(scores, axis=-1, keepdims=True)
            e = jnp.exp(scores - top)
            if index == 0:
                e = jnp.where(inside, e, 0.0)
            total = jnp.sum(e, axis=-1, keepdims=True)
            copy_v.wait()
            out = jnp.dot(e.astype(jnp.bfloat16), kvbuf[slot, 1], preferred_element_type=jnp.float32)
            wide = jnp.concatenate([out, jnp.broadcast_to(top, (2 * ROWS, STAT)),
                                    jnp.broadcast_to(total, (2 * ROWS, STAT))], axis=-1)
            row = lax.broadcasted_iota(jnp.int32, wide.shape, 0) % ROWS
            part[index, h] = jnp.where(row == r, wide, part[index, h])
            return carry

        lax.fori_loop(0, items, body, 0)
        step = step + 1 + items

        mine = part.at[index]
        theirs = precv.at[index]
        near = (send(base + 3, 0, mine.at[dest[0]], theirs.at[0]), send(base + 4, 0, mine.at[dest[2]], theirs.at[1]))
        for copy in near:
            copy.start()
        new_k2 = jnp.concatenate([new_k, new_k], axis=0).astype(jnp.float32)
        new_v2 = jnp.concatenate([new_v, new_v], axis=0).astype(jnp.float32)
        new_s = softcap(jnp.sum(q.astype(jnp.float32) * new_k2, axis=-1, keepdims=True))
        new = (new_v2, new_s, jnp.ones_like(new_s))
        for copy in near:
            copy.wait()

        def split(block):
            return block[:, :HEAD], block[:, HEAD:HEAD + 1], block[:, HEAD + STAT:HEAD + STAT + 1]

        def merge(blocks):
            top = blocks[0][1]
            for _, m, _ in blocks[1:]:
                top = jnp.maximum(top, m)
            acc, total = 0.0, 0.0
            for o, m, l in blocks:
                scale = jnp.exp(m - top)
                acc = acc + scale * o
                total = total + scale * l
            return acc, top, total

        def packed(acc, top, total):
            return jnp.concatenate([acc, jnp.broadcast_to(top, (2 * ROWS, STAT)),
                                    jnp.broadcast_to(total, (2 * ROWS, STAT))], axis=-1)

        both = [split(mine[me]), split(theirs[0]), new]
        across = pair.at[index]
        across[0] = packed(*merge([split(mine[dest[1]]), split(theirs[1])]))
        across[1] = packed(*merge(both))
        result = att.at[index]
        far = [send(base + 5 + i, 1, across.at[i], theirs.at[2 + i]) for i in (0, 1)]
        reply = send(base + 7, 1, result.at[1], result.at[0])

        @pl.when(me < 2)
        def _():
            for copy in far:
                copy.start()

        pump(step)

        @pl.when(me >= 2)
        def _():
            for copy in far:
                copy.wait_recv()
            acc, _, total = merge(both + [split(theirs[2])])
            result[0] = (acc / total).astype(jnp.bfloat16)
            acc, _, total = merge([split(across[0]), split(theirs[3])])
            result[1] = (acc / total).astype(jnp.bfloat16)
            reply.start()

        pump(step + 1)

        @pl.when(me >= 2)
        def _():
            reply.wait_send()

        @pl.when(me < 2)
        def _():
            for copy in far:
                copy.wait_send()
            reply.wait_recv()

        heads = result[0]
        step = step + 1
        own = jnp.concatenate([heads[:ROWS], heads[ROWS:]], axis=-1)
        y = jnp.dot(own, wo[index], preferred_element_type=jnp.float32).astype(jnp.bfloat16)
        y_ref = ybuf.at[index]
        y_ref[me] = y
        near = send(base + 8, 0, y_ref.at[me], y_ref.at[me])
        far = [send(base + 8 + k, k, y_ref.at[me], y_ref.at[me]) for k in (1, 2)]
        half = hbuf.at[index]
        side = me % 2
        back = send(22 + 2 * index, 1, half.at[side], half.at[side])
        swap = send(23 + 2 * index, 0, half.at[side], half.at[side])

        @pl.when(me >= 2)
        def _():
            near.start()

        @pl.when(me < 2)
        def _():
            for copy in far:
                copy.start()

        pump(step + 1)

        @pl.when(me >= 2)
        def _():
            near.wait_recv()
            for copy in far:
                copy.wait_recv()
            summed = y_ref[0].astype(jnp.float32)
            for d in range(1, GROUP):
                summed = summed + y_ref[d].astype(jnp.float32)
            after = (hidden + norm(summed, post[...])).astype(jnp.bfloat16)
            half[0] = after[:, :after.shape[1] // 2]
            half[1] = after[:, after.shape[1] // 2:]
            back.start()

        pump(step + 2)

        @pl.when(me >= 2)
        def _():
            near.wait_send()
            back.wait_send()

        @pl.when(me < 2)
        def _():
            for copy in far:
                copy.wait_send()
            back.wait_recv()
            swap.start()
            swap.wait()

        return jnp.concatenate([half[0], half[1]], axis=-1), step + 3

    part[...] = jnp.zeros_like(part)
    hidden, step = layer(0, hid[...].astype(jnp.float32), lk, lv, lpre, lpost, 2)
    hidden, step = layer(1, hidden.astype(jnp.float32), gk, gv, gpre, gpost, step)
    hid_end[...] = hidden
    outs = (pltpu.make_async_copy(hid_end, hid_out, out_sem.at[0]), pltpu.make_async_copy(new_kv, new_out, out_sem.at[1]))
    for copy in outs:
        copy.start()
    for copy in outs:
        copy.wait()

    for late, target, rows in ((late_a, 0, LATE[0]), (late_b, 1, LATE[1])):
        @pl.when(me == target + 2)
        def _():
            def late_in(r):
                return pltpu.make_async_copy(gv.at[ROWS - rows + r, target], kvbuf.at[(r // 2) % 2, r % 2], late_sem.at[0, r])

            def late_out(r):
                target_ref = late.at[r] if r < rows - 1 else late_c.at[0]
                return pltpu.make_async_copy(kvbuf.at[(r // 2) % 2, r % 2], target_ref, late_sem.at[1, r])

            for r in range(rows):
                if r >= 4:
                    late_out(r - 4).wait()
                late_in(r).start()
                if r >= 1:
                    late_in(r - 1).wait()
                    late_out(r - 1).start()
            late_in(rows - 1).wait()
            late_out(rows - 1).start()
            for r in range(max(rows - 4, 0), rows):
                late_out(r).wait()

    def rest(s, carry):
        pump(s)
        return carry

    lax.fori_loop(step, STEPS, rest, 0)

    def tail(r, j):
        unit = PER * me + j
        return pltpu.make_async_remote_copy(
            src_ref=gv.at[r, dest[1], pl.ds(j * UNIT, UNIT)],
            dst_ref=land_gv.at[r, 0, pl.ds(pl.multiple_of(unit * UNIT, UNIT), UNIT)],
            send_sem=tail_send.at[r - ROWS + LATE[0], j], recv_sem=glo_recv.at[1, unit],
            device_id=(dp, dest[1]), device_id_type=MESH)

    tails = [(r, j) for r in range(ROWS - LATE[0], ROWS - LATE[1]) for j in range(PER)]

    @pl.when(me == 3)
    def _():
        for piece in tails:
            tail(*piece).start()

    for s in range(STEPS - DEPTH, STEPS):
        for k in range(3):
            @pl.when(valid(s, k))
            def _():
                pltpu.make_async_remote_copy(
                    src_ref=gk.at[0, 0, pl.ds(0, UNIT)], dst_ref=land_gk.at[0, 0, pl.ds(0, UNIT)],
                    send_sem=bulk_send.at[k, s % DEPTH], recv_sem=glo_recv.at[0, 0],
                    device_id=(dp, dest[k]), device_id_type=MESH).wait_send()

    @pl.when(me == 3)
    def _():
        for piece in tails:
            tail(*piece).wait_send()

    for i in range(4):
        for u in range(LOC_UNITS if i < 2 else GLO_UNITS):
            owner = (u if i >= 2 or u >= FIRST_UNIT else u + LOC_UNITS) // PER
            sem = loc_recv.at[i, u] if i < 2 else glo_recv.at[i - 2, u]

            def await_rows(rows):
                view = lands[i].at[pl.ds(0, rows), :, pl.ds(u * UNIT, UNIT)]
                pltpu.make_async_remote_copy(
                    src_ref=view, dst_ref=view, send_sem=bulk_send.at[0, 0], recv_sem=sem,
                    device_id=(dp, dest[0]), device_id_type=MESH).wait_recv()

            if i == 3 and owner >= 2:
                short = me == owner - 2

                @pl.when(short)
                def _():
                    await_rows(ROWS - LATE[owner - 2])

                @pl.when(jnp.logical_and(me != owner, jnp.logical_not(short)))
                def _():
                    await_rows(ROWS)
            else:
                @pl.when(me != owner)
                def _():
                    await_rows(ROWS)


SLOTS = 6


def write_kernel(hid, new_kv, lk, lv, gk, gv, land_lk, land_lv, land_gk, land_gv,
                 hid_out, lk_out, lv_out, gk_out, gv_out, buf, in_sem, out_sem):
    me = lax.axis_index("a")
    hid_out[...] = hid[...]
    jobs = []
    for i in range(4):
        for u in range(LOC_UNITS if i < 2 else GLO_UNITS + 1):
            jobs.append((i, u))
    caches = (lk, lv, gk, gv)
    lands = (land_lk, land_lv, land_gk, land_gv)
    outs = (lk_out, lv_out, gk_out, gv_out)

    def load(n):
        i, u = jobs[n]
        slot = n % SLOTS
        if i >= 2 and u == GLO_UNITS:
            return
        full = u if i >= 2 or u >= FIRST_UNIT else u + LOC_UNITS
        owner, j = full // PER, full % PER

        @pl.when(me == owner)
        def _():
            pltpu.make_async_copy(caches[i].at[:, owner, pl.ds(j * UNIT, UNIT)], buf.at[slot], in_sem.at[slot]).start()

        @pl.when(me != owner)
        def _():
            pltpu.make_async_copy(lands[i].at[:, 0, pl.ds(u * UNIT, UNIT)], buf.at[slot], in_sem.at[slot]).start()

    def store(n):
        i, u = jobs[n]
        slot = n % SLOTS
        return pltpu.make_async_copy(buf.at[slot], outs[i].at[:, 0, pl.ds(u * UNIT, UNIT)], out_sem.at[slot])

    ahead = SLOTS // 2
    for n in range(ahead):
        load(n)
    for n, (i, u) in enumerate(jobs):
        slot = n % SLOTS
        if n + ahead < len(jobs):
            if n + ahead >= SLOTS:
                store(n + ahead - SLOTS).wait()
            load(n + ahead)
        pad = i >= 2 and u == GLO_UNITS
        if not pad:
            pltpu.make_async_copy(lands[i].at[:, 0, pl.ds(0, UNIT)], buf.at[slot], in_sem.at[slot]).wait()
        else:
            buf[slot] = jnp.zeros((ROWS, UNIT, HEAD), jnp.bfloat16)
        if pad or (i < 2 and u == SEQ % WINDOW // UNIT):
            head = buf[slot, :, 0:16, :].astype(jnp.float32)
            first = lax.broadcasted_iota(jnp.int32, head.shape, 1) == 0
            new = jnp.broadcast_to(new_kv[i].astype(jnp.float32)[:, None, :], head.shape)
            buf[slot, :, 0:16, :] = jnp.where(first, new, head).astype(jnp.bfloat16)
        store(n).start()
    for n in range(len(jobs) - SLOTS, len(jobs)):
        store(n).wait()


def late_kernel(late_a, late_b, old, out, sem):
    me = lax.axis_index("a")
    for target, late in enumerate((late_a, late_b)):
        rows = LATE[target]

        @pl.when(me == target)
        def _():
            place = out.at[pl.ds(ROWS - rows, rows - 1), 0, pl.ds((target + 2) * BLOCK, BLOCK)]
            copy = pltpu.make_async_copy(late, place, sem)
            copy.start()
            copy.wait()


def last_kernel(late_c, old, out, sem):
    me = lax.axis_index("a")

    @pl.when(me < 2)
    def _():
        place = pl.multiple_of((me + 2) * BLOCK, BLOCK)
        copy = pltpu.make_async_copy(late_c, out.at[pl.ds(ROWS - 1, 1), 0, pl.ds(place, BLOCK)], sem)
        copy.start()
        copy.wait()


def trig_table():
    half = HEAD // 2
    inv_freq = ROPE_BASE ** (-2.0 * np.arange(half) / HEAD)
    angles = SEQ * inv_freq
    return np.stack([np.cos(angles), np.sin(angles)]).astype(np.float32)


def solution(mesh):
    cache_in = P('dp', None, 'a', None)
    cache_out = P('dp', 'a', None, None)
    rows_spec = P('dp', None)
    layer_specs = (P(None, 'a'), P(None, 'a'), P(None, 'a'), P('a', None), P(None), P(None))
    in_specs = (rows_spec, cache_in, cache_in, cache_in, cache_in) + layer_specs + layer_specs
    out_specs = (rows_spec, cache_out, cache_out, cache_out, cache_out)
    bf16, f32 = jnp.bfloat16, jnp.float32
    anywhere = pl.BlockSpec(memory_space=pl.ANY)
    vmem = pl.BlockSpec(memory_space=pltpu.VMEM)

    def device_step(hidden_in, loc_k, loc_v, glo_k, glo_v, loc_wq, loc_wk, loc_wv, loc_wo, loc_pre, loc_post, glo_wq, glo_wk, glo_wv, glo_wo, glo_pre, glo_post):
        model = hidden_in.shape[1]
        gains = [loc_pre, loc_post, glo_pre, glo_post]
        loc_land = jax.ShapeDtypeStruct((ROWS, 1, WINDOW, HEAD), bf16)
        glo_land = jax.ShapeDtypeStruct((ROWS, 1, SEQ, HEAD), bf16)
        dma = pltpu.SemaphoreType.DMA
        moved = pl.pallas_call(
            move_kernel,
            out_shape=(loc_land, loc_land, glo_land, glo_land,
                       jax.ShapeDtypeStruct((ROWS, model), bf16), jax.ShapeDtypeStruct((4, ROWS, HEAD), bf16),
                       jax.ShapeDtypeStruct((LATE[0] - 1, BLOCK, HEAD), bf16),
                       jax.ShapeDtypeStruct((LATE[1] - 1, BLOCK, HEAD), bf16), jax.ShapeDtypeStruct((1, BLOCK, HEAD), bf16)),
            in_specs=[anywhere] * 18,
            out_specs=(anywhere,) * 9,
            scratch_shapes=[
                pltpu.VMEM((ROWS, model), bf16), pltpu.VMEM((2, HEAD // 2), f32),
                pltpu.VMEM((model,), bf16), pltpu.VMEM((model,), bf16), pltpu.VMEM((model,), bf16), pltpu.VMEM((model,), bf16),
                pltpu.VMEM((4, ROWS, HEAD), bf16), pltpu.VMEM((ROWS, model), bf16),
                pltpu.VMEM((2,) + loc_wq.shape, bf16), pltpu.VMEM((2,) + loc_wk.shape, bf16),
                pltpu.VMEM((2,) + loc_wv.shape, bf16), pltpu.VMEM((2,) + loc_wo.shape, bf16),
                pltpu.VMEM((2, 2, BLOCK, HEAD), bf16),
                pltpu.VMEM((2, GROUP, 2 * ROWS, HEAD), bf16),
                pltpu.VMEM((2, GROUP, 2 * ROWS, HEAD + 2 * STAT), f32),
                pltpu.VMEM((2, 4, 2 * ROWS, HEAD + 2 * STAT), f32),
                pltpu.VMEM((2, 2, 2 * ROWS, HEAD + 2 * STAT), f32),
                pltpu.VMEM((2, 2, 2 * ROWS, HEAD), bf16),
                pltpu.VMEM((2, GROUP, ROWS, model), bf16), pltpu.VMEM((2, 2, ROWS, model // 2), bf16),
                dma((3, DEPTH)), dma((2, LOC_UNITS)), dma((2, GLO_UNITS)), dma((8,)), dma((2, 2)),
                dma((26,)), dma((26,)), dma((2, LATE[0])),
                dma((LATE[0] - LATE[1], PER)), dma((6,)), dma((2,)), dma((2,))],
            compiler_params=pltpu.CompilerParams(collective_id=0, has_side_effects=True),
        )(hidden_in, jnp.asarray(trig_table()), *gains, loc_k, loc_v, glo_k, glo_v,
          loc_wq, loc_wk, loc_wv, loc_wo, glo_wq, glo_wk, glo_wv, glo_wo)
        land, hid, new_kv = moved[:4], moved[4], moved[5]
        late_a = lax.ppermute(moved[6], 'a', [(2, 0)])
        late_b = lax.ppermute(moved[7], 'a', [(3, 1)])
        late_c = lax.ppermute(moved[8], 'a', [(2, 0), (3, 1)])
        hidden_out, loc_k_out, loc_v_out, glo_k_out, glo_v_out = pl.pallas_call(
            write_kernel,
            out_shape=(jax.ShapeDtypeStruct((ROWS, model), bf16),)
            + (jax.ShapeDtypeStruct((ROWS, 1, WINDOW, HEAD), bf16),) * 2
            + (jax.ShapeDtypeStruct((ROWS, 1, SEQ + CACHE_ROOM, HEAD), bf16),) * 2,
            in_specs=[vmem, vmem] + [anywhere] * 8,
            out_specs=(vmem,) + (anywhere,) * 4,
            scratch_shapes=[pltpu.VMEM((SLOTS, ROWS, UNIT, HEAD), bf16), dma((SLOTS,)), dma((SLOTS,))],
            compiler_params=pltpu.CompilerParams(vmem_limit_bytes=50 * 2 ** 20),
            cost_estimate=pl.CostEstimate(flops=10 ** 9, bytes_accessed=180 * 10 ** 6, transcendentals=0),
        )(hid, new_kv, loc_k, loc_v, glo_k, glo_v, *land)
        glo_v_out = pl.pallas_call(
            late_kernel,
            out_shape=jax.ShapeDtypeStruct(glo_v_out.shape, bf16),
            in_specs=[vmem, vmem, anywhere],
            out_specs=anywhere,
            scratch_shapes=[dma],
            input_output_aliases={2: 0},
            compiler_params=pltpu.CompilerParams(vmem_limit_bytes=16 * 2 ** 20),
            cost_estimate=pl.CostEstimate(flops=10 ** 7, bytes_accessed=4 * late_a.size, transcendentals=0),
        )(late_a, late_b, glo_v_out)
        glo_v_out = pl.pallas_call(
            last_kernel,
            out_shape=jax.ShapeDtypeStruct(glo_v_out.shape, bf16),
            in_specs=[vmem, anywhere],
            out_specs=anywhere,
            scratch_shapes=[dma],
            input_output_aliases={1: 0},
            compiler_params=pltpu.CompilerParams(vmem_limit_bytes=16 * 2 ** 20),
            cost_estimate=pl.CostEstimate(flops=10 ** 6, bytes_accessed=4 * late_c.size, transcendentals=0),
        )(late_c, glo_v_out)
        return hidden_out, loc_k_out, loc_v_out, glo_k_out, glo_v_out

    return jax.shard_map(device_step, mesh=mesh, in_specs=in_specs, out_specs=out_specs, check_vma=False)
```

```python
import jax
import jax.numpy as jnp
import numpy as np
from jax import lax
from jax.experimental import pallas as pl
from jax.experimental.pallas import tpu as pltpu
from jax.sharding import PartitionSpec as P

SOFTCAP = 50.0
NORM_EPS = 1e-6
ROPE_BASE = 10000.0
WINDOW = 4096
CACHE_ROOM = 512

GROUP = 4
ROWS = 8
BLOCK = 1536
UNIT = 512
HEAD = 256
SEQ = GROUP * BLOCK
PER = BLOCK // UNIT
GLO_UNITS = SEQ // UNIT
LOC_UNITS = WINDOW // UNIT
FIRST_UNIT = (SEQ - WINDOW) // UNIT
STEPS = 4 * ROWS * PER
DEPTH = 2
LATE = (5, 4)
MESH = pl.DeviceIdType.MESH
PIECES = 8
WO_ROWS = 64
STAT = 64
LOW = -1e30


def peers(me):
    return (me + 1 - 2 * (me % 2), (me + 2) % 4, 3 - me)


def norm(hidden, gain):
    mean_sq = jnp.mean(hidden * hidden, axis=-1, keepdims=True)
    return hidden * lax.rsqrt(mean_sq + NORM_EPS) * (1.0 + gain.astype(jnp.float32).reshape(1, -1))


def softcap(scores):
    return SOFTCAP * jnp.tanh(scores * (HEAD ** -0.5) / SOFTCAP)


def move_kernel(hid_in, trig_in, lpre_in, lpost_in, gpre_in, gpost_in, lk, lv, gk, gv, lwq, lwk, lwv, lwo, gwq, gwk, gwv, gwo,
                land_lk, land_lv, land_gk, land_gv, hid_out, new_out, late_a, late_b, late_c,
                hid, trig, lpre, lpost, gpre, gpost, new_kv, hid_end, wq, wk, wv, wo, kvbuf, qbuf, part, precv, pair, att, ybuf, hbuf, wo_far,
                bulk_send, loc_recv, glo_recv, w_sem, kv_sem, ex_send, ex_recv, late_sem, tail_send, small_sem, out_sem, first_sem, wo_send, wo_recv):
    dp = lax.axis_index("dp")
    me = lax.axis_index("a")
    dest = peers(me)
    caches = (lk, lv, gk, gv)
    lands = (land_lk, land_lv, land_gk, land_gv)

    first = [pltpu.make_async_copy(lk.at[0, dest[k], pl.ds(0, UNIT)], kvbuf.at[0, k - 1, pl.ds(0, UNIT)], first_sem.at[k - 1])
             for k in (1, 2)]

    @pl.when(me >= 2)
    def _():
        for copy in first:
            copy.start()

    barrier = pltpu.get_barrier_semaphore()
    for peer in dest:
        pl.semaphore_signal(barrier, inc=1, device_id=(dp, peer), device_id_type=MESH)
    pl.semaphore_wait(barrier, 3)

    def coords(step):
        c = step // (ROWS * PER) * (3 - 2 * (me // 2)) % 4
        return c, (step // PER) % ROWS, step % PER

    def valid(step, k):
        c, r, j = coords(step)
        in_window = jnp.logical_or(c >= 2, PER * me + j >= FIRST_UNIT)
        ok = jnp.logical_and(step >= 0, in_window)
        if k == 1:
            late = jnp.logical_and(jnp.logical_and(c == 3, r >= ROWS - LATE[0]), me >= 2)
            ok = jnp.logical_and(ok, jnp.logical_not(late))
        return ok

    def pump(step, opening=False):
        c, r, j = coords(step)
        slot = step % DEPTH
        for k in range(3):
            @pl.when(valid(step - DEPTH, k))
            def _():
                pltpu.make_async_remote_copy(
                    src_ref=gk.at[0, 0, pl.ds(0, UNIT)], dst_ref=land_gk.at[0, 0, pl.ds(0, UNIT)],
                    send_sem=bulk_send.at[k, slot], recv_sem=glo_recv.at[0, 0],
                    device_id=(dp, dest[k]), device_id_type=MESH).wait_send()
        def piece(s, ref):
            rows = pl.ds(pl.multiple_of(s % PIECES * WO_ROWS, WO_ROWS), WO_ROWS)
            return pltpu.make_async_remote_copy(
                src_ref=ref.at[rows], dst_ref=wo_far.at[s // PIECES, rows], send_sem=wo_send.at[s % DEPTH],
                recv_sem=wo_recv.at[s // PIECES], device_id=(dp, dest[1]), device_id_type=MESH)

        before = step - DEPTH

        @pl.when(jnp.logical_and(me < 2, jnp.logical_and(before >= 0, before < 2 * PIECES)))
        def _():
            piece(before, lwo).wait_send()

        for i, ref in enumerate((lwo, gwo)):
            @pl.when(jnp.logical_and(me < 2, jnp.logical_and(step >= i * PIECES, step < (i + 1) * PIECES)))
            def _():
                piece(step, ref).start()

        unit = PER * me + j
        for i in range(4):
            place = unit % LOC_UNITS if i < 2 else unit
            sem = loc_recv.at[i, place] if i < 2 else glo_recv.at[i - 2, place]
            for k in range(3):
                now = jnp.logical_and(c == i, valid(step, k))
                if opening and k:
                    now = jnp.logical_and(now, me < 2)

                @pl.when(now)
                def _():
                    pltpu.make_async_remote_copy(
                        src_ref=caches[i].at[r, dest[k], pl.ds(pl.multiple_of(j * UNIT, UNIT), UNIT)],
                        dst_ref=lands[i].at[r, 0, pl.ds(pl.multiple_of(place * UNIT, UNIT), UNIT)],
                        send_sem=bulk_send.at[k, slot], recv_sem=sem,
                        device_id=(dp, dest[k]), device_id_type=MESH).start()

    def send(index, k, src, dst):
        return pltpu.make_async_remote_copy(
            src_ref=src, dst_ref=dst, send_sem=ex_send.at[index], recv_sem=ex_recv.at[index],
            device_id=(dp, dest[k]), device_id_type=MESH)

    weights = [pltpu.make_async_copy(src, dst, w_sem.at[i]) for i, (src, dst) in enumerate((
        (lwq, wq.at[0]), (lwk, wk.at[0]), (lwv, wv.at[0]), (lwo, wo.at[0]),
        (gwq, wq.at[1]), (gwk, wk.at[1]), (gwv, wv.at[1]), (gwo, wo.at[1])))]

    small = [pltpu.make_async_copy(src, dst, small_sem.at[i]) for i, (src, dst) in enumerate((
        (hid_in, hid), (trig_in, trig), (lpre_in, lpre), (lpost_in, lpost),
        (gpre_in, gpre), (gpost_in, gpost)))]

    @pl.when(me >= 2)
    def _():
        place = (PER * me) % LOC_UNITS
        for k in (1, 2):
            first[k - 1].wait()
            pltpu.make_async_remote_copy(
                src_ref=kvbuf.at[0, k - 1, pl.ds(0, UNIT)],
                dst_ref=land_lk.at[0, 0, pl.ds(pl.multiple_of(place * UNIT, UNIT), UNIT)],
                send_sem=bulk_send.at[k, 0], recv_sem=loc_recv.at[0, place],
                device_id=(dp, dest[k]), device_id_type=MESH).start()

    pump(0, opening=True)
    pump(1)
    for copy in small + weights:
        copy.start()
    for copy in small:
        copy.wait()

    cosine, sine = trig[0:1, :], trig[1:2, :]

    def rope(heads):
        first, second = heads[:, :HEAD // 2], heads[:, HEAD // 2:]
        return jnp.concatenate([first * cosine - second * sine, second * cosine + first * sine], axis=-1)

    def layer(index, hidden, key_ref, value_ref, pre, post, step):
        normed = norm(hidden, pre[...]).astype(jnp.bfloat16)
        if index == 0:
            for copy in weights[:4]:
                copy.wait()
        else:
            for copy in weights[4:]:
                copy.wait()
        q = jnp.dot(normed, wq[index], preferred_element_type=jnp.float32)
        q = jnp.concatenate([rope(q[:, :HEAD]), rope(q[:, HEAD:])], axis=0).astype(jnp.bfloat16)
        new_k = rope(jnp.dot(normed, wk[index], preferred_element_type=jnp.float32)).astype(jnp.bfloat16)
        new_v = jnp.dot(normed, wv[index], preferred_element_type=jnp.float32).astype(jnp.bfloat16)
        new_kv[2 * index] = new_k
        new_kv[2 * index + 1] = new_v
        own_q = qbuf.at[index]
        own_q[me] = q
        base = 8 * index
        near = send(base, 0, own_q.at[me], own_q.at[me])
        far = send(base + 1, 1, own_q.at[me], own_q.at[me])
        near.start()
        far.start()
        pump(step)
        far.wait()
        onward = send(base + 2, 0, own_q.at[dest[1]], own_q.at[dest[1]])
        onward.start()
        near.wait()
        onward.wait()

        def fetch(item, slot):
            h, r = item // ROWS, item % ROWS
            return (pltpu.make_async_copy(key_ref.at[r, h], kvbuf.at[slot, 0], kv_sem.at[slot, 0]),
                    pltpu.make_async_copy(value_ref.at[r, h], kvbuf.at[slot, 1], kv_sem.at[slot, 1]))

        for copy in fetch(0, 0):
            copy.start()
        items = GROUP * ROWS

        def body(item, carry):
            pump(step + 1 + item)
            slot = item % 2
            h, r = item // ROWS, item % ROWS

            @pl.when(item + 1 < items)
            def _():
                for copy in fetch(item + 1, 1 - slot):
                    copy.start()

            copy_k, copy_v = fetch(item, slot)
            copy_k.wait()
            scores = softcap(lax.dot_general(own_q[h], kvbuf[slot, 0], (((1,), (1,)), ((), ())),
                                             preferred_element_type=jnp.float32))
            if index == 0:
                place = me * BLOCK + lax.broadcasted_iota(jnp.int32, scores.shape, 1)
                inside = place > SEQ - WINDOW
                scores = jnp.where(inside, scores, LOW)
            top = jnp.max(scores, axis=-1, keepdims=True)
            e = jnp.exp(scores - top)
            if index == 0:
                e = jnp.where(inside, e, 0.0)
            total = jnp.sum(e, axis=-1, keepdims=True)
            copy_v.wait()
            out = jnp.dot(e.astype(jnp.bfloat16), kvbuf[slot, 1], preferred_element_type=jnp.float32)
            wide = jnp.concatenate([out, jnp.broadcast_to(top, (2 * ROWS, STAT)),
                                    jnp.broadcast_to(total, (2 * ROWS, STAT))], axis=-1)
            row = lax.broadcasted_iota(jnp.int32, wide.shape, 0) % ROWS
            part[index, h] = jnp.where(row == r, wide, part[index, h])
            return carry

        lax.fori_loop(0, items, body, 0)
        step = step + 1 + items

        mine = part.at[index]
        theirs = precv.at[index]
        near = (send(base + 3, 0, mine.at[dest[0]], theirs.at[0]), send(base + 4, 0, mine.at[dest[2]], theirs.at[1]))
        for copy in near:
            copy.start()
        new_k2 = jnp.concatenate([new_k, new_k], axis=0).astype(jnp.float32)
        new_v2 = jnp.concatenate([new_v, new_v], axis=0).astype(jnp.float32)
        new_s = softcap(jnp.sum(q.astype(jnp.float32) * new_k2, axis=-1, keepdims=True))
        new = (new_v2, new_s, jnp.ones_like(new_s))
        for copy in near:
            copy.wait()

        def split(block):
            return block[:, :HEAD], block[:, HEAD:HEAD + 1], block[:, HEAD + STAT:HEAD + STAT + 1]

        def merge(blocks):
            top = blocks[0][1]
            for _, m, _ in blocks[1:]:
                top = jnp.maximum(top, m)
            acc, total = 0.0, 0.0
            for o, m, l in blocks:
                scale = jnp.exp(m - top)
                acc = acc + scale * o
                total = total + scale * l
            return acc, top, total

        def packed(acc, top, total):
            return jnp.concatenate([acc, jnp.broadcast_to(top, (2 * ROWS, STAT)),
                                    jnp.broadcast_to(total, (2 * ROWS, STAT))], axis=-1)

        both = [split(mine[me]), split(theirs[0]), new]
        across = pair.at[index]
        across[0] = packed(*merge([split(mine[dest[1]]), split(theirs[1])]))
        across[1] = packed(*merge(both))
        heads = att.at[index]
        far = [send(base + 5 + i, 1, across.at[i], theirs.at[2 + i]) for i in (0, 1)]
        y_ref = ybuf.at[index]
        half = hbuf.at[index]
        side = me % 2
        near = send(base + 7, 0, y_ref.at[side], y_ref.at[side])
        back = send(16 + 2 * index, 1, half.at[side], half.at[side])
        swap = send(17 + 2 * index, 0, half.at[side], half.at[side])

        @pl.when(me < 2)
        def _():
            for copy in far:
                copy.start()

        pump(step)

        @pl.when(me >= 2)
        def _():
            for copy in far:
                copy.wait_recv()

            def finished(blocks):
                acc, _, total = merge(blocks)
                out = (acc / total).astype(jnp.bfloat16)
                return jnp.concatenate([out[:ROWS], out[ROWS:]], axis=-1)

            heads[0] = finished(both + [split(theirs[2])])
            heads[1] = finished([split(across[0]), split(theirs[3])])

        pump(step + 1)

        @pl.when(me >= 2)
        def _():
            pltpu.make_async_remote_copy(
                src_ref=wo_far.at[index], dst_ref=wo_far.at[index], send_sem=wo_send.at[0], recv_sem=wo_recv.at[index],
                device_id=(dp, dest[1]), device_id_type=MESH).wait_recv()
            y_ref[side] = (jnp.dot(heads[0], wo[index], preferred_element_type=jnp.float32)
                           + jnp.dot(heads[1], wo_far[index], preferred_element_type=jnp.float32))
            near.start()
            near.wait()
            after = (hidden + norm(y_ref[0] + y_ref[1], post[...])).astype(jnp.bfloat16)
            half[0] = after[:, :after.shape[1] // 2]
            half[1] = after[:, after.shape[1] // 2:]
            back.start()

        pump(step + 2)

        @pl.when(me >= 2)
        def _():
            back.wait_send()

        @pl.when(me < 2)
        def _():
            for copy in far:
                copy.wait_send()
            back.wait_recv()
            swap.start()
            swap.wait()

        return jnp.concatenate([half[0], half[1]], axis=-1), step + 3

    part[...] = jnp.zeros_like(part)
    hidden, step = layer(0, hid[...].astype(jnp.float32), lk, lv, lpre, lpost, 2)
    hidden, step = layer(1, hidden.astype(jnp.float32), gk, gv, gpre, gpost, step)
    hid_end[...] = hidden
    outs = (pltpu.make_async_copy(hid_end, hid_out, out_sem.at[0]), pltpu.make_async_copy(new_kv, new_out, out_sem.at[1]))
    for copy in outs:
        copy.start()
    for copy in outs:
        copy.wait()

    for late, target, rows in ((late_a, 0, LATE[0]), (late_b, 1, LATE[1])):
        @pl.when(me == target + 2)
        def _():
            def late_in(r):
                return pltpu.make_async_copy(gv.at[ROWS - rows + r, target], kvbuf.at[(r // 2) % 2, r % 2], late_sem.at[0, r])

            def late_out(r):
                buf, size = kvbuf.at[(r // 2) % 2, r % 2], BLOCK if r < rows - 1 else BLOCK - UNIT
                return pltpu.make_async_copy(buf.at[pl.ds(0, size)], late.at[pl.ds(r * BLOCK, size)], late_sem.at[1, r])

            end = kvbuf.at[((rows - 1) // 2) % 2, (rows - 1) % 2, pl.ds(BLOCK - UNIT, UNIT)]
            last_out = pltpu.make_async_copy(end, late_c, late_sem.at[0, rows - 1])
            for r in range(rows):
                if r >= 4:
                    late_out(r - 4).wait()
                late_in(r).start()
                if r >= 1:
                    late_in(r - 1).wait()
                    late_out(r - 1).start()
            late_in(rows - 1).wait()
            late_out(rows - 1).start()
            last_out.start()
            for r in range(max(rows - 4, 0), rows):
                late_out(r).wait()
            last_out.wait()

    def rest(s, carry):
        pump(s)
        return carry

    lax.fori_loop(step, STEPS, rest, 0)

    def tail(r, j):
        unit = PER * me + j
        return pltpu.make_async_remote_copy(
            src_ref=gv.at[r, dest[1], pl.ds(j * UNIT, UNIT)],
            dst_ref=land_gv.at[r, 0, pl.ds(pl.multiple_of(unit * UNIT, UNIT), UNIT)],
            send_sem=tail_send.at[r - ROWS + LATE[0], j], recv_sem=glo_recv.at[1, unit],
            device_id=(dp, dest[1]), device_id_type=MESH)

    tails = [(r, j) for r in range(ROWS - LATE[0], ROWS - LATE[1]) for j in range(PER)]

    @pl.when(me == 3)
    def _():
        for piece in tails:
            tail(*piece).start()

    for s in range(STEPS - DEPTH, STEPS):
        for k in range(3):
            @pl.when(valid(s, k))
            def _():
                pltpu.make_async_remote_copy(
                    src_ref=gk.at[0, 0, pl.ds(0, UNIT)], dst_ref=land_gk.at[0, 0, pl.ds(0, UNIT)],
                    send_sem=bulk_send.at[k, s % DEPTH], recv_sem=glo_recv.at[0, 0],
                    device_id=(dp, dest[k]), device_id_type=MESH).wait_send()

    @pl.when(me == 3)
    def _():
        for piece in tails:
            tail(*piece).wait_send()

    for i in range(4):
        for u in range(LOC_UNITS if i < 2 else GLO_UNITS):
            owner = (u if i >= 2 or u >= FIRST_UNIT else u + LOC_UNITS) // PER
            sem = loc_recv.at[i, u] if i < 2 else glo_recv.at[i - 2, u]

            def await_rows(rows):
                view = lands[i].at[pl.ds(0, rows), :, pl.ds(u * UNIT, UNIT)]
                pltpu.make_async_remote_copy(
                    src_ref=view, dst_ref=view, send_sem=bulk_send.at[0, 0], recv_sem=sem,
                    device_id=(dp, dest[0]), device_id_type=MESH).wait_recv()

            if i == 3 and owner >= 2:
                short = me == owner - 2

                @pl.when(short)
                def _():
                    await_rows(ROWS - LATE[owner - 2])

                @pl.when(jnp.logical_and(me != owner, jnp.logical_not(short)))
                def _():
                    await_rows(ROWS)
            else:
                @pl.when(me != owner)
                def _():
                    await_rows(ROWS)


SLOTS = 6


def write_kernel(hid, new_kv, lk, lv, gk, gv, land_lk, land_lv, land_gk, land_gv,
                 hid_out, lk_out, lv_out, gk_out, gv_out, buf, in_sem, out_sem):
    me = lax.axis_index("a")
    hid_out[...] = hid[...]
    jobs = []
    for i in range(4):
        for u in range(LOC_UNITS if i < 2 else GLO_UNITS + 1):
            jobs.append((i, u))
    caches = (lk, lv, gk, gv)
    lands = (land_lk, land_lv, land_gk, land_gv)
    outs = (lk_out, lv_out, gk_out, gv_out)

    def load(n):
        i, u = jobs[n]
        slot = n % SLOTS
        if i >= 2 and u == GLO_UNITS:
            return
        full = u if i >= 2 or u >= FIRST_UNIT else u + LOC_UNITS
        owner, j = full // PER, full % PER

        @pl.when(me == owner)
        def _():
            pltpu.make_async_copy(caches[i].at[:, owner, pl.ds(j * UNIT, UNIT)], buf.at[slot], in_sem.at[slot]).start()

        @pl.when(me != owner)
        def _():
            pltpu.make_async_copy(lands[i].at[:, 0, pl.ds(u * UNIT, UNIT)], buf.at[slot], in_sem.at[slot]).start()

    def store(n):
        i, u = jobs[n]
        slot = n % SLOTS
        return pltpu.make_async_copy(buf.at[slot], outs[i].at[:, 0, pl.ds(u * UNIT, UNIT)], out_sem.at[slot])

    ahead = SLOTS // 2
    for n in range(ahead):
        load(n)
    for n, (i, u) in enumerate(jobs):
        slot = n % SLOTS
        if n + ahead < len(jobs):
            if n + ahead >= SLOTS:
                store(n + ahead - SLOTS).wait()
            load(n + ahead)
        pad = i >= 2 and u == GLO_UNITS
        if not pad:
            pltpu.make_async_copy(lands[i].at[:, 0, pl.ds(0, UNIT)], buf.at[slot], in_sem.at[slot]).wait()
        else:
            buf[slot] = jnp.zeros((ROWS, UNIT, HEAD), jnp.bfloat16)
        if pad or (i < 2 and u == SEQ % WINDOW // UNIT):
            head = buf[slot, :, 0:16, :].astype(jnp.float32)
            first = lax.broadcasted_iota(jnp.int32, head.shape, 1) == 0
            new = jnp.broadcast_to(new_kv[i].astype(jnp.float32)[:, None, :], head.shape)
            buf[slot, :, 0:16, :] = jnp.where(first, new, head).astype(jnp.bfloat16)
        store(n).start()
    for n in range(len(jobs) - SLOTS, len(jobs)):
        store(n).wait()


def late_kernel(late_a, late_b, old, out, sem):
    me = lax.axis_index("a")
    for target, late in enumerate((late_a, late_b)):
        @pl.when(me == target)
        def _():
            copies = []
            for r in range(LATE[target]):
                size = BLOCK if r < LATE[target] - 1 else BLOCK - UNIT
                copies.append(pltpu.make_async_copy(
                    late.at[pl.ds(r * BLOCK, size)],
                    out.at[ROWS - LATE[target] + r, 0, pl.ds((target + 2) * BLOCK, size)], sem.at[r]))
            for copy in copies:
                copy.start()
            for copy in copies:
                copy.wait()


def last_kernel(late_c, old, out, sem):
    me = lax.axis_index("a")

    @pl.when(me < 2)
    def _():
        place = pl.multiple_of((me + 3) * BLOCK - UNIT, UNIT)
        copy = pltpu.make_async_copy(late_c, out.at[ROWS - 1, 0, pl.ds(place, UNIT)], sem)
        copy.start()
        copy.wait()


def trig_table():
    half = HEAD // 2
    inv_freq = ROPE_BASE ** (-2.0 * np.arange(half) / HEAD)
    angles = SEQ * inv_freq
    return np.stack([np.cos(angles), np.sin(angles)]).astype(np.float32)


def solution(mesh):
    cache_in = P('dp', None, 'a', None)
    cache_out = P('dp', 'a', None, None)
    rows_spec = P('dp', None)
    layer_specs = (P(None, 'a'), P(None, 'a'), P(None, 'a'), P('a', None), P(None), P(None))
    in_specs = (rows_spec, cache_in, cache_in, cache_in, cache_in) + layer_specs + layer_specs
    out_specs = (rows_spec, cache_out, cache_out, cache_out, cache_out)
    bf16, f32 = jnp.bfloat16, jnp.float32
    anywhere = pl.BlockSpec(memory_space=pl.ANY)
    vmem = pl.BlockSpec(memory_space=pltpu.VMEM)

    def device_step(hidden_in, loc_k, loc_v, glo_k, glo_v, loc_wq, loc_wk, loc_wv, loc_wo, loc_pre, loc_post, glo_wq, glo_wk, glo_wv, glo_wo, glo_pre, glo_post):
        model = hidden_in.shape[1]
        gains = [loc_pre, loc_post, glo_pre, glo_post]
        loc_land = jax.ShapeDtypeStruct((ROWS, 1, WINDOW, HEAD), bf16)
        glo_land = jax.ShapeDtypeStruct((ROWS, 1, SEQ, HEAD), bf16)
        dma = pltpu.SemaphoreType.DMA
        moved = pl.pallas_call(
            move_kernel,
            out_shape=(loc_land, loc_land, glo_land, glo_land,
                       jax.ShapeDtypeStruct((ROWS, model), bf16), jax.ShapeDtypeStruct((4, ROWS, HEAD), bf16),
                       jax.ShapeDtypeStruct((LATE[0] * BLOCK - UNIT, HEAD), bf16),
                       jax.ShapeDtypeStruct((LATE[1] * BLOCK - UNIT, HEAD), bf16), jax.ShapeDtypeStruct((UNIT, HEAD), bf16)),
            in_specs=[anywhere] * 18,
            out_specs=(anywhere,) * 9,
            scratch_shapes=[
                pltpu.VMEM((ROWS, model), bf16), pltpu.VMEM((2, HEAD // 2), f32),
                pltpu.VMEM((model,), bf16), pltpu.VMEM((model,), bf16), pltpu.VMEM((model,), bf16), pltpu.VMEM((model,), bf16),
                pltpu.VMEM((4, ROWS, HEAD), bf16), pltpu.VMEM((ROWS, model), bf16),
                pltpu.VMEM((2,) + loc_wq.shape, bf16), pltpu.VMEM((2,) + loc_wk.shape, bf16),
                pltpu.VMEM((2,) + loc_wv.shape, bf16), pltpu.VMEM((2,) + loc_wo.shape, bf16),
                pltpu.VMEM((2, 2, BLOCK, HEAD), bf16),
                pltpu.VMEM((2, GROUP, 2 * ROWS, HEAD), bf16),
                pltpu.VMEM((2, GROUP, 2 * ROWS, HEAD + 2 * STAT), f32),
                pltpu.VMEM((2, 4, 2 * ROWS, HEAD + 2 * STAT), f32),
                pltpu.VMEM((2, 2, 2 * ROWS, HEAD + 2 * STAT), f32),
                pltpu.VMEM((2, 2, ROWS, 2 * HEAD), bf16),
                pltpu.VMEM((2, 2, ROWS, model), f32), pltpu.VMEM((2, 2, ROWS, model // 2), bf16),
                pltpu.VMEM((2,) + loc_wo.shape, bf16),
                dma((3, DEPTH)), dma((2, LOC_UNITS)), dma((2, GLO_UNITS)), dma((8,)), dma((2, 2)),
                dma((20,)), dma((20,)), dma((2, LATE[0])),
                dma((LATE[0] - LATE[1], PER)), dma((6,)), dma((2,)), dma((2,)), dma((DEPTH,)), dma((2,))],
            compiler_params=pltpu.CompilerParams(collective_id=0, has_side_effects=True),
        )(hidden_in, jnp.asarray(trig_table()), *gains, loc_k, loc_v, glo_k, glo_v,
          loc_wq, loc_wk, loc_wv, loc_wo, glo_wq, glo_wk, glo_wv, glo_wo)
        land, hid, new_kv = moved[:4], moved[4], moved[5]
        late_a = lax.ppermute(moved[6], 'a', [(2, 0)])
        late_b = lax.ppermute(moved[7], 'a', [(3, 1)])
        late_c = lax.ppermute(moved[8], 'a', [(2, 0), (3, 1)])
        hidden_out, loc_k_out, loc_v_out, glo_k_out, glo_v_out = pl.pallas_call(
            write_kernel,
            out_shape=(jax.ShapeDtypeStruct((ROWS, model), bf16),)
            + (jax.ShapeDtypeStruct((ROWS, 1, WINDOW, HEAD), bf16),) * 2
            + (jax.ShapeDtypeStruct((ROWS, 1, SEQ + CACHE_ROOM, HEAD), bf16),) * 2,
            in_specs=[vmem, vmem] + [anywhere] * 8,
            out_specs=(vmem,) + (anywhere,) * 4,
            scratch_shapes=[pltpu.VMEM((SLOTS, ROWS, UNIT, HEAD), bf16), dma((SLOTS,)), dma((SLOTS,))],
            compiler_params=pltpu.CompilerParams(vmem_limit_bytes=50 * 2 ** 20),
            cost_estimate=pl.CostEstimate(flops=10 ** 9, bytes_accessed=180 * 10 ** 6, transcendentals=0),
        )(hid, new_kv, loc_k, loc_v, glo_k, glo_v, *land)
        glo_v_out = pl.pallas_call(
            late_kernel,
            out_shape=jax.ShapeDtypeStruct(glo_v_out.shape, bf16),
            in_specs=[vmem, vmem, anywhere],
            out_specs=anywhere,
            scratch_shapes=[dma((LATE[0],))],
            input_output_aliases={2: 0},
            compiler_params=pltpu.CompilerParams(vmem_limit_bytes=16 * 2 ** 20),
            cost_estimate=pl.CostEstimate(flops=10 ** 7, bytes_accessed=4 * late_a.size, transcendentals=0),
        )(late_a, late_b, glo_v_out)
        glo_v_out = pl.pallas_call(
            last_kernel,
            out_shape=jax.ShapeDtypeStruct(glo_v_out.shape, bf16),
            in_specs=[vmem, anywhere],
            out_specs=anywhere,
            scratch_shapes=[dma],
            input_output_aliases={1: 0},
            compiler_params=pltpu.CompilerParams(vmem_limit_bytes=16 * 2 ** 20),
            cost_estimate=pl.CostEstimate(flops=10 ** 6, bytes_accessed=4 * late_c.size, transcendentals=0),
        )(late_c, glo_v_out)
        return hidden_out, loc_k_out, loc_v_out, glo_k_out, glo_v_out

    return jax.shard_map(device_step, mesh=mesh, in_specs=in_specs, out_specs=out_specs, check_vma=False)
```

```python
import jax
import jax.numpy as jnp
import numpy as np
from jax import lax
from jax.experimental import pallas as pl
from jax.experimental.pallas import tpu as pltpu
from jax.sharding import PartitionSpec as P

SOFTCAP = 50.0
NORM_EPS = 1e-6
ROPE_BASE = 10000.0
WINDOW = 4096
CACHE_ROOM = 512

GROUP = 4
ROWS = 8
BLOCK = 1536
UNIT = 512
HEAD = 256
SEQ = GROUP * BLOCK
PER = BLOCK // UNIT
GLO_UNITS = SEQ // UNIT
LOC_UNITS = WINDOW // UNIT
FIRST_UNIT = (SEQ - WINDOW) // UNIT
STEPS = 4 * ROWS * PER
DEPTH = 2
LATE = (5, 4)
MESH = pl.DeviceIdType.MESH
PIECES = 8
WO_ROWS = 64
LAST = 256
FIRST = 16
STAT = 64
LOW = -1e30


def peers(me):
    return (me + 1 - 2 * (me % 2), (me + 2) % 4, 3 - me)


def norm(hidden, gain):
    mean_sq = jnp.mean(hidden * hidden, axis=-1, keepdims=True)
    return hidden * lax.rsqrt(mean_sq + NORM_EPS) * (1.0 + gain.astype(jnp.float32).reshape(1, -1))


def softcap(scores):
    return SOFTCAP * jnp.tanh(scores * (HEAD ** -0.5) / SOFTCAP)


def move_kernel(hid_in, trig_in, lpre_in, lpost_in, gpre_in, gpost_in, lk, lv, gk, gv, lwq, lwk, lwv, lwo, gwq, gwk, gwv, gwo,
                land_lk, land_lv, land_gk, land_gv, hid_out, new_out, late_a, late_b, late_c,
                hid, trig, lpre, lpost, gpre, gpost, new_kv, hid_end, wq, wk, wv, wo, kvbuf, qbuf, part, precv, pair, att, ybuf, hbuf, wo_far,
                bulk_send, loc_recv, glo_recv, w_sem, kv_sem, ex_send, ex_recv, late_sem, tail_send, small_sem, out_sem, first_sem, wo_send, wo_recv):
    dp = lax.axis_index("dp")
    me = lax.axis_index("a")
    dest = peers(me)
    caches = (lk, lv, gk, gv)
    lands = (land_lk, land_lv, land_gk, land_gv)

    first = [pltpu.make_async_copy(lk.at[0, dest[k], pl.ds(0, FIRST)], kvbuf.at[0, k - 1, pl.ds(0, FIRST)], first_sem.at[k - 1])
             for k in (1, 2)]

    @pl.when(me >= 2)
    def _():
        for copy in first:
            copy.start()

    barrier = pltpu.get_barrier_semaphore()
    for peer in dest:
        pl.semaphore_signal(barrier, inc=1, device_id=(dp, peer), device_id_type=MESH)
    pl.semaphore_wait(barrier, 3)

    def coords(step):
        c = step // (ROWS * PER) * (3 - 2 * (me // 2)) % 4
        return c, (step // PER) % ROWS, step % PER

    def valid(step, k):
        c, r, j = coords(step)
        in_window = jnp.logical_or(c >= 2, PER * me + j >= FIRST_UNIT)
        ok = jnp.logical_and(step >= 0, in_window)
        if k == 1:
            late = jnp.logical_and(jnp.logical_and(c == 3, r >= ROWS - LATE[0]), me >= 2)
            ok = jnp.logical_and(ok, jnp.logical_not(late))
        return ok

    def pump(step, opening=False):
        c, r, j = coords(step)
        slot = step % DEPTH
        for k in range(3):
            @pl.when(valid(step - DEPTH, k))
            def _():
                pltpu.make_async_remote_copy(
                    src_ref=gk.at[0, 0, pl.ds(0, UNIT)], dst_ref=land_gk.at[0, 0, pl.ds(0, UNIT)],
                    send_sem=bulk_send.at[k, slot], recv_sem=glo_recv.at[0, 0],
                    device_id=(dp, dest[k]), device_id_type=MESH).wait_send()
        def piece(s, ref):
            rows = pl.ds(pl.multiple_of(s % PIECES * WO_ROWS, WO_ROWS), WO_ROWS)
            return pltpu.make_async_remote_copy(
                src_ref=ref.at[rows], dst_ref=wo_far.at[s // PIECES, rows], send_sem=wo_send.at[s % DEPTH],
                recv_sem=wo_recv.at[s // PIECES], device_id=(dp, dest[1]), device_id_type=MESH)

        before = step - DEPTH

        @pl.when(jnp.logical_and(me < 2, jnp.logical_and(before >= 0, before < 2 * PIECES)))
        def _():
            piece(before, lwo).wait_send()

        for i, ref in enumerate((lwo, gwo)):
            @pl.when(jnp.logical_and(me < 2, jnp.logical_and(step >= i * PIECES, step < (i + 1) * PIECES)))
            def _():
                piece(step, ref).start()

        unit = PER * me + j
        for i in range(4):
            place = unit % LOC_UNITS if i < 2 else unit
            sem = loc_recv.at[i, place] if i < 2 else glo_recv.at[i - 2, place]
            for k in range(3):
                now = jnp.logical_and(c == i, valid(step, k))
                if opening and k:
                    now = jnp.logical_and(now, me < 2)

                @pl.when(now)
                def _():
                    pltpu.make_async_remote_copy(
                        src_ref=caches[i].at[r, dest[k], pl.ds(pl.multiple_of(j * UNIT, UNIT), UNIT)],
                        dst_ref=lands[i].at[r, 0, pl.ds(pl.multiple_of(place * UNIT, UNIT), UNIT)],
                        send_sem=bulk_send.at[k, slot], recv_sem=sem,
                        device_id=(dp, dest[k]), device_id_type=MESH).start()

    def send(index, k, src, dst):
        return pltpu.make_async_remote_copy(
            src_ref=src, dst_ref=dst, send_sem=ex_send.at[index], recv_sem=ex_recv.at[index],
            device_id=(dp, dest[k]), device_id_type=MESH)

    weights = [pltpu.make_async_copy(src, dst, w_sem.at[i]) for i, (src, dst) in enumerate((
        (lwq, wq.at[0]), (lwk, wk.at[0]), (lwv, wv.at[0]), (lwo, wo.at[0]),
        (gwq, wq.at[1]), (gwk, wk.at[1]), (gwv, wv.at[1]), (gwo, wo.at[1])))]

    small = [pltpu.make_async_copy(src, dst, small_sem.at[i]) for i, (src, dst) in enumerate((
        (hid_in, hid), (trig_in, trig), (lpre_in, lpre), (lpost_in, lpost),
        (gpre_in, gpre), (gpost_in, gpost)))]

    @pl.when(me >= 2)
    def _():
        place = (PER * me) % LOC_UNITS
        for k in (1, 2):
            first[k - 1].wait()
            pltpu.make_async_remote_copy(
                src_ref=kvbuf.at[0, k - 1, pl.ds(0, FIRST)],
                dst_ref=land_lk.at[0, 0, pl.ds(pl.multiple_of(place * UNIT, UNIT), FIRST)],
                send_sem=bulk_send.at[k, 0], recv_sem=loc_recv.at[0, place],
                device_id=(dp, dest[k]), device_id_type=MESH).start()
            pltpu.make_async_remote_copy(
                src_ref=lk.at[0, dest[k], pl.ds(FIRST, UNIT - FIRST)],
                dst_ref=land_lk.at[0, 0, pl.ds(pl.multiple_of(place * UNIT + FIRST, FIRST), UNIT - FIRST)],
                send_sem=bulk_send.at[k, 0], recv_sem=loc_recv.at[0, place],
                device_id=(dp, dest[k]), device_id_type=MESH).start()

    pump(0, opening=True)
    pump(1)
    for copy in small + weights:
        copy.start()
    for copy in small:
        copy.wait()

    cosine, sine = trig[0:1, :], trig[1:2, :]

    def rope(heads):
        first, second = heads[:, :HEAD // 2], heads[:, HEAD // 2:]
        return jnp.concatenate([first * cosine - second * sine, second * cosine + first * sine], axis=-1)

    def layer(index, hidden, key_ref, value_ref, pre, post, step):
        normed = norm(hidden, pre[...]).astype(jnp.bfloat16)
        if index == 0:
            for copy in weights[:4]:
                copy.wait()
        else:
            for copy in weights[4:]:
                copy.wait()
        q = jnp.dot(normed, wq[index], preferred_element_type=jnp.float32)
        q = jnp.concatenate([rope(q[:, :HEAD]), rope(q[:, HEAD:])], axis=0).astype(jnp.bfloat16)
        new_k = rope(jnp.dot(normed, wk[index], preferred_element_type=jnp.float32)).astype(jnp.bfloat16)
        new_v = jnp.dot(normed, wv[index], preferred_element_type=jnp.float32).astype(jnp.bfloat16)
        new_kv[2 * index] = new_k
        new_kv[2 * index + 1] = new_v
        own_q = qbuf.at[index]
        own_q[me] = q
        base = 8 * index
        near = send(base, 0, own_q.at[me], own_q.at[me])
        far = send(base + 1, 1, own_q.at[me], own_q.at[me])
        near.start()
        far.start()
        pump(step)
        far.wait()
        onward = send(base + 2, 0, own_q.at[dest[1]], own_q.at[dest[1]])
        onward.start()
        near.wait()
        onward.wait()

        def fetch(item, slot):
            h, r = item // ROWS, item % ROWS
            return (pltpu.make_async_copy(key_ref.at[r, h], kvbuf.at[slot, 0], kv_sem.at[slot, 0]),
                    pltpu.make_async_copy(value_ref.at[r, h], kvbuf.at[slot, 1], kv_sem.at[slot, 1]))

        for copy in fetch(0, 0):
            copy.start()
        items = GROUP * ROWS

        def body(item, carry):
            pump(step + 1 + item)
            slot = item % 2
            h, r = item // ROWS, item % ROWS

            @pl.when(item + 1 < items)
            def _():
                for copy in fetch(item + 1, 1 - slot):
                    copy.start()

            copy_k, copy_v = fetch(item, slot)
            copy_k.wait()
            scores = softcap(lax.dot_general(own_q[h], kvbuf[slot, 0], (((1,), (1,)), ((), ())),
                                             preferred_element_type=jnp.float32))
            if index == 0:
                place = me * BLOCK + lax.broadcasted_iota(jnp.int32, scores.shape, 1)
                inside = place > SEQ - WINDOW
                scores = jnp.where(inside, scores, LOW)
            top = jnp.max(scores, axis=-1, keepdims=True)
            e = jnp.exp(scores - top)
            if index == 0:
                e = jnp.where(inside, e, 0.0)
            total = jnp.sum(e, axis=-1, keepdims=True)
            copy_v.wait()
            out = jnp.dot(e.astype(jnp.bfloat16), kvbuf[slot, 1], preferred_element_type=jnp.float32)
            wide = jnp.concatenate([out, jnp.broadcast_to(top, (2 * ROWS, STAT)),
                                    jnp.broadcast_to(total, (2 * ROWS, STAT))], axis=-1)
            row = lax.broadcasted_iota(jnp.int32, wide.shape, 0) % ROWS
            part[index, h] = jnp.where(row == r, wide, part[index, h])
            return carry

        lax.fori_loop(0, items, body, 0)
        step = step + 1 + items

        mine = part.at[index]
        theirs = precv.at[index]
        near = (send(base + 3, 0, mine.at[dest[0]], theirs.at[0]), send(base + 4, 0, mine.at[dest[2]], theirs.at[1]))
        for copy in near:
            copy.start()
        new_k2 = jnp.concatenate([new_k, new_k], axis=0).astype(jnp.float32)
        new_v2 = jnp.concatenate([new_v, new_v], axis=0).astype(jnp.float32)
        new_s = softcap(jnp.sum(q.astype(jnp.float32) * new_k2, axis=-1, keepdims=True))
        new = (new_v2, new_s, jnp.ones_like(new_s))
        for copy in near:
            copy.wait()

        def split(block):
            return block[:, :HEAD], block[:, HEAD:HEAD + 1], block[:, HEAD + STAT:HEAD + STAT + 1]

        def merge(blocks):
            top = blocks[0][1]
            for _, m, _ in blocks[1:]:
                top = jnp.maximum(top, m)
            acc, total = 0.0, 0.0
            for o, m, l in blocks:
                scale = jnp.exp(m - top)
                acc = acc + scale * o
                total = total + scale * l
            return acc, top, total

        def packed(acc, top, total):
            return jnp.concatenate([acc, jnp.broadcast_to(top, (2 * ROWS, STAT)),
                                    jnp.broadcast_to(total, (2 * ROWS, STAT))], axis=-1)

        both = [split(mine[me]), split(theirs[0]), new]
        across = pair.at[index]
        across[0] = packed(*merge([split(mine[dest[1]]), split(theirs[1])]))
        across[1] = packed(*merge(both))
        heads = att.at[index]
        far = [send(base + 5 + i, 1, across.at[i], theirs.at[2 + i]) for i in (0, 1)]
        y_ref = ybuf.at[index]
        half = hbuf.at[index]
        side = me % 2
        near = send(base + 7, 0, y_ref.at[side], y_ref.at[side])
        back = send(16 + 2 * index, 1, half.at[side], half.at[side])
        swap = send(17 + 2 * index, 0, half.at[side], half.at[side])

        @pl.when(me < 2)
        def _():
            for copy in far:
                copy.start()

        pump(step)

        @pl.when(me >= 2)
        def _():
            for copy in far:
                copy.wait_recv()

            def finished(blocks):
                acc, _, total = merge(blocks)
                out = (acc / total).astype(jnp.bfloat16)
                return jnp.concatenate([out[:ROWS], out[ROWS:]], axis=-1)

            heads[0] = finished(both + [split(theirs[2])])
            heads[1] = finished([split(across[0]), split(theirs[3])])

        pump(step + 1)

        @pl.when(me >= 2)
        def _():
            pltpu.make_async_remote_copy(
                src_ref=wo_far.at[index], dst_ref=wo_far.at[index], send_sem=wo_send.at[0], recv_sem=wo_recv.at[index],
                device_id=(dp, dest[1]), device_id_type=MESH).wait_recv()
            y_ref[side] = (jnp.dot(heads[0], wo[index], preferred_element_type=jnp.float32)
                           + jnp.dot(heads[1], wo_far[index], preferred_element_type=jnp.float32))
            near.start()
            near.wait()
            after = (hidden + norm(y_ref[0] + y_ref[1], post[...])).astype(jnp.bfloat16)
            half[0] = after[:, :after.shape[1] // 2]
            half[1] = after[:, after.shape[1] // 2:]
            back.start()

        pump(step + 2)

        @pl.when(me >= 2)
        def _():
            back.wait_send()

        @pl.when(me < 2)
        def _():
            for copy in far:
                copy.wait_send()
            back.wait_recv()
            swap.start()
            swap.wait()

        return jnp.concatenate([half[0], half[1]], axis=-1), step + 3

    part[...] = jnp.zeros_like(part)
    hidden, step = layer(0, hid[...].astype(jnp.float32), lk, lv, lpre, lpost, 2)
    hidden, step = layer(1, hidden.astype(jnp.float32), gk, gv, gpre, gpost, step)
    hid_end[...] = hidden
    outs = (pltpu.make_async_copy(hid_end, hid_out, out_sem.at[0]), pltpu.make_async_copy(new_kv, new_out, out_sem.at[1]))
    for copy in outs:
        copy.start()
    for copy in outs:
        copy.wait()

    for late, target, rows in ((late_a, 0, LATE[0]), (late_b, 1, LATE[1])):
        @pl.when(me == target + 2)
        def _():
            def late_in(r):
                return pltpu.make_async_copy(gv.at[ROWS - rows + r, target], kvbuf.at[(r // 2) % 2, r % 2], late_sem.at[0, r])

            def late_out(r):
                buf, size = kvbuf.at[(r // 2) % 2, r % 2], BLOCK if r < rows - 1 else BLOCK - LAST
                return pltpu.make_async_copy(buf.at[pl.ds(0, size)], late.at[pl.ds(r * BLOCK, size)], late_sem.at[1, r])

            end = kvbuf.at[((rows - 1) // 2) % 2, (rows - 1) % 2, pl.ds(BLOCK - LAST, LAST)]
            last_out = pltpu.make_async_copy(end, late_c, late_sem.at[0, rows - 1])
            for r in range(rows):
                if r >= 4:
                    late_out(r - 4).wait()
                late_in(r).start()
                if r >= 1:
                    late_in(r - 1).wait()
                    late_out(r - 1).start()
            late_in(rows - 1).wait()
            late_out(rows - 1).start()
            last_out.start()
            for r in range(max(rows - 4, 0), rows):
                late_out(r).wait()
            last_out.wait()

    def rest(s, carry):
        pump(s)
        return carry

    lax.fori_loop(step, STEPS, rest, 0)

    def tail(r, j):
        unit = PER * me + j
        return pltpu.make_async_remote_copy(
            src_ref=gv.at[r, dest[1], pl.ds(j * UNIT, UNIT)],
            dst_ref=land_gv.at[r, 0, pl.ds(pl.multiple_of(unit * UNIT, UNIT), UNIT)],
            send_sem=tail_send.at[r - ROWS + LATE[0], j], recv_sem=glo_recv.at[1, unit],
            device_id=(dp, dest[1]), device_id_type=MESH)

    tails = [(r, j) for r in range(ROWS - LATE[0], ROWS - LATE[1]) for j in range(PER)]

    @pl.when(me == 3)
    def _():
        for piece in tails:
            tail(*piece).start()

    for s in range(STEPS - DEPTH, STEPS):
        for k in range(3):
            @pl.when(valid(s, k))
            def _():
                pltpu.make_async_remote_copy(
                    src_ref=gk.at[0, 0, pl.ds(0, UNIT)], dst_ref=land_gk.at[0, 0, pl.ds(0, UNIT)],
                    send_sem=bulk_send.at[k, s % DEPTH], recv_sem=glo_recv.at[0, 0],
                    device_id=(dp, dest[k]), device_id_type=MESH).wait_send()

    @pl.when(me == 3)
    def _():
        for piece in tails:
            tail(*piece).wait_send()

    for i in range(4):
        for u in range(LOC_UNITS if i < 2 else GLO_UNITS):
            owner = (u if i >= 2 or u >= FIRST_UNIT else u + LOC_UNITS) // PER
            sem = loc_recv.at[i, u] if i < 2 else glo_recv.at[i - 2, u]

            def await_rows(rows):
                view = lands[i].at[pl.ds(0, rows), :, pl.ds(u * UNIT, UNIT)]
                pltpu.make_async_remote_copy(
                    src_ref=view, dst_ref=view, send_sem=bulk_send.at[0, 0], recv_sem=sem,
                    device_id=(dp, dest[0]), device_id_type=MESH).wait_recv()

            if i == 3 and owner >= 2:
                short = me == owner - 2

                @pl.when(short)
                def _():
                    await_rows(ROWS - LATE[owner - 2])

                @pl.when(jnp.logical_and(me != owner, jnp.logical_not(short)))
                def _():
                    await_rows(ROWS)
            else:
                @pl.when(me != owner)
                def _():
                    await_rows(ROWS)


SLOTS = 6


def write_kernel(hid, new_kv, lk, lv, gk, gv, land_lk, land_lv, land_gk, land_gv,
                 hid_out, lk_out, lv_out, gk_out, gv_out, buf, in_sem, out_sem):
    me = lax.axis_index("a")
    hid_out[...] = hid[...]
    jobs = []
    for i in range(4):
        for u in range(LOC_UNITS if i < 2 else GLO_UNITS + 1):
            jobs.append((i, u))
    caches = (lk, lv, gk, gv)
    lands = (land_lk, land_lv, land_gk, land_gv)
    outs = (lk_out, lv_out, gk_out, gv_out)

    def load(n):
        i, u = jobs[n]
        slot = n % SLOTS
        if i >= 2 and u == GLO_UNITS:
            return
        full = u if i >= 2 or u >= FIRST_UNIT else u + LOC_UNITS
        owner, j = full // PER, full % PER

        @pl.when(me == owner)
        def _():
            pltpu.make_async_copy(caches[i].at[:, owner, pl.ds(j * UNIT, UNIT)], buf.at[slot], in_sem.at[slot]).start()

        @pl.when(me != owner)
        def _():
            pltpu.make_async_copy(lands[i].at[:, 0, pl.ds(u * UNIT, UNIT)], buf.at[slot], in_sem.at[slot]).start()

    def store(n):
        i, u = jobs[n]
        slot = n % SLOTS
        return pltpu.make_async_copy(buf.at[slot], outs[i].at[:, 0, pl.ds(u * UNIT, UNIT)], out_sem.at[slot])

    ahead = SLOTS // 2
    for n in range(ahead):
        load(n)
    for n, (i, u) in enumerate(jobs):
        slot = n % SLOTS
        if n + ahead < len(jobs):
            if n + ahead >= SLOTS:
                store(n + ahead - SLOTS).wait()
            load(n + ahead)
        pad = i >= 2 and u == GLO_UNITS
        if not pad:
            pltpu.make_async_copy(lands[i].at[:, 0, pl.ds(0, UNIT)], buf.at[slot], in_sem.at[slot]).wait()
        else:
            buf[slot] = jnp.zeros((ROWS, UNIT, HEAD), jnp.bfloat16)
        if pad or (i < 2 and u == SEQ % WINDOW // UNIT):
            head = buf[slot, :, 0:16, :].astype(jnp.float32)
            first = lax.broadcasted_iota(jnp.int32, head.shape, 1) == 0
            new = jnp.broadcast_to(new_kv[i].astype(jnp.float32)[:, None, :], head.shape)
            buf[slot, :, 0:16, :] = jnp.where(first, new, head).astype(jnp.bfloat16)
        store(n).start()
    for n in range(len(jobs) - SLOTS, len(jobs)):
        store(n).wait()


def late_kernel(late_a, late_b, old, out, sem):
    me = lax.axis_index("a")
    for target, late in enumerate((late_a, late_b)):
        @pl.when(me == target)
        def _():
            copies = []
            for r in range(LATE[target]):
                size = BLOCK if r < LATE[target] - 1 else BLOCK - LAST
                copies.append(pltpu.make_async_copy(
                    late.at[pl.ds(r * BLOCK, size)],
                    out.at[ROWS - LATE[target] + r, 0, pl.ds((target + 2) * BLOCK, size)], sem.at[r]))
            for copy in copies:
                copy.start()
            for copy in copies:
                copy.wait()


def last_kernel(late_c, old, out, sem):
    me = lax.axis_index("a")

    @pl.when(me < 2)
    def _():
        place = pl.multiple_of((me + 3) * BLOCK - LAST, LAST)
        copy = pltpu.make_async_copy(late_c, out.at[ROWS - 1, 0, pl.ds(place, LAST)], sem)
        copy.start()
        copy.wait()


def trig_table():
    half = HEAD // 2
    inv_freq = ROPE_BASE ** (-2.0 * np.arange(half) / HEAD)
    angles = SEQ * inv_freq
    return np.stack([np.cos(angles), np.sin(angles)]).astype(np.float32)


def solution(mesh):
    cache_in = P('dp', None, 'a', None)
    cache_out = P('dp', 'a', None, None)
    rows_spec = P('dp', None)
    layer_specs = (P(None, 'a'), P(None, 'a'), P(None, 'a'), P('a', None), P(None), P(None))
    in_specs = (rows_spec, cache_in, cache_in, cache_in, cache_in) + layer_specs + layer_specs
    out_specs = (rows_spec, cache_out, cache_out, cache_out, cache_out)
    bf16, f32 = jnp.bfloat16, jnp.float32
    anywhere = pl.BlockSpec(memory_space=pl.ANY)
    vmem = pl.BlockSpec(memory_space=pltpu.VMEM)

    def device_step(hidden_in, loc_k, loc_v, glo_k, glo_v, loc_wq, loc_wk, loc_wv, loc_wo, loc_pre, loc_post, glo_wq, glo_wk, glo_wv, glo_wo, glo_pre, glo_post):
        model = hidden_in.shape[1]
        gains = [loc_pre, loc_post, glo_pre, glo_post]
        loc_land = jax.ShapeDtypeStruct((ROWS, 1, WINDOW, HEAD), bf16)
        glo_land = jax.ShapeDtypeStruct((ROWS, 1, SEQ, HEAD), bf16)
        dma = pltpu.SemaphoreType.DMA
        moved = pl.pallas_call(
            move_kernel,
            out_shape=(loc_land, loc_land, glo_land, glo_land,
                       jax.ShapeDtypeStruct((ROWS, model), bf16), jax.ShapeDtypeStruct((4, ROWS, HEAD), bf16),
                       jax.ShapeDtypeStruct((LATE[0] * BLOCK - LAST, HEAD), bf16),
                       jax.ShapeDtypeStruct((LATE[1] * BLOCK - LAST, HEAD), bf16), jax.ShapeDtypeStruct((LAST, HEAD), bf16)),
            in_specs=[anywhere] * 18,
            out_specs=(anywhere,) * 9,
            scratch_shapes=[
                pltpu.VMEM((ROWS, model), bf16), pltpu.VMEM((2, HEAD // 2), f32),
                pltpu.VMEM((model,), bf16), pltpu.VMEM((model,), bf16), pltpu.VMEM((model,), bf16), pltpu.VMEM((model,), bf16),
                pltpu.VMEM((4, ROWS, HEAD), bf16), pltpu.VMEM((ROWS, model), bf16),
                pltpu.VMEM((2,) + loc_wq.shape, bf16), pltpu.VMEM((2,) + loc_wk.shape, bf16),
                pltpu.VMEM((2,) + loc_wv.shape, bf16), pltpu.VMEM((2,) + loc_wo.shape, bf16),
                pltpu.VMEM((2, 2, BLOCK, HEAD), bf16),
                pltpu.VMEM((2, GROUP, 2 * ROWS, HEAD), bf16),
                pltpu.VMEM((2, GROUP, 2 * ROWS, HEAD + 2 * STAT), f32),
                pltpu.VMEM((2, 4, 2 * ROWS, HEAD + 2 * STAT), f32),
                pltpu.VMEM((2, 2, 2 * ROWS, HEAD + 2 * STAT), f32),
                pltpu.VMEM((2, 2, ROWS, 2 * HEAD), bf16),
                pltpu.VMEM((2, 2, ROWS, model), f32), pltpu.VMEM((2, 2, ROWS, model // 2), bf16),
                pltpu.VMEM((2,) + loc_wo.shape, bf16),
                dma((3, DEPTH)), dma((2, LOC_UNITS)), dma((2, GLO_UNITS)), dma((8,)), dma((2, 2)),
                dma((20,)), dma((20,)), dma((2, LATE[0])),
                dma((LATE[0] - LATE[1], PER)), dma((6,)), dma((2,)), dma((2,)), dma((DEPTH,)), dma((2,))],
            compiler_params=pltpu.CompilerParams(collective_id=0, has_side_effects=True),
        )(hidden_in, jnp.asarray(trig_table()), *gains, loc_k, loc_v, glo_k, glo_v,
          loc_wq, loc_wk, loc_wv, loc_wo, glo_wq, glo_wk, glo_wv, glo_wo)
        land, hid, new_kv = moved[:4], moved[4], moved[5]
        late_a = lax.ppermute(moved[6], 'a', [(2, 0)])
        late_b = lax.ppermute(moved[7], 'a', [(3, 1)])
        late_c = lax.ppermute(moved[8], 'a', [(2, 0), (3, 1)])
        hidden_out, loc_k_out, loc_v_out, glo_k_out, glo_v_out = pl.pallas_call(
            write_kernel,
            out_shape=(jax.ShapeDtypeStruct((ROWS, model), bf16),)
            + (jax.ShapeDtypeStruct((ROWS, 1, WINDOW, HEAD), bf16),) * 2
            + (jax.ShapeDtypeStruct((ROWS, 1, SEQ + CACHE_ROOM, HEAD), bf16),) * 2,
            in_specs=[vmem, vmem] + [anywhere] * 8,
            out_specs=(vmem,) + (anywhere,) * 4,
            scratch_shapes=[pltpu.VMEM((SLOTS, ROWS, UNIT, HEAD), bf16), dma((SLOTS,)), dma((SLOTS,))],
            compiler_params=pltpu.CompilerParams(vmem_limit_bytes=50 * 2 ** 20),
            cost_estimate=pl.CostEstimate(flops=10 ** 9, bytes_accessed=180 * 10 ** 6, transcendentals=0),
        )(hid, new_kv, loc_k, loc_v, glo_k, glo_v, *land)
        glo_v_out = pl.pallas_call(
            late_kernel,
            out_shape=jax.ShapeDtypeStruct(glo_v_out.shape, bf16),
            in_specs=[vmem, vmem, anywhere],
            out_specs=anywhere,
            scratch_shapes=[dma((LATE[0],))],
            input_output_aliases={2: 0},
            compiler_params=pltpu.CompilerParams(vmem_limit_bytes=16 * 2 ** 20),
            cost_estimate=pl.CostEstimate(flops=10 ** 7, bytes_accessed=4 * late_a.size, transcendentals=0),
        )(late_a, late_b, glo_v_out)
        glo_v_out = pl.pallas_call(
            last_kernel,
            out_shape=jax.ShapeDtypeStruct(glo_v_out.shape, bf16),
            in_specs=[vmem, anywhere],
            out_specs=anywhere,
            scratch_shapes=[dma],
            input_output_aliases={1: 0},
            compiler_params=pltpu.CompilerParams(vmem_limit_bytes=16 * 2 ** 20),
            cost_estimate=pl.CostEstimate(flops=10 ** 6, bytes_accessed=4 * late_c.size, transcendentals=0),
        )(late_c, glo_v_out)
        return hidden_out, loc_k_out, loc_v_out, glo_k_out, glo_v_out

    return jax.shard_map(device_step, mesh=mesh, in_specs=in_specs, out_specs=out_specs, check_vma=False)
```

```python
import jax
import jax.numpy as jnp
import numpy as np
from jax import lax
from jax.experimental import pallas as pl
from jax.experimental.pallas import tpu as pltpu
from jax.sharding import PartitionSpec as P

SOFTCAP = 50.0
NORM_EPS = 1e-6
ROPE_BASE = 10000.0
WINDOW = 4096
CACHE_ROOM = 512

GROUP = 4
ROWS = 8
BLOCK = 1536
UNIT = 512
HEAD = 256
SEQ = GROUP * BLOCK
PER = BLOCK // UNIT
GLO_UNITS = SEQ // UNIT
LOC_UNITS = WINDOW // UNIT
FIRST_UNIT = (SEQ - WINDOW) // UNIT
STEPS = 4 * ROWS * PER
DEPTH = 2
LATE = (5, 4)
MESH = pl.DeviceIdType.MESH
PIECES = 8
WO_ROWS = 64
LAST = 256
FIRST = 16
STAT = 64
LOW = -1e30


def peers(me):
    return (me + 1 - 2 * (me % 2), (me + 2) % 4, 3 - me)


def norm(hidden, gain):
    mean_sq = jnp.mean(hidden * hidden, axis=-1, keepdims=True)
    return hidden * lax.rsqrt(mean_sq + NORM_EPS) * (1.0 + gain.astype(jnp.float32).reshape(1, -1))


def softcap(scores):
    return SOFTCAP * jnp.tanh(scores * (HEAD ** -0.5) / SOFTCAP)


def move_kernel(hid_in, trig_in, lpre_in, lpost_in, gpre_in, gpost_in, lk, lv, gk, gv, lwq, lwk, lwv, lwo, gwq, gwk, gwv, gwo,
                land_lk, land_lv, land_gk, land_gv, hid_out, new_out, late_a, late_b, late_c,
                hid, trig, lpre, lpost, gpre, gpost, new_kv, hid_end, wq, wk, wv, wo, kvbuf, qbuf, part, precv, pair, att, ybuf, hbuf, wo_far,
                bulk_send, loc_recv, glo_recv, w_sem, kv_sem, ex_send, ex_recv, late_sem, tail_send, small_sem, out_sem, first_sem, wo_send, wo_recv):
    dp = lax.axis_index("dp")
    me = lax.axis_index("a")
    dest = peers(me)
    caches = (lk, lv, gk, gv)
    lands = (land_lk, land_lv, land_gk, land_gv)

    first = [pltpu.make_async_copy(lk.at[0, dest[k], pl.ds(0, FIRST)], kvbuf.at[0, k - 1, pl.ds(0, FIRST)], first_sem.at[k - 1])
             for k in (1, 2)]

    @pl.when(me >= 2)
    def _():
        for copy in first:
            copy.start()

    barrier = pltpu.get_barrier_semaphore()
    for peer in dest:
        pl.semaphore_signal(barrier, inc=1, device_id=(dp, peer), device_id_type=MESH)
    pl.semaphore_wait(barrier, 3)

    def coords(step):
        c = step // (ROWS * PER) * (3 - 2 * (me // 2)) % 4
        return c, (step // PER) % ROWS, step % PER

    def valid(step, k):
        c, r, j = coords(step)
        in_window = jnp.logical_or(c >= 2, PER * me + j >= FIRST_UNIT)
        ok = jnp.logical_and(step >= 0, in_window)
        if k == 1:
            late = jnp.logical_and(jnp.logical_and(c == 3, r >= ROWS - LATE[0]), me >= 2)
            ok = jnp.logical_and(ok, jnp.logical_not(late))
        return ok

    def pump(step, opening=False):
        c, r, j = coords(step)
        slot = step % DEPTH
        for k in range(3):
            @pl.when(valid(step - DEPTH, k))
            def _():
                pltpu.make_async_remote_copy(
                    src_ref=gk.at[0, 0, pl.ds(0, UNIT)], dst_ref=land_gk.at[0, 0, pl.ds(0, UNIT)],
                    send_sem=bulk_send.at[k, slot], recv_sem=glo_recv.at[0, 0],
                    device_id=(dp, dest[k]), device_id_type=MESH).wait_send()
        def piece(s, ref):
            rows = pl.ds(pl.multiple_of(s % PIECES * WO_ROWS, WO_ROWS), WO_ROWS)
            return pltpu.make_async_remote_copy(
                src_ref=ref.at[rows], dst_ref=wo_far.at[s // PIECES, rows], send_sem=wo_send.at[s % DEPTH],
                recv_sem=wo_recv.at[s // PIECES], device_id=(dp, dest[1]), device_id_type=MESH)

        before = step - DEPTH

        @pl.when(jnp.logical_and(me < 2, jnp.logical_and(before >= 0, before < 2 * PIECES)))
        def _():
            piece(before, lwo).wait_send()

        for i, ref in enumerate((lwo, gwo)):
            @pl.when(jnp.logical_and(me < 2, jnp.logical_and(step >= i * PIECES, step < (i + 1) * PIECES)))
            def _():
                piece(step, ref).start()

        unit = PER * me + j
        for i in range(4):
            place = unit % LOC_UNITS if i < 2 else unit
            sem = loc_recv.at[i, place] if i < 2 else glo_recv.at[i - 2, place]
            for k in range(3):
                now = jnp.logical_and(c == i, valid(step, k))
                if opening and k:
                    now = jnp.logical_and(now, me < 2)

                @pl.when(now)
                def _():
                    pltpu.make_async_remote_copy(
                        src_ref=caches[i].at[r, dest[k], pl.ds(pl.multiple_of(j * UNIT, UNIT), UNIT)],
                        dst_ref=lands[i].at[r, 0, pl.ds(pl.multiple_of(place * UNIT, UNIT), UNIT)],
                        send_sem=bulk_send.at[k, slot], recv_sem=sem,
                        device_id=(dp, dest[k]), device_id_type=MESH).start()

    def send(index, k, src, dst):
        return pltpu.make_async_remote_copy(
            src_ref=src, dst_ref=dst, send_sem=ex_send.at[index], recv_sem=ex_recv.at[index],
            device_id=(dp, dest[k]), device_id_type=MESH)

    weights = [pltpu.make_async_copy(src, dst, w_sem.at[i]) for i, (src, dst) in enumerate((
        (lwq, wq.at[0]), (lwk, wk.at[0]), (lwv, wv.at[0]), (lwo, wo.at[0]),
        (gwq, wq.at[1]), (gwk, wk.at[1]), (gwv, wv.at[1]), (gwo, wo.at[1])))]

    small = [pltpu.make_async_copy(src, dst, small_sem.at[i]) for i, (src, dst) in enumerate((
        (hid_in, hid), (trig_in, trig), (lpre_in, lpre), (lpost_in, lpost),
        (gpre_in, gpre), (gpost_in, gpost)))]

    @pl.when(me >= 2)
    def _():
        place = (PER * me) % LOC_UNITS
        for k in (1, 2):
            first[k - 1].wait()
            pltpu.make_async_remote_copy(
                src_ref=kvbuf.at[0, k - 1, pl.ds(0, FIRST)],
                dst_ref=land_lk.at[0, 0, pl.ds(pl.multiple_of(place * UNIT, UNIT), FIRST)],
                send_sem=bulk_send.at[k, 0], recv_sem=loc_recv.at[0, place],
                device_id=(dp, dest[k]), device_id_type=MESH).start()
            pltpu.make_async_remote_copy(
                src_ref=lk.at[0, dest[k], pl.ds(FIRST, UNIT - FIRST)],
                dst_ref=land_lk.at[0, 0, pl.ds(pl.multiple_of(place * UNIT + FIRST, FIRST), UNIT - FIRST)],
                send_sem=bulk_send.at[k, 0], recv_sem=loc_recv.at[0, place],
                device_id=(dp, dest[k]), device_id_type=MESH).start()

    pump(0, opening=True)
    pump(1)
    for copy in small + weights:
        copy.start()
    for copy in small:
        copy.wait()

    cosine, sine = trig[0:1, :], trig[1:2, :]

    def rope(heads):
        first, second = heads[:, :HEAD // 2], heads[:, HEAD // 2:]
        return jnp.concatenate([first * cosine - second * sine, second * cosine + first * sine], axis=-1)

    def layer(index, hidden, key_ref, value_ref, pre, post, step):
        normed = norm(hidden, pre[...]).astype(jnp.bfloat16)
        if index == 0:
            for copy in weights[:4]:
                copy.wait()
        else:
            for copy in weights[4:]:
                copy.wait()
        q = jnp.dot(normed, wq[index], preferred_element_type=jnp.float32)
        q = jnp.concatenate([rope(q[:, :HEAD]), rope(q[:, HEAD:])], axis=0).astype(jnp.bfloat16)
        new_k = rope(jnp.dot(normed, wk[index], preferred_element_type=jnp.float32)).astype(jnp.bfloat16)
        new_v = jnp.dot(normed, wv[index], preferred_element_type=jnp.float32).astype(jnp.bfloat16)
        new_kv[2 * index] = new_k
        new_kv[2 * index + 1] = new_v
        own_q = qbuf.at[index]
        own_q[me] = q
        base = 8 * index
        near = send(base, 0, own_q.at[me], own_q.at[me])
        far = send(base + 1, 1, own_q.at[me], own_q.at[me])
        near.start()
        far.start()
        pump(step)
        far.wait()
        onward = send(base + 2, 0, own_q.at[dest[1]], own_q.at[dest[1]])
        onward.start()
        near.wait()
        onward.wait()

        def fetch(item, slot):
            h, r = item // ROWS, item % ROWS
            return (pltpu.make_async_copy(key_ref.at[r, h], kvbuf.at[slot, 0], kv_sem.at[slot, 0]),
                    pltpu.make_async_copy(value_ref.at[r, h], kvbuf.at[slot, 1], kv_sem.at[slot, 1]))

        for copy in fetch(0, 0):
            copy.start()
        items = GROUP * ROWS

        def body(item, carry):
            pump(step + 1 + item)
            slot = item % 2
            h, r = item // ROWS, item % ROWS

            @pl.when(item + 1 < items)
            def _():
                for copy in fetch(item + 1, 1 - slot):
                    copy.start()

            copy_k, copy_v = fetch(item, slot)
            copy_k.wait()
            scores = softcap(lax.dot_general(own_q[h], kvbuf[slot, 0], (((1,), (1,)), ((), ())),
                                             preferred_element_type=jnp.float32))
            if index == 0:
                place = me * BLOCK + lax.broadcasted_iota(jnp.int32, scores.shape, 1)
                inside = place > SEQ - WINDOW
                scores = jnp.where(inside, scores, LOW)
            top = jnp.max(scores, axis=-1, keepdims=True)
            e = jnp.exp(scores - top)
            if index == 0:
                e = jnp.where(inside, e, 0.0)
            total = jnp.sum(e, axis=-1, keepdims=True)
            copy_v.wait()
            out = jnp.dot(e.astype(jnp.bfloat16), kvbuf[slot, 1], preferred_element_type=jnp.float32)
            wide = jnp.concatenate([out, jnp.broadcast_to(top, (2 * ROWS, STAT)),
                                    jnp.broadcast_to(total, (2 * ROWS, STAT))], axis=-1)
            row = lax.broadcasted_iota(jnp.int32, wide.shape, 0) % ROWS
            part[index, h] = jnp.where(row == r, wide, part[index, h])
            return carry

        lax.fori_loop(0, items, body, 0)
        step = step + 1 + items

        mine = part.at[index]
        theirs = precv.at[index]
        near = (send(base + 3, 0, mine.at[dest[0]], theirs.at[0]), send(base + 4, 0, mine.at[dest[2]], theirs.at[1]))
        for copy in near:
            copy.start()
        new_k2 = jnp.concatenate([new_k, new_k], axis=0).astype(jnp.float32)
        new_v2 = jnp.concatenate([new_v, new_v], axis=0).astype(jnp.float32)
        new_s = softcap(jnp.sum(q.astype(jnp.float32) * new_k2, axis=-1, keepdims=True))
        new = (new_v2, new_s, jnp.ones_like(new_s))
        for copy in near:
            copy.wait()

        def split(block):
            return block[:, :HEAD], block[:, HEAD:HEAD + 1], block[:, HEAD + STAT:HEAD + STAT + 1]

        def merge(blocks):
            top = blocks[0][1]
            for _, m, _ in blocks[1:]:
                top = jnp.maximum(top, m)
            acc, total = 0.0, 0.0
            for o, m, l in blocks:
                scale = jnp.exp(m - top)
                acc = acc + scale * o
                total = total + scale * l
            return acc, top, total

        def packed(acc, top, total):
            return jnp.concatenate([acc, jnp.broadcast_to(top, (2 * ROWS, STAT)),
                                    jnp.broadcast_to(total, (2 * ROWS, STAT))], axis=-1)

        both = [split(mine[me]), split(theirs[0]), new]
        across = pair.at[index]
        across[0] = packed(*merge([split(mine[dest[1]]), split(theirs[1])]))
        across[1] = packed(*merge(both))
        heads = att.at[index]
        far = [send(base + 5 + i, 1, across.at[i], theirs.at[2 + i]) for i in (0, 1)]
        y_ref = ybuf.at[index]
        half = hbuf.at[index]
        side = me % 2
        near = send(base + 7, 0, y_ref.at[side], y_ref.at[side])
        back = send(16 + 2 * index, 1, half.at[side], half.at[side])
        swap = send(17 + 2 * index, 0, half.at[side], half.at[side])

        @pl.when(me < 2)
        def _():
            for copy in far:
                copy.start()

        pump(step)

        @pl.when(me >= 2)
        def _():
            for copy in far:
                copy.wait_recv()

            def finished(blocks):
                acc, _, total = merge(blocks)
                out = (acc / total).astype(jnp.bfloat16)
                return jnp.concatenate([out[:ROWS], out[ROWS:]], axis=-1)

            heads[0] = finished(both + [split(theirs[2])])
            heads[1] = finished([split(across[0]), split(theirs[3])])

        pump(step + 1)

        @pl.when(me >= 2)
        def _():
            pltpu.make_async_remote_copy(
                src_ref=wo_far.at[index], dst_ref=wo_far.at[index], send_sem=wo_send.at[0], recv_sem=wo_recv.at[index],
                device_id=(dp, dest[1]), device_id_type=MESH).wait_recv()
            y_ref[side] = (jnp.dot(heads[0], wo[index], preferred_element_type=jnp.float32)
                           + jnp.dot(heads[1], wo_far[index], preferred_element_type=jnp.float32))
            near.start()
            near.wait()
            after = (hidden + norm(y_ref[0] + y_ref[1], post[...])).astype(jnp.bfloat16)
            half[0] = after[:, :after.shape[1] // 2]
            half[1] = after[:, after.shape[1] // 2:]
            back.start()

        pump(step + 2)

        @pl.when(me >= 2)
        def _():
            back.wait_send()

        @pl.when(me < 2)
        def _():
            for copy in far:
                copy.wait_send()
            back.wait_recv()
            swap.start()
            swap.wait()

        return jnp.concatenate([half[0], half[1]], axis=-1), step + 3

    part[...] = jnp.zeros_like(part)
    hidden, step = layer(0, hid[...].astype(jnp.float32), lk, lv, lpre, lpost, 2)
    hidden, step = layer(1, hidden.astype(jnp.float32), gk, gv, gpre, gpost, step)
    hid_end[...] = hidden
    outs = (pltpu.make_async_copy(hid_end, hid_out, out_sem.at[0]), pltpu.make_async_copy(new_kv, new_out, out_sem.at[1]))
    for copy in outs:
        copy.start()
    for copy in outs:
        copy.wait()

    for late, target, rows in ((late_a, 0, LATE[0]), (late_b, 1, LATE[1])):
        @pl.when(me == target + 2)
        def _():
            def late_in(r):
                return pltpu.make_async_copy(gv.at[ROWS - rows + r, target], kvbuf.at[(r // 2) % 2, r % 2], late_sem.at[0, r])

            def late_out(r):
                buf, size = kvbuf.at[(r // 2) % 2, r % 2], BLOCK if r < rows - 1 else BLOCK - LAST
                return pltpu.make_async_copy(buf.at[pl.ds(0, size)], late.at[pl.ds(r * BLOCK, size)], late_sem.at[1, r])

            end = kvbuf.at[((rows - 1) // 2) % 2, (rows - 1) % 2, pl.ds(BLOCK - LAST, LAST)]
            last_out = pltpu.make_async_copy(end, late_c, late_sem.at[0, rows - 1])
            for r in range(rows):
                if r >= 4:
                    late_out(r - 4).wait()
                late_in(r).start()
                if r >= 1:
                    late_in(r - 1).wait()
                    late_out(r - 1).start()
            late_in(rows - 1).wait()
            late_out(rows - 1).start()
            last_out.start()
            for r in range(max(rows - 4, 0), rows):
                late_out(r).wait()
            last_out.wait()

    def rest(s, carry):
        pump(s)
        return carry

    lax.fori_loop(step, STEPS, rest, 0)

    def tail(r, j):
        unit = PER * me + j
        return pltpu.make_async_remote_copy(
            src_ref=gv.at[r, dest[1], pl.ds(j * UNIT, UNIT)],
            dst_ref=land_gv.at[r, 0, pl.ds(pl.multiple_of(unit * UNIT, UNIT), UNIT)],
            send_sem=tail_send.at[r - ROWS + LATE[0], j], recv_sem=glo_recv.at[1, unit],
            device_id=(dp, dest[1]), device_id_type=MESH)

    tails = [(r, j) for r in range(ROWS - LATE[0], ROWS - LATE[1]) for j in range(PER)]

    @pl.when(me == 3)
    def _():
        for piece in tails:
            tail(*piece).start()

    for s in range(STEPS - DEPTH, STEPS):
        for k in range(3):
            @pl.when(valid(s, k))
            def _():
                pltpu.make_async_remote_copy(
                    src_ref=gk.at[0, 0, pl.ds(0, UNIT)], dst_ref=land_gk.at[0, 0, pl.ds(0, UNIT)],
                    send_sem=bulk_send.at[k, s % DEPTH], recv_sem=glo_recv.at[0, 0],
                    device_id=(dp, dest[k]), device_id_type=MESH).wait_send()

    @pl.when(me == 3)
    def _():
        for piece in tails:
            tail(*piece).wait_send()

    for i in range(4):
        for u in range(LOC_UNITS if i < 2 else GLO_UNITS):
            owner = (u if i >= 2 or u >= FIRST_UNIT else u + LOC_UNITS) // PER
            sem = loc_recv.at[i, u] if i < 2 else glo_recv.at[i - 2, u]

            def await_rows(rows):
                view = lands[i].at[pl.ds(0, rows), :, pl.ds(u * UNIT, UNIT)]
                pltpu.make_async_remote_copy(
                    src_ref=view, dst_ref=view, send_sem=bulk_send.at[0, 0], recv_sem=sem,
                    device_id=(dp, dest[0]), device_id_type=MESH).wait_recv()

            if i == 3 and owner >= 2:
                short = me == owner - 2

                @pl.when(short)
                def _():
                    await_rows(ROWS - LATE[owner - 2])

                @pl.when(jnp.logical_and(me != owner, jnp.logical_not(short)))
                def _():
                    await_rows(ROWS)
            else:
                @pl.when(me != owner)
                def _():
                    await_rows(ROWS)


SLOTS = 6


def write_kernel(hid, new_kv, lk, lv, gk, gv, land_lk, land_lv, land_gk, land_gv,
                 hid_out, lk_out, lv_out, gk_out, gv_out, buf, in_sem, out_sem):
    me = lax.axis_index("a")
    hid_out[...] = hid[...]
    jobs = []
    for i in range(4):
        for u in range(LOC_UNITS if i < 2 else GLO_UNITS + 1):
            jobs.append((i, u))
    caches = (lk, lv, gk, gv)
    lands = (land_lk, land_lv, land_gk, land_gv)
    outs = (lk_out, lv_out, gk_out, gv_out)

    def load(n):
        i, u = jobs[n]
        slot = n % SLOTS
        if i >= 2 and u == GLO_UNITS:
            return
        full = u if i >= 2 or u >= FIRST_UNIT else u + LOC_UNITS
        owner, j = full // PER, full % PER

        @pl.when(me == owner)
        def _():
            pltpu.make_async_copy(caches[i].at[:, owner, pl.ds(j * UNIT, UNIT)], buf.at[slot], in_sem.at[slot]).start()

        @pl.when(me != owner)
        def _():
            pltpu.make_async_copy(lands[i].at[:, 0, pl.ds(u * UNIT, UNIT)], buf.at[slot], in_sem.at[slot]).start()

    def store(n):
        i, u = jobs[n]
        slot = n % SLOTS
        return pltpu.make_async_copy(buf.at[slot], outs[i].at[:, 0, pl.ds(u * UNIT, UNIT)], out_sem.at[slot])

    ahead = SLOTS // 2
    for n in range(ahead):
        load(n)
    for n, (i, u) in enumerate(jobs):
        slot = n % SLOTS
        if n + ahead < len(jobs):
            if n + ahead >= SLOTS:
                store(n + ahead - SLOTS).wait()
            load(n + ahead)
        pad = i >= 2 and u == GLO_UNITS
        if not pad:
            pltpu.make_async_copy(lands[i].at[:, 0, pl.ds(0, UNIT)], buf.at[slot], in_sem.at[slot]).wait()
        else:
            buf[slot] = jnp.zeros((ROWS, UNIT, HEAD), jnp.bfloat16)
        if pad or (i < 2 and u == SEQ % WINDOW // UNIT):
            head = buf[slot, :, 0:16, :].astype(jnp.float32)
            first = lax.broadcasted_iota(jnp.int32, head.shape, 1) == 0
            new = jnp.broadcast_to(new_kv[i].astype(jnp.float32)[:, None, :], head.shape)
            buf[slot, :, 0:16, :] = jnp.where(first, new, head).astype(jnp.bfloat16)
        store(n).start()
    for n in range(len(jobs) - SLOTS, len(jobs)):
        store(n).wait()


def late_kernel(late_a, late_b, old, out, sem):
    me = lax.axis_index("a")
    for target, late in enumerate((late_a, late_b)):
        @pl.when(me == target)
        def _():
            copies = []
            for r in range(LATE[target]):
                size = BLOCK if r < LATE[target] - 1 else BLOCK - LAST
                copies.append(pltpu.make_async_copy(
                    late.at[pl.ds(r * BLOCK, size)],
                    out.at[ROWS - LATE[target] + r, 0, pl.ds((target + 2) * BLOCK, size)], sem.at[r]))
            for copy in copies:
                copy.start()
            for copy in copies:
                copy.wait()


def last_kernel(late_c, old, out, sem):
    me = lax.axis_index("a")
    far = me // 2
    place = pl.multiple_of((1 - far) * ((me + 3) * BLOCK - LAST) + far * (SEQ + CACHE_ROOM - LAST), LAST)
    copy = pltpu.make_async_copy(late_c, out.at[ROWS - 1, 0, pl.ds(place, LAST)], sem)
    copy.start()
    copy.wait()


def trig_table():
    half = HEAD // 2
    inv_freq = ROPE_BASE ** (-2.0 * np.arange(half) / HEAD)
    angles = SEQ * inv_freq
    return np.stack([np.cos(angles), np.sin(angles)]).astype(np.float32)


def solution(mesh):
    cache_in = P('dp', None, 'a', None)
    cache_out = P('dp', 'a', None, None)
    rows_spec = P('dp', None)
    layer_specs = (P(None, 'a'), P(None, 'a'), P(None, 'a'), P('a', None), P(None), P(None))
    in_specs = (rows_spec, cache_in, cache_in, cache_in, cache_in) + layer_specs + layer_specs
    out_specs = (rows_spec, cache_out, cache_out, cache_out, cache_out)
    bf16, f32 = jnp.bfloat16, jnp.float32
    anywhere = pl.BlockSpec(memory_space=pl.ANY)
    vmem = pl.BlockSpec(memory_space=pltpu.VMEM)

    def device_step(hidden_in, loc_k, loc_v, glo_k, glo_v, loc_wq, loc_wk, loc_wv, loc_wo, loc_pre, loc_post, glo_wq, glo_wk, glo_wv, glo_wo, glo_pre, glo_post):
        model = hidden_in.shape[1]
        gains = [loc_pre, loc_post, glo_pre, glo_post]
        loc_land = jax.ShapeDtypeStruct((ROWS, 1, WINDOW, HEAD), bf16)
        glo_land = jax.ShapeDtypeStruct((ROWS, 1, SEQ, HEAD), bf16)
        dma = pltpu.SemaphoreType.DMA
        moved = pl.pallas_call(
            move_kernel,
            out_shape=(loc_land, loc_land, glo_land, glo_land,
                       jax.ShapeDtypeStruct((ROWS, model), bf16), jax.ShapeDtypeStruct((4, ROWS, HEAD), bf16),
                       jax.ShapeDtypeStruct((LATE[0] * BLOCK - LAST, HEAD), bf16),
                       jax.ShapeDtypeStruct((LATE[1] * BLOCK - LAST, HEAD), bf16), jax.ShapeDtypeStruct((LAST, HEAD), bf16)),
            in_specs=[anywhere] * 18,
            out_specs=(anywhere,) * 9,
            scratch_shapes=[
                pltpu.VMEM((ROWS, model), bf16), pltpu.VMEM((2, HEAD // 2), f32),
                pltpu.VMEM((model,), bf16), pltpu.VMEM((model,), bf16), pltpu.VMEM((model,), bf16), pltpu.VMEM((model,), bf16),
                pltpu.VMEM((4, ROWS, HEAD), bf16), pltpu.VMEM((ROWS, model), bf16),
                pltpu.VMEM((2,) + loc_wq.shape, bf16), pltpu.VMEM((2,) + loc_wk.shape, bf16),
                pltpu.VMEM((2,) + loc_wv.shape, bf16), pltpu.VMEM((2,) + loc_wo.shape, bf16),
                pltpu.VMEM((2, 2, BLOCK, HEAD), bf16),
                pltpu.VMEM((2, GROUP, 2 * ROWS, HEAD), bf16),
                pltpu.VMEM((2, GROUP, 2 * ROWS, HEAD + 2 * STAT), f32),
                pltpu.VMEM((2, 4, 2 * ROWS, HEAD + 2 * STAT), f32),
                pltpu.VMEM((2, 2, 2 * ROWS, HEAD + 2 * STAT), f32),
                pltpu.VMEM((2, 2, ROWS, 2 * HEAD), bf16),
                pltpu.VMEM((2, 2, ROWS, model), f32), pltpu.VMEM((2, 2, ROWS, model // 2), bf16),
                pltpu.VMEM((2,) + loc_wo.shape, bf16),
                dma((3, DEPTH)), dma((2, LOC_UNITS)), dma((2, GLO_UNITS)), dma((8,)), dma((2, 2)),
                dma((20,)), dma((20,)), dma((2, LATE[0])),
                dma((LATE[0] - LATE[1], PER)), dma((6,)), dma((2,)), dma((2,)), dma((DEPTH,)), dma((2,))],
            compiler_params=pltpu.CompilerParams(collective_id=0, has_side_effects=True),
        )(hidden_in, jnp.asarray(trig_table()), *gains, loc_k, loc_v, glo_k, glo_v,
          loc_wq, loc_wk, loc_wv, loc_wo, glo_wq, glo_wk, glo_wv, glo_wo)
        land, hid, new_kv = moved[:4], moved[4], moved[5]
        late_a = lax.ppermute(moved[6], 'a', [(2, 0)])
        late_b = lax.ppermute(moved[7], 'a', [(3, 1)])
        late_c = lax.ppermute(moved[8], 'a', [(2, 0), (3, 1)])
        hidden_out, loc_k_out, loc_v_out, glo_k_out, glo_v_out = pl.pallas_call(
            write_kernel,
            out_shape=(jax.ShapeDtypeStruct((ROWS, model), bf16),)
            + (jax.ShapeDtypeStruct((ROWS, 1, WINDOW, HEAD), bf16),) * 2
            + (jax.ShapeDtypeStruct((ROWS, 1, SEQ + CACHE_ROOM, HEAD), bf16),) * 2,
            in_specs=[vmem, vmem] + [anywhere] * 8,
            out_specs=(vmem,) + (anywhere,) * 4,
            scratch_shapes=[pltpu.VMEM((SLOTS, ROWS, UNIT, HEAD), bf16), dma((SLOTS,)), dma((SLOTS,))],
            compiler_params=pltpu.CompilerParams(vmem_limit_bytes=50 * 2 ** 20),
            cost_estimate=pl.CostEstimate(flops=10 ** 9, bytes_accessed=180 * 10 ** 6, transcendentals=0),
        )(hid, new_kv, loc_k, loc_v, glo_k, glo_v, *land)
        glo_v_out = pl.pallas_call(
            late_kernel,
            out_shape=jax.ShapeDtypeStruct(glo_v_out.shape, bf16),
            in_specs=[vmem, vmem, anywhere],
            out_specs=anywhere,
            scratch_shapes=[dma((LATE[0],))],
            input_output_aliases={2: 0},
            compiler_params=pltpu.CompilerParams(vmem_limit_bytes=16 * 2 ** 20),
            cost_estimate=pl.CostEstimate(flops=10 ** 7, bytes_accessed=4 * late_a.size, transcendentals=0),
        )(late_a, late_b, glo_v_out)
        glo_v_out = pl.pallas_call(
            last_kernel,
            out_shape=jax.ShapeDtypeStruct(glo_v_out.shape, bf16),
            in_specs=[vmem, anywhere],
            out_specs=anywhere,
            scratch_shapes=[dma],
            input_output_aliases={1: 0},
            compiler_params=pltpu.CompilerParams(vmem_limit_bytes=16 * 2 ** 20),
            cost_estimate=pl.CostEstimate(flops=10 ** 6, bytes_accessed=4 * late_c.size, transcendentals=0),
        )(late_c, glo_v_out)
        return hidden_out, loc_k_out, loc_v_out, glo_k_out, glo_v_out

    return jax.shard_map(device_step, mesh=mesh, in_specs=in_specs, out_specs=out_specs, check_vma=False)
```

```python
import jax
import jax.numpy as jnp
import numpy as np
from jax import lax
from jax.experimental import pallas as pl
from jax.experimental.pallas import tpu as pltpu
from jax.sharding import PartitionSpec as P

SOFTCAP = 50.0
NORM_EPS = 1e-6
ROPE_BASE = 10000.0
WINDOW = 4096
CACHE_ROOM = 512

GROUP = 4
ROWS = 8
BLOCK = 1536
UNIT = 512
HEAD = 256
SEQ = GROUP * BLOCK
PER = BLOCK // UNIT
GLO_UNITS = SEQ // UNIT
LOC_UNITS = WINDOW // UNIT
FIRST_UNIT = (SEQ - WINDOW) // UNIT
STEPS = 4 * ROWS * PER
DEPTH = 2
LATE = (5, 4)
MESH = pl.DeviceIdType.MESH
PIECES = 8
WO_ROWS = 64
LAST = 256
FIRST = 8
STAT = 64
LOW = -1e30


def peers(me):
    return (me + 1 - 2 * (me % 2), (me + 2) % 4, 3 - me)


def norm(hidden, gain):
    mean_sq = jnp.mean(hidden * hidden, axis=-1, keepdims=True)
    return hidden * lax.rsqrt(mean_sq + NORM_EPS) * (1.0 + gain.astype(jnp.float32).reshape(1, -1))


def softcap(scores):
    return SOFTCAP * jnp.tanh(scores * (HEAD ** -0.5) / SOFTCAP)


def move_kernel(hid_in, trig_in, lpre_in, lpost_in, gpre_in, gpost_in, lk, lv, gk, gv, lwq, lwk, lwv, lwo, gwq, gwk, gwv, gwo,
                land_lk, land_lv, land_gk, land_gv, hid_out, new_out, late_a, late_b, late_c,
                hid, trig, lpre, lpost, gpre, gpost, new_kv, hid_end, wq, wk, wv, wo, kvbuf, qbuf, part, precv, pair, att, ybuf, hbuf, wo_far,
                bulk_send, loc_recv, glo_recv, w_sem, kv_sem, ex_send, ex_recv, late_sem, tail_send, small_sem, out_sem, first_sem, wo_send, wo_recv):
    dp = lax.axis_index("dp")
    me = lax.axis_index("a")
    dest = peers(me)
    caches = (lk, lv, gk, gv)
    lands = (land_lk, land_lv, land_gk, land_gv)

    first = [pltpu.make_async_copy(lk.at[0, dest[k], pl.ds(0, FIRST)], kvbuf.at[0, k - 1, pl.ds(0, FIRST)], first_sem.at[k - 1])
             for k in (1, 2)]

    @pl.when(me >= 2)
    def _():
        for copy in first:
            copy.start()

    barrier = pltpu.get_barrier_semaphore()
    for peer in dest:
        pl.semaphore_signal(barrier, inc=1, device_id=(dp, peer), device_id_type=MESH)
    pl.semaphore_wait(barrier, 3)

    def coords(step):
        c = step // (ROWS * PER) * (3 - 2 * (me // 2)) % 4
        return c, (step // PER) % ROWS, step % PER

    def valid(step, k):
        c, r, j = coords(step)
        in_window = jnp.logical_or(c >= 2, PER * me + j >= FIRST_UNIT)
        ok = jnp.logical_and(step >= 0, in_window)
        if k == 1:
            late = jnp.logical_and(jnp.logical_and(c == 3, r >= ROWS - LATE[0]), me >= 2)
            ok = jnp.logical_and(ok, jnp.logical_not(late))
        return ok

    def pump(step, opening=False):
        c, r, j = coords(step)
        slot = step % DEPTH
        for k in range(3):
            @pl.when(valid(step - DEPTH, k))
            def _():
                pltpu.make_async_remote_copy(
                    src_ref=gk.at[0, 0, pl.ds(0, UNIT)], dst_ref=land_gk.at[0, 0, pl.ds(0, UNIT)],
                    send_sem=bulk_send.at[k, slot], recv_sem=glo_recv.at[0, 0],
                    device_id=(dp, dest[k]), device_id_type=MESH).wait_send()
        def piece(s, ref):
            rows = pl.ds(pl.multiple_of(s % PIECES * WO_ROWS, WO_ROWS), WO_ROWS)
            return pltpu.make_async_remote_copy(
                src_ref=ref.at[rows], dst_ref=wo_far.at[s // PIECES, rows], send_sem=wo_send.at[s % DEPTH],
                recv_sem=wo_recv.at[s // PIECES], device_id=(dp, dest[1]), device_id_type=MESH)

        before = step - DEPTH

        @pl.when(jnp.logical_and(me < 2, jnp.logical_and(before >= 0, before < 2 * PIECES)))
        def _():
            piece(before, lwo).wait_send()

        for i, ref in enumerate((lwo, gwo)):
            @pl.when(jnp.logical_and(me < 2, jnp.logical_and(step >= i * PIECES, step < (i + 1) * PIECES)))
            def _():
                piece(step, ref).start()

        unit = PER * me + j
        for i in range(4):
            place = unit % LOC_UNITS if i < 2 else unit
            sem = loc_recv.at[i, place] if i < 2 else glo_recv.at[i - 2, place]
            for k in range(3):
                now = jnp.logical_and(c == i, valid(step, k))
                if opening and k:
                    now = jnp.logical_and(now, me < 2)

                @pl.when(now)
                def _():
                    pltpu.make_async_remote_copy(
                        src_ref=caches[i].at[r, dest[k], pl.ds(pl.multiple_of(j * UNIT, UNIT), UNIT)],
                        dst_ref=lands[i].at[r, 0, pl.ds(pl.multiple_of(place * UNIT, UNIT), UNIT)],
                        send_sem=bulk_send.at[k, slot], recv_sem=sem,
                        device_id=(dp, dest[k]), device_id_type=MESH).start()

    def send(index, k, src, dst):
        return pltpu.make_async_remote_copy(
            src_ref=src, dst_ref=dst, send_sem=ex_send.at[index], recv_sem=ex_recv.at[index],
            device_id=(dp, dest[k]), device_id_type=MESH)

    weights = [pltpu.make_async_copy(src, dst, w_sem.at[i]) for i, (src, dst) in enumerate((
        (lwq, wq.at[0]), (lwk, wk.at[0]), (lwv, wv.at[0]), (lwo, wo.at[0]),
        (gwq, wq.at[1]), (gwk, wk.at[1]), (gwv, wv.at[1]), (gwo, wo.at[1])))]

    small = [pltpu.make_async_copy(src, dst, small_sem.at[i]) for i, (src, dst) in enumerate((
        (hid_in, hid), (trig_in, trig), (lpre_in, lpre), (lpost_in, lpost),
        (gpre_in, gpre), (gpost_in, gpost)))]

    @pl.when(me >= 2)
    def _():
        place = (PER * me) % LOC_UNITS
        for k in (1, 2):
            first[k - 1].wait()
            pltpu.make_async_remote_copy(
                src_ref=kvbuf.at[0, k - 1, pl.ds(0, FIRST)],
                dst_ref=land_lk.at[0, 0, pl.ds(pl.multiple_of(place * UNIT, UNIT), FIRST)],
                send_sem=bulk_send.at[k, 0], recv_sem=loc_recv.at[0, place],
                device_id=(dp, dest[k]), device_id_type=MESH).start()
            pltpu.make_async_remote_copy(
                src_ref=lk.at[0, dest[k], pl.ds(FIRST, UNIT - FIRST)],
                dst_ref=land_lk.at[0, 0, pl.ds(pl.multiple_of(place * UNIT + FIRST, FIRST), UNIT - FIRST)],
                send_sem=bulk_send.at[k, 0], recv_sem=loc_recv.at[0, place],
                device_id=(dp, dest[k]), device_id_type=MESH).start()

    pump(0, opening=True)
    pump(1)
    for copy in small + weights:
        copy.start()
    for copy in small:
        copy.wait()

    cosine, sine = trig[0:1, :], trig[1:2, :]

    def rope(heads):
        first, second = heads[:, :HEAD // 2], heads[:, HEAD // 2:]
        return jnp.concatenate([first * cosine - second * sine, second * cosine + first * sine], axis=-1)

    def layer(index, hidden, key_ref, value_ref, pre, post, step):
        normed = norm(hidden, pre[...]).astype(jnp.bfloat16)
        if index == 0:
            for copy in weights[:4]:
                copy.wait()
        else:
            for copy in weights[4:]:
                copy.wait()
        q = jnp.dot(normed, wq[index], preferred_element_type=jnp.float32)
        q = jnp.concatenate([rope(q[:, :HEAD]), rope(q[:, HEAD:])], axis=0).astype(jnp.bfloat16)
        new_k = rope(jnp.dot(normed, wk[index], preferred_element_type=jnp.float32)).astype(jnp.bfloat16)
        new_v = jnp.dot(normed, wv[index], preferred_element_type=jnp.float32).astype(jnp.bfloat16)
        new_kv[2 * index] = new_k
        new_kv[2 * index + 1] = new_v
        own_q = qbuf.at[index]
        own_q[me] = q
        base = 8 * index
        near = send(base, 0, own_q.at[me], own_q.at[me])
        far = send(base + 1, 1, own_q.at[me], own_q.at[me])
        near.start()
        far.start()
        pump(step)
        far.wait()
        onward = send(base + 2, 0, own_q.at[dest[1]], own_q.at[dest[1]])
        onward.start()
        near.wait()
        onward.wait()

        def fetch(item, slot):
            h, r = item // ROWS, item % ROWS
            return (pltpu.make_async_copy(key_ref.at[r, h], kvbuf.at[slot, 0], kv_sem.at[slot, 0]),
                    pltpu.make_async_copy(value_ref.at[r, h], kvbuf.at[slot, 1], kv_sem.at[slot, 1]))

        for copy in fetch(0, 0):
            copy.start()
        items = GROUP * ROWS

        def body(item, carry):
            pump(step + 1 + item)
            slot = item % 2
            h, r = item // ROWS, item % ROWS

            @pl.when(item + 1 < items)
            def _():
                for copy in fetch(item + 1, 1 - slot):
                    copy.start()

            copy_k, copy_v = fetch(item, slot)
            copy_k.wait()
            scores = softcap(lax.dot_general(own_q[h], kvbuf[slot, 0], (((1,), (1,)), ((), ())),
                                             preferred_element_type=jnp.float32))
            if index == 0:
                place = me * BLOCK + lax.broadcasted_iota(jnp.int32, scores.shape, 1)
                inside = place > SEQ - WINDOW
                scores = jnp.where(inside, scores, LOW)
            top = jnp.max(scores, axis=-1, keepdims=True)
            e = jnp.exp(scores - top)
            if index == 0:
                e = jnp.where(inside, e, 0.0)
            total = jnp.sum(e, axis=-1, keepdims=True)
            copy_v.wait()
            out = jnp.dot(e.astype(jnp.bfloat16), kvbuf[slot, 1], preferred_element_type=jnp.float32)
            wide = jnp.concatenate([out, jnp.broadcast_to(top, (2 * ROWS, STAT)),
                                    jnp.broadcast_to(total, (2 * ROWS, STAT))], axis=-1)
            row = lax.broadcasted_iota(jnp.int32, wide.shape, 0) % ROWS
            part[index, h] = jnp.where(row == r, wide, part[index, h])
            return carry

        lax.fori_loop(0, items, body, 0)
        step = step + 1 + items

        mine = part.at[index]
        theirs = precv.at[index]
        near = (send(base + 3, 0, mine.at[dest[0]], theirs.at[0]), send(base + 4, 0, mine.at[dest[2]], theirs.at[1]))
        for copy in near:
            copy.start()
        new_k2 = jnp.concatenate([new_k, new_k], axis=0).astype(jnp.float32)
        new_v2 = jnp.concatenate([new_v, new_v], axis=0).astype(jnp.float32)
        new_s = softcap(jnp.sum(q.astype(jnp.float32) * new_k2, axis=-1, keepdims=True))
        new = (new_v2, new_s, jnp.ones_like(new_s))
        for copy in near:
            copy.wait()

        def split(block):
            return block[:, :HEAD], block[:, HEAD:HEAD + 1], block[:, HEAD + STAT:HEAD + STAT + 1]

        def merge(blocks):
            top = blocks[0][1]
            for _, m, _ in blocks[1:]:
                top = jnp.maximum(top, m)
            acc, total = 0.0, 0.0
            for o, m, l in blocks:
                scale = jnp.exp(m - top)
                acc = acc + scale * o
                total = total + scale * l
            return acc, top, total

        def packed(acc, top, total):
            return jnp.concatenate([acc, jnp.broadcast_to(top, (2 * ROWS, STAT)),
                                    jnp.broadcast_to(total, (2 * ROWS, STAT))], axis=-1)

        both = [split(mine[me]), split(theirs[0]), new]
        across = pair.at[index]
        across[0] = packed(*merge([split(mine[dest[1]]), split(theirs[1])]))
        across[1] = packed(*merge(both))
        heads = att.at[index]
        far = [send(base + 5 + i, 1, across.at[i], theirs.at[2 + i]) for i in (0, 1)]
        y_ref = ybuf.at[index]
        half = hbuf.at[index]
        side = me % 2
        near = send(base + 7, 0, y_ref.at[side], y_ref.at[side])
        back = send(16 + 2 * index, 1, half.at[side], half.at[side])
        swap = send(17 + 2 * index, 0, half.at[side], half.at[side])

        @pl.when(me < 2)
        def _():
            for copy in far:
                copy.start()

        pump(step)

        @pl.when(me >= 2)
        def _():
            for copy in far:
                copy.wait_recv()

            def finished(blocks):
                acc, _, total = merge(blocks)
                out = (acc / total).astype(jnp.bfloat16)
                return jnp.concatenate([out[:ROWS], out[ROWS:]], axis=-1)

            heads[0] = finished(both + [split(theirs[2])])
            heads[1] = finished([split(across[0]), split(theirs[3])])

        pump(step + 1)

        @pl.when(me >= 2)
        def _():
            pltpu.make_async_remote_copy(
                src_ref=wo_far.at[index], dst_ref=wo_far.at[index], send_sem=wo_send.at[0], recv_sem=wo_recv.at[index],
                device_id=(dp, dest[1]), device_id_type=MESH).wait_recv()
            y_ref[side] = (jnp.dot(heads[0], wo[index], preferred_element_type=jnp.float32)
                           + jnp.dot(heads[1], wo_far[index], preferred_element_type=jnp.float32))
            near.start()
            near.wait()
            after = (hidden + norm(y_ref[0] + y_ref[1], post[...])).astype(jnp.bfloat16)
            half[0] = after[:, :after.shape[1] // 2]
            half[1] = after[:, after.shape[1] // 2:]
            back.start()

        pump(step + 2)

        @pl.when(me >= 2)
        def _():
            back.wait_send()

        @pl.when(me < 2)
        def _():
            for copy in far:
                copy.wait_send()
            back.wait_recv()
            swap.start()
            swap.wait()

        return jnp.concatenate([half[0], half[1]], axis=-1), step + 3

    part[...] = jnp.zeros_like(part)
    hidden, step = layer(0, hid[...].astype(jnp.float32), lk, lv, lpre, lpost, 2)
    hidden, step = layer(1, hidden.astype(jnp.float32), gk, gv, gpre, gpost, step)
    hid_end[...] = hidden
    outs = (pltpu.make_async_copy(hid_end, hid_out, out_sem.at[0]), pltpu.make_async_copy(new_kv, new_out, out_sem.at[1]))
    for copy in outs:
        copy.start()
    for copy in outs:
        copy.wait()

    for late, target, rows in ((late_a, 0, LATE[0]), (late_b, 1, LATE[1])):
        @pl.when(me == target + 2)
        def _():
            def late_in(r):
                return pltpu.make_async_copy(gv.at[ROWS - rows + r, target], kvbuf.at[(r // 2) % 2, r % 2], late_sem.at[0, r])

            def late_out(r):
                buf, size = kvbuf.at[(r // 2) % 2, r % 2], BLOCK if r < rows - 1 else BLOCK - LAST
                return pltpu.make_async_copy(buf.at[pl.ds(0, size)], late.at[pl.ds(r * BLOCK, size)], late_sem.at[1, r])

            end = kvbuf.at[((rows - 1) // 2) % 2, (rows - 1) % 2, pl.ds(BLOCK - LAST, LAST)]
            last_out = pltpu.make_async_copy(end, late_c, late_sem.at[0, rows - 1])
            for r in range(rows):
                if r >= 4:
                    late_out(r - 4).wait()
                late_in(r).start()
                if r >= 1:
                    late_in(r - 1).wait()
                    late_out(r - 1).start()
            late_in(rows - 1).wait()
            late_out(rows - 1).start()
            last_out.start()
            for r in range(max(rows - 4, 0), rows):
                late_out(r).wait()
            last_out.wait()

    def rest(s, carry):
        pump(s)
        return carry

    lax.fori_loop(step, STEPS, rest, 0)

    def tail(r, j):
        unit = PER * me + j
        return pltpu.make_async_remote_copy(
            src_ref=gv.at[r, dest[1], pl.ds(j * UNIT, UNIT)],
            dst_ref=land_gv.at[r, 0, pl.ds(pl.multiple_of(unit * UNIT, UNIT), UNIT)],
            send_sem=tail_send.at[r - ROWS + LATE[0], j], recv_sem=glo_recv.at[1, unit],
            device_id=(dp, dest[1]), device_id_type=MESH)

    tails = [(r, j) for r in range(ROWS - LATE[0], ROWS - LATE[1]) for j in range(PER)]

    @pl.when(me == 3)
    def _():
        for piece in tails:
            tail(*piece).start()

    for s in range(STEPS - DEPTH, STEPS):
        for k in range(3):
            @pl.when(valid(s, k))
            def _():
                pltpu.make_async_remote_copy(
                    src_ref=gk.at[0, 0, pl.ds(0, UNIT)], dst_ref=land_gk.at[0, 0, pl.ds(0, UNIT)],
                    send_sem=bulk_send.at[k, s % DEPTH], recv_sem=glo_recv.at[0, 0],
                    device_id=(dp, dest[k]), device_id_type=MESH).wait_send()

    @pl.when(me == 3)
    def _():
        for piece in tails:
            tail(*piece).wait_send()

    for i in range(4):
        for u in range(LOC_UNITS if i < 2 else GLO_UNITS):
            owner = (u if i >= 2 or u >= FIRST_UNIT else u + LOC_UNITS) // PER
            sem = loc_recv.at[i, u] if i < 2 else glo_recv.at[i - 2, u]

            def await_rows(rows):
                view = lands[i].at[pl.ds(0, rows), :, pl.ds(u * UNIT, UNIT)]
                pltpu.make_async_remote_copy(
                    src_ref=view, dst_ref=view, send_sem=bulk_send.at[0, 0], recv_sem=sem,
                    device_id=(dp, dest[0]), device_id_type=MESH).wait_recv()

            if i == 3 and owner >= 2:
                short = me == owner - 2

                @pl.when(short)
                def _():
                    await_rows(ROWS - LATE[owner - 2])

                @pl.when(jnp.logical_and(me != owner, jnp.logical_not(short)))
                def _():
                    await_rows(ROWS)
            else:
                @pl.when(me != owner)
                def _():
                    await_rows(ROWS)


SLOTS = 6


def write_kernel(hid, new_kv, lk, lv, gk, gv, land_lk, land_lv, land_gk, land_gv,
                 hid_out, lk_out, lv_out, gk_out, gv_out, buf, in_sem, out_sem):
    me = lax.axis_index("a")
    hid_out[...] = hid[...]
    jobs = []
    for i in range(4):
        for u in range(LOC_UNITS if i < 2 else GLO_UNITS + 1):
            jobs.append((i, u))
    caches = (lk, lv, gk, gv)
    lands = (land_lk, land_lv, land_gk, land_gv)
    outs = (lk_out, lv_out, gk_out, gv_out)

    def load(n):
        i, u = jobs[n]
        slot = n % SLOTS
        if i >= 2 and u == GLO_UNITS:
            return
        full = u if i >= 2 or u >= FIRST_UNIT else u + LOC_UNITS
        owner, j = full // PER, full % PER

        @pl.when(me == owner)
        def _():
            pltpu.make_async_copy(caches[i].at[:, owner, pl.ds(j * UNIT, UNIT)], buf.at[slot], in_sem.at[slot]).start()

        @pl.when(me != owner)
        def _():
            pltpu.make_async_copy(lands[i].at[:, 0, pl.ds(u * UNIT, UNIT)], buf.at[slot], in_sem.at[slot]).start()

    def store(n):
        i, u = jobs[n]
        slot = n % SLOTS
        return pltpu.make_async_copy(buf.at[slot], outs[i].at[:, 0, pl.ds(u * UNIT, UNIT)], out_sem.at[slot])

    ahead = SLOTS // 2
    for n in range(ahead):
        load(n)
    for n, (i, u) in enumerate(jobs):
        slot = n % SLOTS
        if n + ahead < len(jobs):
            if n + ahead >= SLOTS:
                store(n + ahead - SLOTS).wait()
            load(n + ahead)
        pad = i >= 2 and u == GLO_UNITS
        if not pad:
            pltpu.make_async_copy(lands[i].at[:, 0, pl.ds(0, UNIT)], buf.at[slot], in_sem.at[slot]).wait()
        else:
            buf[slot] = jnp.zeros((ROWS, UNIT, HEAD), jnp.bfloat16)
        if pad or (i < 2 and u == SEQ % WINDOW // UNIT):
            head = buf[slot, :, 0:16, :].astype(jnp.float32)
            first = lax.broadcasted_iota(jnp.int32, head.shape, 1) == 0
            new = jnp.broadcast_to(new_kv[i].astype(jnp.float32)[:, None, :], head.shape)
            buf[slot, :, 0:16, :] = jnp.where(first, new, head).astype(jnp.bfloat16)
        store(n).start()
    for n in range(len(jobs) - SLOTS, len(jobs)):
        store(n).wait()


def late_kernel(late_a, late_b, old, out, sem):
    me = lax.axis_index("a")
    for target, late in enumerate((late_a, late_b)):
        @pl.when(me == target)
        def _():
            copies = []
            for r in range(LATE[target]):
                size = BLOCK if r < LATE[target] - 1 else BLOCK - LAST
                copies.append(pltpu.make_async_copy(
                    late.at[pl.ds(r * BLOCK, size)],
                    out.at[ROWS - LATE[target] + r, 0, pl.ds((target + 2) * BLOCK, size)], sem.at[r]))
            for copy in copies:
                copy.start()
            for copy in copies:
                copy.wait()


def last_kernel(late_c, old, out, sem):
    me = lax.axis_index("a")

    @pl.when(me < 2)
    def _():
        place = pl.multiple_of((me + 3) * BLOCK - LAST, LAST)
        copy = pltpu.make_async_copy(late_c, out.at[ROWS - 1, 0, pl.ds(place, LAST)], sem)
        copy.start()
        copy.wait()


def trig_table():
    half = HEAD // 2
    inv_freq = ROPE_BASE ** (-2.0 * np.arange(half) / HEAD)
    angles = SEQ * inv_freq
    return np.stack([np.cos(angles), np.sin(angles)]).astype(np.float32)


def solution(mesh):
    cache_in = P('dp', None, 'a', None)
    cache_out = P('dp', 'a', None, None)
    rows_spec = P('dp', None)
    layer_specs = (P(None, 'a'), P(None, 'a'), P(None, 'a'), P('a', None), P(None), P(None))
    in_specs = (rows_spec, cache_in, cache_in, cache_in, cache_in) + layer_specs + layer_specs
    out_specs = (rows_spec, cache_out, cache_out, cache_out, cache_out)
    bf16, f32 = jnp.bfloat16, jnp.float32
    anywhere = pl.BlockSpec(memory_space=pl.ANY)
    vmem = pl.BlockSpec(memory_space=pltpu.VMEM)

    def device_step(hidden_in, loc_k, loc_v, glo_k, glo_v, loc_wq, loc_wk, loc_wv, loc_wo, loc_pre, loc_post, glo_wq, glo_wk, glo_wv, glo_wo, glo_pre, glo_post):
        model = hidden_in.shape[1]
        gains = [loc_pre, loc_post, glo_pre, glo_post]
        loc_land = jax.ShapeDtypeStruct((ROWS, 1, WINDOW, HEAD), bf16)
        glo_land = jax.ShapeDtypeStruct((ROWS, 1, SEQ, HEAD), bf16)
        dma = pltpu.SemaphoreType.DMA
        moved = pl.pallas_call(
            move_kernel,
            out_shape=(loc_land, loc_land, glo_land, glo_land,
                       jax.ShapeDtypeStruct((ROWS, model), bf16), jax.ShapeDtypeStruct((4, ROWS, HEAD), bf16),
                       jax.ShapeDtypeStruct((LATE[0] * BLOCK - LAST, HEAD), bf16),
                       jax.ShapeDtypeStruct((LATE[1] * BLOCK - LAST, HEAD), bf16), jax.ShapeDtypeStruct((LAST, HEAD), bf16)),
            in_specs=[anywhere] * 18,
            out_specs=(anywhere,) * 9,
            scratch_shapes=[
                pltpu.VMEM((ROWS, model), bf16), pltpu.VMEM((2, HEAD // 2), f32),
                pltpu.VMEM((model,), bf16), pltpu.VMEM((model,), bf16), pltpu.VMEM((model,), bf16), pltpu.VMEM((model,), bf16),
                pltpu.VMEM((4, ROWS, HEAD), bf16), pltpu.VMEM((ROWS, model), bf16),
                pltpu.VMEM((2,) + loc_wq.shape, bf16), pltpu.VMEM((2,) + loc_wk.shape, bf16),
                pltpu.VMEM((2,) + loc_wv.shape, bf16), pltpu.VMEM((2,) + loc_wo.shape, bf16),
                pltpu.VMEM((2, 2, BLOCK, HEAD), bf16),
                pltpu.VMEM((2, GROUP, 2 * ROWS, HEAD), bf16),
                pltpu.VMEM((2, GROUP, 2 * ROWS, HEAD + 2 * STAT), f32),
                pltpu.VMEM((2, 4, 2 * ROWS, HEAD + 2 * STAT), f32),
                pltpu.VMEM((2, 2, 2 * ROWS, HEAD + 2 * STAT), f32),
                pltpu.VMEM((2, 2, ROWS, 2 * HEAD), bf16),
                pltpu.VMEM((2, 2, ROWS, model), f32), pltpu.VMEM((2, 2, ROWS, model // 2), bf16),
                pltpu.VMEM((2,) + loc_wo.shape, bf16),
                dma((3, DEPTH)), dma((2, LOC_UNITS)), dma((2, GLO_UNITS)), dma((8,)), dma((2, 2)),
                dma((20,)), dma((20,)), dma((2, LATE[0])),
                dma((LATE[0] - LATE[1], PER)), dma((6,)), dma((2,)), dma((2,)), dma((DEPTH,)), dma((2,))],
            compiler_params=pltpu.CompilerParams(collective_id=0, has_side_effects=True),
        )(hidden_in, jnp.asarray(trig_table()), *gains, loc_k, loc_v, glo_k, glo_v,
          loc_wq, loc_wk, loc_wv, loc_wo, glo_wq, glo_wk, glo_wv, glo_wo)
        land, hid, new_kv = moved[:4], moved[4], moved[5]
        late_a = lax.ppermute(moved[6], 'a', [(2, 0)])
        late_b = lax.ppermute(moved[7], 'a', [(3, 1)])
        late_c = lax.ppermute(moved[8], 'a', [(2, 0), (3, 1)])
        hidden_out, loc_k_out, loc_v_out, glo_k_out, glo_v_out = pl.pallas_call(
            write_kernel,
            out_shape=(jax.ShapeDtypeStruct((ROWS, model), bf16),)
            + (jax.ShapeDtypeStruct((ROWS, 1, WINDOW, HEAD), bf16),) * 2
            + (jax.ShapeDtypeStruct((ROWS, 1, SEQ + CACHE_ROOM, HEAD), bf16),) * 2,
            in_specs=[vmem, vmem] + [anywhere] * 8,
            out_specs=(vmem,) + (anywhere,) * 4,
            scratch_shapes=[pltpu.VMEM((SLOTS, ROWS, UNIT, HEAD), bf16), dma((SLOTS,)), dma((SLOTS,))],
            compiler_params=pltpu.CompilerParams(vmem_limit_bytes=50 * 2 ** 20),
            cost_estimate=pl.CostEstimate(flops=10 ** 9, bytes_accessed=180 * 10 ** 6, transcendentals=0),
        )(hid, new_kv, loc_k, loc_v, glo_k, glo_v, *land)
        glo_v_out = pl.pallas_call(
            late_kernel,
            out_shape=jax.ShapeDtypeStruct(glo_v_out.shape, bf16),
            in_specs=[vmem, vmem, anywhere],
            out_specs=anywhere,
            scratch_shapes=[dma((LATE[0],))],
            input_output_aliases={2: 0},
            compiler_params=pltpu.CompilerParams(vmem_limit_bytes=16 * 2 ** 20),
            cost_estimate=pl.CostEstimate(flops=10 ** 7, bytes_accessed=4 * late_a.size, transcendentals=0),
        )(late_a, late_b, glo_v_out)
        glo_v_out = pl.pallas_call(
            last_kernel,
            out_shape=jax.ShapeDtypeStruct(glo_v_out.shape, bf16),
            in_specs=[vmem, anywhere],
            out_specs=anywhere,
            scratch_shapes=[dma],
            input_output_aliases={1: 0},
            compiler_params=pltpu.CompilerParams(vmem_limit_bytes=16 * 2 ** 20),
            cost_estimate=pl.CostEstimate(flops=10 ** 6, bytes_accessed=4 * late_c.size, transcendentals=0),
        )(late_c, glo_v_out)
        return hidden_out, loc_k_out, loc_v_out, glo_k_out, glo_v_out

    return jax.shard_map(device_step, mesh=mesh, in_specs=in_specs, out_specs=out_specs, check_vma=False)
```
